256 devices in a mesh: col: 32 (over z, y), row: 8 (over x, core).
Axes of the slice: x: 4, y: 4, z: 8, core: 2. Of those that a mesh axis runs over, the one named last changes fastest.
Arguments:
- inter_mask: int32 [65536, 4096], P('row', 'col')
- emb_user: bfloat16 [65536, 64], P(('row', 'col'))
- emb_item: bfloat16 [4096, 64], P(('col', 'row'))
- triples: int32 [128, 3], replicated
Outputs:
- output 1: bfloat16 [65536, 64], P(('row', 'col'))
- output 2: bfloat16 [4096, 64], P(('col', 'row'))
- output 3: float32 [], replicated
All inputs are finite; a program needn't handle non-finite values.
Results may differ from the reference program's by a relative error of at most 0.00519882.
Values are sent between devices in bfloat16 or wider.
A program may use at most 768 MiB of HBM per device.

```python
import jax
import jax.numpy as jnp
from jax import lax

USERS = 65536
ITEMS = 4096
DIM = 64
LAYERS = 3
TRIPLES = 128
USER_DEGREE = 3


def draw_triples(trip_key):
    key_user, key_pos, key_neg = jax.random.split(trip_key, 3)
    row_pos = jnp.arange(TRIPLES)
    user_ids = jax.random.randint(key_user, (TRIPLES,), 0, USERS)
    pos_ids = jax.random.randint(key_pos, (TRIPLES,), 0, ITEMS)
    neg_ids = jax.random.randint(key_neg, (TRIPLES,), 0, ITEMS)
    user_ids = jnp.where(row_pos == 0, USERS - 1, jnp.where(row_pos == 1, 0, user_ids))
    pos_ids = jnp.where(row_pos == 0, ITEMS - 1, jnp.where(row_pos == 1, 0, pos_ids))
    neg_ids = jnp.where(row_pos == 0, 0, jnp.where(row_pos == 1, ITEMS - 1, neg_ids))
    return jnp.stack([user_ids, pos_ids, neg_ids], axis=1).astype(jnp.int32)


def setup_inputs(seed: int = 0) -> dict:
    base_key = jax.random.key(seed)
    key_mask, key_user, key_item, key_trip = jax.random.split(base_key, 4)
    raw_draw = jax.random.randint(key_mask, (USERS, ITEMS), 0, ITEMS)
    inter_mask = (raw_draw < USER_DEGREE).astype(jnp.int32)
    emb_user = jax.random.normal(key_user, (USERS, DIM), jnp.float32).astype(jnp.bfloat16)
    emb_item = jax.random.normal(key_item, (ITEMS, DIM), jnp.float32).astype(jnp.bfloat16)
    return {"inter_mask": inter_mask, "emb_user": emb_user, "emb_item": emb_item, "triples": draw_triples(key_trip)}


def reference(inter_mask, emb_user, emb_item, triples):
    deg_user = jnp.maximum(jnp.sum(inter_mask, axis=1), 1)
    deg_item = jnp.maximum(jnp.sum(inter_mask, axis=0), 1)
    scale_user = lax.rsqrt(deg_user.astype(jnp.float32))
    scale_item = lax.rsqrt(deg_item.astype(jnp.float32))
    norm_adj = (inter_mask.astype(jnp.float32) * scale_user[:, None] * scale_item[None, :]).astype(jnp.bfloat16)
    layer_user = emb_user
    layer_item = emb_item
    total_user = emb_user.astype(jnp.float32)
    total_item = emb_item.astype(jnp.float32)
    for layer_idx in range(LAYERS):
        next_user = jnp.dot(norm_adj, layer_item, preferred_element_type=jnp.float32).astype(jnp.bfloat16)
        next_item = lax.dot_general(norm_adj, layer_user, (((0,), (0,)), ((), ())), preferred_element_type=jnp.float32).astype(jnp.bfloat16)
        total_user = total_user + next_user.astype(jnp.float32)
        total_item = total_item + next_item.astype(jnp.float32)
        layer_user = next_user
        layer_item = next_item
    out_user = (total_user / (LAYERS + 1)).astype(jnp.bfloat16)
    out_item = (total_item / (LAYERS + 1)).astype(jnp.bfloat16)
    user_vec = jnp.take(out_user, triples[:, 0], axis=0).astype(jnp.float32)
    pos_vec = jnp.take(out_item, triples[:, 1], axis=0).astype(jnp.float32)
    neg_vec = jnp.take(out_item, triples[:, 2], axis=0).astype(jnp.float32)
    margin = jnp.sum(user_vec * pos_vec, axis=1) - jnp.sum(user_vec * neg_vec, axis=1)
    bpr_loss = jnp.mean(jax.nn.softplus(-margin))
    return out_user, out_item, bpr_loss
```

```python
import functools

import jax
import jax.numpy as jnp
from jax import lax
from jax.experimental import pallas as pl
from jax.experimental.pallas import tpu as pltpu
from jax.sharding import PartitionSpec as P

MESH = pl.DeviceIdType.MESH
F32 = jnp.float32
BF16 = jnp.bfloat16
FEAT = 64
TRIPLES = 128
LAYERS = 3


def kernel(dims, mask, eu0, ei0, trip, out_user, out_item, loss, *scratch):
    Z, Y, X, SH, UD = dims
    C, R, Q = Z * Y, 2 * X, Y * X
    IB = R * SH
    HS = SH // 2
    (deg_s, deg_r, deg_f, own_deg, ideg, send_a, slab, slab_t, tbl0, tbl_j, acc, eu_j, eu_2, p_j, rd_j, s1_j, rxy_j, s2_j, rz_j,
     p_3, rd_3, s1_3, rxy_3, s2_3, rz_3, pk_z, pk_q, pk_d, xc, xr, sends, recvs, a2a_recv) = scratch
    row = lax.axis_index("row")
    col = lax.axis_index("col")
    core, x = row % 2, row // 2
    z, y = col // Y, col % Y
    q = y * X + x
    mate = x * 2 + (1 - core)

    def remote(src, dst, sem, r, c, recv=None):
        return pltpu.make_async_remote_copy(
            src_ref=src, dst_ref=dst, send_sem=sends.at[sem], recv_sem=recvs.at[sem] if recv is None else recv,
            device_id=(c, r), device_id_type=MESH)

    def await_recv(ref, sem):
        remote(ref, ref, sem, row, col).wait_recv()

    def await_send(ref, sem):
        remote(ref, ref, sem, row, col).wait_send()

    def q_to_rc(p):
        return (p % X) * 2 + core, z * Y + p // X

    barrier = pltpu.get_barrier_semaphore()

    def hail_col(k, _):
        pl.semaphore_signal(barrier, inc=1, device_id=((col + k) % C, row), device_id_type=MESH)
        return 0

    def hail_row(k, _):
        pl.semaphore_signal(barrier, inc=1, device_id=(col, (row + k) % R), device_id_type=MESH)
        return 0

    def hail_diag(k, _):
        ny = (y + 1 + k // (X - 1)) % Y
        nx = (x + 1 + k % (X - 1)) % X
        pl.semaphore_signal(barrier, inc=1, device_id=(z * Y + ny, nx * 2 + core), device_id_type=MESH)
        return 0

    lax.fori_loop(1, C, hail_col, 0)
    lax.fori_loop(1, R, hail_row, 0)
    lax.fori_loop(0, (X - 1) * (Y - 1), hail_diag, 0)

    ones = jnp.ones((8, IB), BF16)

    def count(k, part):
        blk = mask[k].astype(F32)
        sums = lax.dot_general(ones, blk.astype(BF16), (((1,), (1,)), ((), ())), preferred_element_type=F32)
        deg_s[k] = sums[0:1]
        return part + jnp.sum(blk.reshape(UD // 8, 8, IB), axis=0)

    part = lax.fori_loop(0, C, count, jnp.zeros((8, IB), F32))
    ideg[row] = jnp.sum(part, axis=0, keepdims=True)
    deg_r[col] = deg_s[col]
    tbl0[core, q, z] = ei0[...]
    pl.semaphore_wait(barrier, (C - 1) + (R - 1) + (X - 1) * (Y - 1))

    def send_deg(k, _):
        to = (col + k) % C
        remote(deg_s.at[to], deg_r.at[col], 0, row, to).start()
        return 0

    def send_ideg(k, _):
        remote(ideg.at[row], ideg.at[row], 1, (row + k) % R, col).start()
        return 0

    def gather_z(tbl, sem):
        def go(k, _):
            to = (z + k) % Z
            remote(tbl.at[core, q, z], tbl.at[core, q, z], sem, row, to * Y + y).start()
            return 0
        lax.fori_loop(1, Z, go, 0)

    def gather_q(tbl, sem):
        await_recv(tbl.at[core, q, pl.ds(0, Z - 1)], sem)

        def go(k, _):
            r, c = q_to_rc((q + k) % Q)
            remote(tbl.at[core, q], tbl.at[core, q], sem + 1, r, c).start()
            return 0
        lax.fori_loop(1, Q, go, 0)

    def gather_d(tbl, sem):
        await_recv(tbl.at[core, pl.ds(0, Q - 1)], sem + 1)
        remote(tbl.at[core], tbl.at[core], sem + 2, mate, col).start()

    def gather_end(tbl, sem):
        await_recv(tbl.at[core], sem + 2)
        await_send(tbl.at[core, q, pl.ds(0, Z - 1)], sem)
        await_send(tbl.at[core, pl.ds(0, Q - 1)], sem + 1)
        await_send(tbl.at[core], sem + 2)

    lax.fori_loop(1, C, send_deg, 0)
    lax.fori_loop(1, R, send_ideg, 0)
    gather_z(tbl0, 4)
    await_recv(deg_r.at[pl.ds(0, C - 1)], 0)

    own_deg[...] = lax.fori_loop(0, C, lambda k, t: t + deg_r[k], jnp.zeros((1, UD), F32))
    deg_f[col] = own_deg[...]

    def spread_deg(k, _):
        remote(own_deg, deg_f.at[col], 2, row, (col + k) % C).start()
        return 0

    lax.fori_loop(1, C, spread_deg, 0)
    await_recv(ideg.at[pl.ds(0, R - 1)], 1)
    scale_item = lax.rsqrt(jnp.maximum(lax.fori_loop(0, R, lambda k, t: t + ideg[k], jnp.zeros((1, IB), F32)), 1.0))
    gather_q(tbl0, 4)
    await_recv(deg_f.at[pl.ds(0, C - 1)], 2)

    def order(k):
        j, dy = k // Y, (k + 1) % Y
        m = Z // 2 - (j + 1) // 2
        odd = j % 2
        dz = (odd * m + (1 - odd) * (Z - m)) % Z
        return dz, dy

    def piece(c):
        scale = lax.rsqrt(jnp.maximum(deg_f[c], 1.0))
        scale = jnp.transpose(jnp.broadcast_to(scale, (IB, UD)))
        return (mask[c].astype(F32) * scale * scale_item).astype(BF16)

    def target(k):
        dz, dy = order(k)
        return ((z + dz) % Z) * Y + (y + dy) % Y

    def ship(k):
        to = target(k)
        remote(send_a.at[to], slab.at[col], 3, row, to, recv=a2a_recv.at[col]).start()

    send_a[target(0)] = piece(target(0))

    def make_and_ship(k, _):
        send_a[target(k)] = piece(target(k))
        ship(k - 1)
        return 0

    lax.fori_loop(1, C - 1, make_and_ship, 0)
    slab[col] = piece(col)
    ship(C - 2)
    gather_d(tbl0, 4)
    gather_end(tbl0, 4)

    def rows_of(tbl, c):
        cz, cy = c // Y, c % Y
        return jnp.concatenate([tbl[i % 2, cy * X + i // 2, cz] for i in range(R)], axis=0)

    def use(c):
        blk = slab[c]
        slab_t[c] = jnp.transpose(blk)
        acc[...] += jnp.dot(blk, rows_of(tbl0, c), preferred_element_type=F32)

    acc[...] = jnp.zeros_like(acc)
    use(col)

    def arrive(k, _):
        dz, dy = order(k)
        c = ((z - dz + Z) % Z) * Y + (y - dy + Y) % Y
        pltpu.make_async_remote_copy(src_ref=slab.at[c], dst_ref=slab.at[c], send_sem=sends.at[3], recv_sem=a2a_recv.at[c],
                                     device_id=(col, row), device_id_type=MESH).wait_recv()
        use(c)
        return 0

    lax.fori_loop(0, C - 1, arrive, 0)

    eu_j[...] = eu0[...] + acc[...].astype(BF16)

    def partial_j(c, _):
        cz, cy = c // Y, c % Y
        val = jnp.dot(slab_t[c], eu_j[...], preferred_element_type=F32)
        for i in range(R):
            p_j[i % 2, cy * X + i // 2, cz] = val[i * SH:(i + 1) * SH]
        return 0

    lax.fori_loop(0, C, partial_j, 0)

    def scatter_d(p, rd, sem):
        remote(p.at[1 - core], rd, sem, mate, col).start()

    def scatter_q(p, rd, s1, rxy, sem):
        await_recv(rd, sem)

        def fold(k):
            to = (q + k) % Q
            s1[to] = p[core, to] + rd[to]

        def go(k):
            to = (q + k) % Q
            r, c = q_to_rc(to)
            remote(s1.at[to], rxy.at[q], sem + 1, r, c).start()

        def both(k, _):
            fold(k)
            go(k - 1)
            return 0

        fold(1)
        lax.fori_loop(2, Q, both, 0)
        go(Q - 1)
        rxy[q] = p[core, q] + rd[q]

    def scatter_z(rxy, s2, rz, sem):
        await_recv(rxy.at[pl.ds(0, Q - 1)], sem + 1)

        def fold(to):
            return lax.fori_loop(1, Q, lambda k, t: t + rxy[k, to], rxy[0, to])

        def go(k):
            to = (z + k) % Z
            remote(s2.at[to], rz.at[z], sem + 2, row, to * Y + y).start()

        def both(k, _):
            to = (z + k) % Z
            s2[to] = fold(to)
            go(k - 1)
            return 0

        s2[(z + 1) % Z] = fold((z + 1) % Z)
        lax.fori_loop(2, Z, both, 0)
        go(Z - 1)
        rz[z] = fold(z)

    def scatter_end(p, s1, s2, rz, sem):
        await_recv(rz.at[pl.ds(0, Z - 1)], sem + 2)
        await_send(p.at[0], sem)
        await_send(s1.at[pl.ds(0, Q - 1)], sem + 1)
        await_send(s2.at[pl.ds(0, Z - 1)], sem + 2)
        return lax.fori_loop(1, Z, lambda k, t: t + rz[k], rz[0])

    scatter_d(p_j, rd_j, 7)
    scatter_q(p_j, rd_j, s1_j, rxy_j, 7)
    scatter_z(rxy_j, s2_j, rz_j, 7)
    mid_item = scatter_end(p_j, s1_j, s2_j, rz_j, 7).astype(BF16)

    tbl_j[core, q, z] = mid_item
    gather_z(tbl_j, 10)
    gather_q(tbl_j, 10)
    gather_d(tbl_j, 10)
    gather_end(tbl_j, 10)

    acc[...] = jnp.zeros_like(acc)

    def absorb(c, _):
        acc[...] += jnp.dot(slab[c], rows_of(tbl_j, c), preferred_element_type=F32)
        return 0

    lax.fori_loop(0, C, absorb, 0)

    def swap(v):
        return pltpu.roll(v, FEAT, 1)

    late_user = acc[...].astype(BF16).astype(F32)
    early_user = eu_j[...].astype(F32)
    sum_user = ((early_user + swap(early_user)) + late_user) + swap(late_user)
    user_rows = (sum_user / (LAYERS + 1)).astype(BF16)
    out_user[...] = user_rows[:, :FEAT]
    left = lax.broadcasted_iota(jnp.int32, late_user.shape, 1) < FEAT
    eu_2[...] = jnp.where(left, late_user, swap(late_user)).astype(BF16)

    ids = lax.broadcasted_iota(jnp.int32, (UD, TRIPLES), 0) + (row * C + col) * UD
    hit = (ids == trip[0:1, :]).astype(BF16)
    pk_z[z] = lax.dot_general(user_rows, hit, (((0,), (0,)), ((), ())), preferred_element_type=F32)[:FEAT].astype(BF16)

    def pick_z(k, _):
        remote(pk_z.at[z], pk_z.at[z], 16, row, ((z + k) % Z) * Y + y).start()
        return 0

    def pick_q(k, _):
        r, c = q_to_rc((q + k) % Q)
        remote(pk_q.at[q], pk_q.at[q], 17, r, c).start()
        return 0

    lax.fori_loop(1, Z, pick_z, 0)

    lane_left = lax.broadcasted_iota(jnp.int32, (HS, 2 * FEAT), 1) < FEAT

    def partial_3(c, _):
        cz, cy = c // Y, c % Y
        val = jnp.dot(slab_t[c], eu_2[...], preferred_element_type=F32)
        for i in range(R):
            p_3[i % 2, cy * X + i // 2, cz] = jnp.where(lane_left, val[i * SH:i * SH + HS], val[i * SH + HS:(i + 1) * SH])
        return 0

    lax.fori_loop(0, C, partial_3, 0)
    scatter_d(p_3, rd_3, 13)
    scatter_q(p_3, rd_3, s1_3, rxy_3, 13)
    await_recv(pk_z.at[pl.ds(0, Z - 1)], 16)
    pk_q[q] = lax.fori_loop(1, Z, lambda k, t: t + pk_z[k].astype(F32), pk_z[0].astype(F32)).astype(BF16)
    lax.fori_loop(1, Q, pick_q, 0)
    scatter_z(rxy_3, s2_3, rz_3, 13)
    await_recv(pk_q.at[pl.ds(0, Q - 1)], 17)
    pk_d[core] = lax.fori_loop(1, Q, lambda k, t: t + pk_q[k].astype(F32), pk_q[0].astype(F32)).astype(BF16)
    remote(pk_d.at[core], pk_d.at[core], 18, mate, col).start()
    last = scatter_end(p_3, s1_3, s2_3, rz_3, 13).astype(BF16).astype(F32)
    last_item = jnp.concatenate([last, swap(last)], axis=0)
    early_item = ei0[...].astype(F32)
    mid = mid_item.astype(F32)
    item_rows = (((swap(early_item) + mid) + swap(mid)) + last_item) / (LAYERS + 1)
    item_rows = item_rows.astype(BF16)[:, :FEAT]
    out_item[...] = item_rows

    await_recv(pk_d.at[0], 18)
    user_vec = (pk_d[0].astype(F32) + pk_d[1].astype(F32)).astype(BF16)
    dots = jnp.dot(item_rows, user_vec, preferred_element_type=F32)
    own = lax.broadcasted_iota(jnp.int32, (SH, TRIPLES), 0) + (col * R + row) * SH
    pos = jnp.sum(jnp.where(own == trip[1:2, :], dots, 0.0), axis=0, keepdims=True)
    neg = jnp.sum(jnp.where(own == trip[2:3, :], dots, 0.0), axis=0, keepdims=True)
    xc[col] = pos - neg

    def margin_col(k, _):
        remote(xc.at[col], xc.at[col], 19, row, (col + k) % C).start()
        return 0

    def margin_row(k, _):
        remote(xr.at[row], xr.at[row], 20, (row + k) % R, col).start()
        return 0

    lax.fori_loop(1, C, margin_col, 0)
    await_recv(xc.at[pl.ds(0, C - 1)], 19)
    xr[row] = lax.fori_loop(1, C, lambda k, t: t + xc[k], xc[0])
    lax.fori_loop(1, R, margin_row, 0)
    await_recv(xr.at[pl.ds(0, R - 1)], 20)
    margin = lax.fori_loop(1, R, lambda k, t: t + xr[k], xr[0])
    soft = jnp.maximum(-margin, 0.0) + jnp.log1p(jnp.exp(-jnp.abs(margin)))
    loss[...] = jnp.sum(soft, axis=1, keepdims=True) / TRIPLES

    await_send(deg_s.at[pl.ds(0, C - 1)], 0)
    await_send(ideg.at[pl.ds(0, R - 1)], 1)
    await_send(deg_f.at[pl.ds(0, C - 1)], 2)
    await_send(send_a.at[pl.ds(0, C - 1)], 3)
    await_send(pk_z.at[pl.ds(0, Z - 1)], 16)
    await_send(pk_q.at[pl.ds(0, Q - 1)], 17)
    await_send(pk_d.at[0], 18)
    await_send(xc.at[pl.ds(0, C - 1)], 19)
    await_send(xr.at[pl.ds(0, R - 1)], 20)


def build(mesh, Y, SH, UD):
    C, R = mesh.shape["col"], mesh.shape["row"]
    Z, X = C // Y, R // 2
    Q, IB, W = Y * X, R * SH, 2 * FEAT
    HS = SH // 2
    vm = pltpu.VMEM
    scratch = [
        vm((C, 1, UD), F32), vm((C, 1, UD), F32), vm((C, 1, UD), F32), vm((1, UD), F32), vm((R, 1, IB), F32),
        vm((C, UD, IB), BF16), vm((C, UD, IB), BF16), vm((C, IB, UD), BF16),
        vm((2, Q, Z, SH, W), BF16), vm((2, Q, Z, SH, W), BF16),
        vm((UD, W), F32), vm((UD, W), BF16), vm((UD, W), BF16),
        vm((2, Q, Z, SH, W), F32), vm((Q, Z, SH, W), F32), vm((Q, Z, SH, W), F32), vm((Q, Z, SH, W), F32),
        vm((Z, SH, W), F32), vm((Z, SH, W), F32),
        vm((2, Q, Z, HS, W), F32), vm((Q, Z, HS, W), F32), vm((Q, Z, HS, W), F32), vm((Q, Z, HS, W), F32),
        vm((Z, HS, W), F32), vm((Z, HS, W), F32),
        vm((Z, FEAT, TRIPLES), BF16), vm((Q, FEAT, TRIPLES), BF16), vm((2, FEAT, TRIPLES), BF16),
        vm((C, 1, TRIPLES), F32), vm((R, 1, TRIPLES), F32),
        pltpu.SemaphoreType.DMA((21,)), pltpu.SemaphoreType.DMA((21,)), pltpu.SemaphoreType.DMA((C,)),
    ]
    dims = (Z, Y, X, SH, UD)

    def local_prog(mask_blk, user_shard, item_shard, triples):
        out_user, out_item, loss = pl.pallas_call(
            functools.partial(kernel, dims),
            out_shape=(
                jax.ShapeDtypeStruct((UD, FEAT), BF16),
                jax.ShapeDtypeStruct((SH, FEAT), BF16),
                jax.ShapeDtypeStruct((1, 1), F32),
            ),
            in_specs=[pl.BlockSpec(memory_space=pltpu.VMEM)] * 4,
            out_specs=(pl.BlockSpec(memory_space=pltpu.VMEM),) * 3,
            scratch_shapes=scratch,
            compiler_params=pltpu.CompilerParams(
                collective_id=0, has_side_effects=True, vmem_limit_bytes=60 * 1024 * 1024),
            name="lightgcn",
        )(
            mask_blk.reshape(C, UD, IB),
            jnp.pad(user_shard, ((0, 0), (0, FEAT))),
            jnp.pad(item_shard, ((0, 0), (FEAT, 0))),
            triples.T,
        )
        return out_user, out_item, loss[0, 0]

    return jax.shard_map(
        local_prog, mesh=mesh,
        in_specs=(P("row", "col"), P(("row", "col"), None), P(("col", "row"), None), P(None, None)),
        out_specs=(P(("row", "col"), None), P(("col", "row"), None), P()), check_vma=False)


def solution(mesh):
    return build(mesh, Y=4, SH=16, UD=256)
```

```python
import functools

import jax
import jax.numpy as jnp
from jax import lax
from jax.experimental import pallas as pl
from jax.experimental.pallas import tpu as pltpu
from jax.sharding import PartitionSpec as P

MESH = pl.DeviceIdType.MESH
F32 = jnp.float32
BF16 = jnp.bfloat16
FEAT = 64
WIDE = 2 * FEAT
TRIPLES = 128
LAYERS = 3

DEG, IDEG, SPREAD, ATOA, GATHER0, GATHER1, GATHER2, PICK, MARGIN, SCATTER1 = 0, 1, 2, 3, 4, 7, 10, 13, 16, 18


def swap(v):
    return pltpu.roll(v, FEAT, 1)


def kernel(dims, mask, eu0, ei0, trip, out_user, out_item, loss, *scratch):
    Z, Y, X, SH, UD, G2 = dims
    C, R, Q = Z * Y, 2 * X, Y * X
    IB = R * SH
    HS = SH // 2
    (deg_s, deg_r, deg_f, own_deg, ideg, send_a, slab, slab_t, tbl0, tbl1, tbl2, acc, ed0, ed1, ed2, pk_z, pk_q, pk_d, xc, xr,
     sends, recvs, a2a_recv) = scratch[:23]
    groups = (Z, G2, G2)
    rs = [scratch[23 + 6 * n:29 + 6 * n] for n in range(3)]
    base = [SCATTER1]
    for n in range(3):
        base.append(base[-1] + 2 * groups[n] + 1)
    row = lax.axis_index("row")
    col = lax.axis_index("col")
    core, x = row % 2, row // 2
    z, y = col // Y, col % Y
    q = y * X + x
    mate = x * 2 + (1 - core)

    def remote(src, dst, sem, r, c, recv=None):
        return pltpu.make_async_remote_copy(
            src_ref=src, dst_ref=dst, send_sem=sends.at[sem], recv_sem=recvs.at[sem] if recv is None else recv,
            device_id=(c, r), device_id_type=MESH)

    def await_recv(ref, sem):
        remote(ref, ref, sem, row, col).wait_recv()

    def await_send(ref, sem):
        remote(ref, ref, sem, row, col).wait_send()

    def at_q(p):
        return (p % X) * 2 + core, z * Y + p // X

    def each(lo, hi, fn):
        lax.fori_loop(lo, hi, lambda k, t: (fn(k), t)[1], 0)

    barrier = pltpu.get_barrier_semaphore()

    def hail(c, r):
        pl.semaphore_signal(barrier, inc=1, device_id=(c, r), device_id_type=MESH)

    each(1, C, lambda k: hail((col + k) % C, row))
    each(1, R, lambda k: hail(col, (row + k) % R))
    each(0, (X - 1) * (Y - 1), lambda k: hail(z * Y + (y + 1 + k // (X - 1)) % Y, ((x + 1 + k % (X - 1)) % X) * 2 + core))

    ones = jnp.ones((8, IB), BF16)

    def count(k, part):
        blk = mask[k].astype(F32)
        sums = lax.dot_general(ones, blk.astype(BF16), (((1,), (1,)), ((), ())), preferred_element_type=F32)
        deg_s[k] = sums[0:1]
        return part + jnp.sum(blk.reshape(UD // 8, 8, IB), axis=0)

    part = lax.fori_loop(0, C, count, jnp.zeros((8, IB), F32), unroll=4)
    ideg[row] = jnp.sum(part, axis=0, keepdims=True)
    deg_r[col] = deg_s[col]

    lane_left = lax.broadcasted_iota(jnp.int32, (HS, WIDE), 1) < FEAT

    def pack(v):
        return jnp.where(lane_left, v[:HS], swap(v[HS:]))

    e0 = ei0[...].astype(F32)
    item0 = pack(jnp.concatenate([e0, jnp.zeros_like(e0)], axis=1))
    tbl0[core, q, z] = item0.astype(BF16)
    user0 = eu0[...].astype(F32)
    ed0[...] = jnp.transpose(jnp.concatenate([user0, user0], axis=0)).astype(BF16)
    pl.semaphore_wait(barrier, (C - 1) + (R - 1) + (X - 1) * (Y - 1))

    def gather_z(tbl, sem):
        each(1, Z, lambda k: remote(tbl.at[core, q, z], tbl.at[core, q, z], sem, row, ((z + k) % Z) * Y + y).start())

    def gather_q(tbl, sem):
        await_recv(tbl.at[core, q, pl.ds(0, Z - 1)], sem)
        each(1, Q, lambda k: remote(tbl.at[core, q], tbl.at[core, q], sem + 1, *at_q((q + k) % Q)).start())

    def gather_d(tbl, sem):
        await_recv(tbl.at[core, pl.ds(0, Q - 1)], sem + 1)
        remote(tbl.at[core], tbl.at[core], sem + 2, mate, col).start()

    def gather_end(tbl, sem):
        await_recv(tbl.at[core], sem + 2)

    def gather_sent(tbl, sem):
        await_send(tbl.at[core, q, pl.ds(0, Z - 1)], sem)
        await_send(tbl.at[core, pl.ds(0, Q - 1)], sem + 1)
        await_send(tbl.at[core], sem + 2)

    def rows_of(tbl, c):
        cz, cy = c // Y, c % Y
        parts = []
        for i in range(R):
            v = tbl[i % 2, cy * X + i // 2, cz].astype(F32)
            parts += [v, swap(v)]
        return jnp.concatenate(parts, axis=0).astype(BF16)

    each(1, C, lambda k: remote(deg_s.at[(col + k) % C], deg_r.at[col], DEG, row, (col + k) % C).start())
    each(1, R, lambda k: remote(ideg.at[row], ideg.at[row], IDEG, (row + k) % R, col).start())
    gather_z(tbl0, GATHER0)
    await_recv(deg_r.at[pl.ds(0, C - 1)], DEG)
    own_deg[...] = lax.fori_loop(0, C, lambda k, t: t + deg_r[k], jnp.zeros((1, UD), F32), unroll=True)
    deg_f[col] = own_deg[...]
    each(1, C, lambda k: remote(own_deg, deg_f.at[col], SPREAD, row, (col + k) % C).start())
    await_recv(ideg.at[pl.ds(0, R - 1)], IDEG)
    scale_item = lax.rsqrt(jnp.maximum(lax.fori_loop(0, R, lambda k, t: t + ideg[k], jnp.zeros((1, IB), F32), unroll=True), 1.0))
    gather_q(tbl0, GATHER0)
    await_recv(deg_f.at[pl.ds(0, C - 1)], SPREAD)

    def order(k):
        j, dy = k // Y, (k + 1) % Y
        m = Z // 2 - (j + 1) // 2
        odd = j % 2
        return (odd * m + (1 - odd) * (Z - m)) % Z, dy

    def piece(c):
        scale = lax.rsqrt(jnp.maximum(deg_f[c], 1.0))
        scale = jnp.transpose(jnp.broadcast_to(scale, (IB, UD)))
        return (mask[c].astype(F32) * scale * scale_item).astype(BF16)

    def target(k):
        dz, dy = order(k)
        return ((z + dz) % Z) * Y + (y + dy) % Y

    def ship(k):
        to = target(k)
        remote(send_a.at[to], slab.at[col], ATOA, row, to, recv=a2a_recv.at[col]).start()

    send_a[target(0)] = piece(target(0))

    def make_and_ship(k):
        send_a[target(k)] = piece(target(k))
        ship(k - 1)

    each(1, C - 1, make_and_ship)
    slab[col] = piece(col)
    ship(C - 2)
    gather_d(tbl0, GATHER0)
    gather_end(tbl0, GATHER0)

    def scatter_a(n, g, ed):
        p, rd = rs[n][0], rs[n][1]
        per = Z // groups[n]

        def block(k):
            zi, cy = k // Y, k % Y
            val = jnp.dot(slab_t[(g * per + zi) * Y + cy], ed[...], preferred_element_type=F32)
            for i in range(R):
                p[i % 2, g, cy * X + i // 2, zi] = jnp.where(lane_left, val[i * SH:i * SH + HS], val[i * SH + HS:(i + 1) * SH])

        lax.fori_loop(0, per * Y, lambda k, t: (block(k), t)[1], 0, unroll=4)
        remote(p.at[1 - core, g], rd.at[g], base[n], mate, col, recv=recvs.at[base[n] + g]).start()

    def scatter_b(n, g):
        p, rd, s1, rxy, _, _ = rs[n]
        remote(rd.at[g], rd.at[g], base[n], row, col, recv=recvs.at[base[n] + g]).wait_recv()

        def fold(k):
            to = (q + k) % Q
            s1[g, to] = p[core, g, to] + rd[g, to]

        def go(k):
            to = (q + k) % Q
            remote(s1.at[g, to], rxy.at[g, q], base[n] + 1, *at_q(to), recv=recvs.at[base[n] + groups[n] + g]).start()

        def both(k):
            fold(k)
            go(k - 1)

        fold(1)
        each(2, Q, both)
        rxy[g, q] = p[core, g, q] + rd[g, q]
        go(Q - 1)

    def scatter_c(n, g):
        _, _, _, rxy, s2, rz = rs[n]
        per = Z // groups[n]
        part = rxy.at[g, pl.ds(0, Q - 1)]
        remote(part, part, base[n], row, col, recv=recvs.at[base[n] + groups[n] + g]).wait_recv()
        for zi in range(per):
            to = g * per + zi
            s2[to] = lax.fori_loop(1, Q, lambda k, t: t + rxy[g, k, zi], rxy[g, 0, zi], unroll=True)
        for zi in range(per):
            to = g * per + zi

            @pl.when(to != z)
            def _():
                remote(s2.at[to], rz.at[z], base[n] + 2, row, to * Y + y, recv=recvs.at[base[n] + 2 * groups[n]]).start()

            @pl.when(to == z)
            def _():
                rz[z] = s2[to]

    def scatter_end(n):
        rz = rs[n][5]
        part = rz.at[pl.ds(0, Z - 1)]
        remote(part, part, base[n], row, col, recv=recvs.at[base[n] + 2 * groups[n]]).wait_recv()
        return lax.fori_loop(1, Z, lambda k, t: t + rz[k], rz[0], unroll=True).astype(BF16)

    def scatter_sent(n):
        p, _, s1, _, s2, _ = rs[n]
        await_send(p.at[0], base[n])
        await_send(s1.at[:, pl.ds(0, Q - 1)], base[n] + 1)
        await_send(s2.at[pl.ds(0, Z - 1)], base[n] + 2)

    def source(k):
        dz, dy = order(k)
        return ((z - dz + Z) % Z) * Y + (y - dy + Y) % Y

    def use(c):
        blk = slab[c]
        slab_t[c] = jnp.transpose(blk)
        acc[...] += jnp.dot(blk, rows_of(tbl0, c), preferred_element_type=F32)

    def arrive(k):
        c = source(k)
        pltpu.make_async_remote_copy(src_ref=slab.at[c], dst_ref=slab.at[c], send_sem=sends.at[ATOA], recv_sem=a2a_recv.at[c],
                                     device_id=(col, row), device_id_type=MESH).wait_recv()
        use(c)

    def group(j):
        return source(j * Y) // Y

    acc[...] = jnp.zeros_like(acc)
    use(col)

    def stream(j):
        each(j * Y, (j + 1) * Y, arrive)
        scatter_a(0, group(j), ed0)

        @pl.when(j >= 1)
        def _():
            scatter_b(0, group(j - 1))

        @pl.when(j >= 2)
        def _():
            scatter_c(0, group(j - 2))

    each(0, Z - 1, stream)
    each((Z - 1) * Y, C - 1, arrive)
    scatter_a(0, z, ed0)
    wide_left = lax.broadcasted_iota(jnp.int32, (UD, WIDE), 1) < FEAT

    def twice(v):
        return jnp.where(wide_left, v, swap(v)).astype(BF16)

    user1 = acc[...].astype(BF16).astype(F32)
    ed1[...] = twice(user1)
    for g in range(G2):
        scatter_a(1, g, ed1)
        if g == 0:
            scatter_b(0, group(Z - 2))
            scatter_b(0, z)
    if Z > 2:
        scatter_c(0, group(Z - 3))
    scatter_c(0, group(Z - 2))
    for g in range(G2):
        scatter_b(1, g)
    scatter_c(0, z)
    item1 = scatter_end(0)
    tbl1[core, q, z] = item1
    gather_z(tbl1, GATHER1)
    for g in range(G2):
        scatter_c(1, g)
        if g == G2 // 2 - 1:
            gather_q(tbl1, GATHER1)
    item2 = scatter_end(1)
    tbl2[core, q, z] = item2
    gather_z(tbl2, GATHER2)
    gather_d(tbl1, GATHER1)
    gather_q(tbl2, GATHER2)
    gather_end(tbl1, GATHER1)

    def absorb(tbl):
        acc[...] = jnp.zeros_like(acc)

        def step(c):
            acc[...] += jnp.dot(slab[c], rows_of(tbl, c), preferred_element_type=F32)

        lax.fori_loop(0, C, lambda k, t: (step(k), t)[1], 0, unroll=4)
        return acc[...].astype(BF16).astype(F32)

    user2 = absorb(tbl1)
    ed2[...] = twice(user2)
    for g in range(G2):
        scatter_a(2, g, ed2)
        if g > 0:
            scatter_b(2, g - 1)
    scatter_b(2, G2 - 1)
    gather_d(tbl2, GATHER2)
    gather_end(tbl2, GATHER2)
    user3 = absorb(tbl2)
    sum_user = ((ed0[...].astype(F32) + ed1[...].astype(F32)) + ed2[...].astype(F32)) + user3
    user_rows = (sum_user / (LAYERS + 1)).astype(BF16)

    ids = lax.broadcasted_iota(jnp.int32, (UD, TRIPLES), 0) + (row * C + col) * UD
    hit = (ids == trip[0:1, :]).astype(BF16)
    pk_z[z] = lax.dot_general(user_rows, hit, (((0,), (0,)), ((), ())), preferred_element_type=F32)[:FEAT].astype(BF16)
    each(1, Z, lambda k: remote(pk_z.at[z], pk_z.at[z], PICK, row, ((z + k) % Z) * Y + y).start())
    out_user[...] = jnp.transpose(user_rows.astype(F32))[:FEAT].astype(BF16)

    for g in range(G2):
        scatter_c(2, g)
    await_recv(pk_z.at[pl.ds(0, Z - 1)], PICK)
    pk_q[q] = lax.fori_loop(1, Z, lambda k, t: t + pk_z[k].astype(F32), pk_z[0].astype(F32)).astype(BF16)
    each(1, Q, lambda k: remote(pk_q.at[q], pk_q.at[q], PICK + 1, *at_q((q + k) % Q)).start())
    item3 = scatter_end(2)
    sum_item = ((item0 + item1.astype(F32)) + item2.astype(F32)) + item3.astype(F32)
    packed = (sum_item / (LAYERS + 1)).astype(BF16).astype(F32)
    item_rows = jnp.concatenate([packed, swap(packed)], axis=0).astype(BF16)[:, :FEAT]
    out_item[...] = item_rows

    await_recv(pk_q.at[pl.ds(0, Q - 1)], PICK + 1)
    pk_d[core] = lax.fori_loop(1, Q, lambda k, t: t + pk_q[k].astype(F32), pk_q[0].astype(F32)).astype(BF16)
    remote(pk_d.at[core], pk_d.at[core], PICK + 2, mate, col).start()
    await_recv(pk_d.at[0], PICK + 2)
    user_vec = (pk_d[0].astype(F32) + pk_d[1].astype(F32)).astype(BF16)
    dots = jnp.dot(item_rows, user_vec, preferred_element_type=F32)
    own = lax.broadcasted_iota(jnp.int32, (SH, TRIPLES), 0) + (col * R + row) * SH
    pos = jnp.sum(jnp.where(own == trip[1:2, :], dots, 0.0), axis=0, keepdims=True)
    neg = jnp.sum(jnp.where(own == trip[2:3, :], dots, 0.0), axis=0, keepdims=True)
    xc[col] = pos - neg
    each(1, C, lambda k: remote(xc.at[col], xc.at[col], MARGIN, row, (col + k) % C).start())
    await_recv(xc.at[pl.ds(0, C - 1)], MARGIN)
    xr[row] = lax.fori_loop(1, C, lambda k, t: t + xc[k], xc[0], unroll=True)
    each(1, R, lambda k: remote(xr.at[row], xr.at[row], MARGIN + 1, (row + k) % R, col).start())
    await_recv(xr.at[pl.ds(0, R - 1)], MARGIN + 1)
    margin = lax.fori_loop(1, R, lambda k, t: t + xr[k], xr[0], unroll=True)
    soft = jnp.maximum(-margin, 0.0) + jnp.log1p(jnp.exp(-jnp.abs(margin)))
    loss[...] = jnp.sum(soft, axis=1, keepdims=True) / TRIPLES

    await_send(deg_s.at[pl.ds(0, C - 1)], DEG)
    await_send(ideg.at[pl.ds(0, R - 1)], IDEG)
    await_send(deg_f.at[pl.ds(0, C - 1)], SPREAD)
    await_send(send_a.at[pl.ds(0, C - 1)], ATOA)
    gather_sent(tbl0, GATHER0)
    gather_sent(tbl1, GATHER1)
    gather_sent(tbl2, GATHER2)
    for n in range(3):
        scatter_sent(n)
    await_send(pk_z.at[pl.ds(0, Z - 1)], PICK)
    await_send(pk_q.at[pl.ds(0, Q - 1)], PICK + 1)
    await_send(pk_d.at[0], PICK + 2)
    await_send(xc.at[pl.ds(0, C - 1)], MARGIN)
    await_send(xr.at[pl.ds(0, R - 1)], MARGIN + 1)


def build(mesh, Y, SH, UD, G2):
    C, R = mesh.shape["col"], mesh.shape["row"]
    Z, X = C // Y, R // 2
    Q, IB, HS = Y * X, R * SH, SH // 2
    vm = pltpu.VMEM
    scratch = [
        vm((C, 1, UD), F32), vm((C, 1, UD), F32), vm((C, 1, UD), F32), vm((1, UD), F32), vm((R, 1, IB), F32),
        vm((C, UD, IB), BF16), vm((C, UD, IB), BF16), vm((C, IB, UD), BF16),
        vm((2, Q, Z, HS, WIDE), BF16), vm((2, Q, Z, HS, WIDE), BF16), vm((2, Q, Z, HS, WIDE), BF16),
        vm((UD, WIDE), F32), vm((UD, WIDE), BF16), vm((UD, WIDE), BF16), vm((UD, WIDE), BF16),
        vm((Z, FEAT, TRIPLES), BF16), vm((Q, FEAT, TRIPLES), BF16), vm((2, FEAT, TRIPLES), BF16),
        vm((C, 1, TRIPLES), F32), vm((R, 1, TRIPLES), F32),
    ]
    count = SCATTER1 + sum(2 * g + 1 for g in (Z, G2, G2)) + 1
    scratch += [pltpu.SemaphoreType.DMA((count,)), pltpu.SemaphoreType.DMA((count,)), pltpu.SemaphoreType.DMA((C,))]
    for g in (Z, G2, G2):
        scratch += [vm((2, g, Q, Z // g, HS, WIDE), F32)] + [vm((g, Q, Z // g, HS, WIDE), F32)] * 3 + [vm((Z, HS, WIDE), F32)] * 2
    dims = (Z, Y, X, SH, UD, G2)

    def local_prog(mask_blk, user_shard, item_shard, triples):
        out_user, out_item, loss = pl.pallas_call(
            functools.partial(kernel, dims),
            out_shape=(
                jax.ShapeDtypeStruct((FEAT, UD), BF16),
                jax.ShapeDtypeStruct((SH, FEAT), BF16),
                jax.ShapeDtypeStruct((1, 1), F32),
            ),
            in_specs=[pl.BlockSpec(memory_space=pltpu.VMEM)] * 4,
            out_specs=(pl.BlockSpec(memory_space=pltpu.VMEM),) * 3,
            scratch_shapes=scratch,
            compiler_params=pltpu.CompilerParams(
                collective_id=0, has_side_effects=True, vmem_limit_bytes=60 * 1024 * 1024),
            name="lightgcn",
        )(mask_blk.reshape(C, UD, IB), user_shard.T, item_shard, triples.T)
        return out_user.T, out_item, loss[0, 0]

    return jax.shard_map(
        local_prog, mesh=mesh,
        in_specs=(P("row", "col"), P(("row", "col"), None), P(("col", "row"), None), P(None, None)),
        out_specs=(P(("row", "col"), None), P(("col", "row"), None), P()), check_vma=False)


def solution(mesh):
    return build(mesh, Y=4, SH=16, UD=256, G2=4)
```

```python
import functools

import jax
import jax.numpy as jnp
from jax import lax
from jax.experimental import pallas as pl
from jax.experimental.pallas import tpu as pltpu
from jax.sharding import PartitionSpec as P

MESH = pl.DeviceIdType.MESH
F32 = jnp.float32
BF16 = jnp.bfloat16
FEAT = 64
WIDE = 2 * FEAT
TRIPLES = 128
LAYERS = 3
LOADS = 8
PICKS = TRIPLES // 4

DEG, IDEG, SPREAD, ATOA, GATHER0, GATHER1, PICK, MARGIN, SCATTER1 = 0, 1, 2, 3, 4, 7, 10, 14, 16


def swap(v):
    return pltpu.roll(v, FEAT, 1)


def kernel(dims, mask_hbm, eu0, ei0, trip, out_user, out_item, loss, *scratch):
    Z, Y, X, SH, UD, G2 = dims
    C, R, Q = Z * Y, 2 * X, Y * X
    IB = R * SH
    HS = SH // 2
    (deg_s, deg_r, deg_f, own_deg, ideg, send_a, slab, slab_t, tbl0, tbl1, acc, ed0, ed1, ed2, pk_a, pk_b, pk_z, pk_q, pk_d, xc, xr,
     sends, recvs, a2a_recv, mask, load_sem) = scratch[:26]
    groups = (Z, G2, G2)
    rs = [scratch[26 + 6 * n:32 + 6 * n] for n in range(3)]
    base = [SCATTER1]
    for n in range(3):
        base.append(base[-1] + 2 * groups[n] + 1)
    row = lax.axis_index("row")
    col = lax.axis_index("col")
    core, x = row % 2, row // 2
    z, y = col // Y, col % Y
    q = y * X + x
    mate = x * 2 + (1 - core)

    def remote(src, dst, sem, r, c, recv=None):
        return pltpu.make_async_remote_copy(
            src_ref=src, dst_ref=dst, send_sem=sends.at[sem], recv_sem=recvs.at[sem] if recv is None else recv,
            device_id=(c, r), device_id_type=MESH)

    def await_recv(ref, sem):
        remote(ref, ref, sem, row, col).wait_recv()

    def await_send(ref, sem):
        remote(ref, ref, sem, row, col).wait_send()

    def at_q(p):
        return (p % X) * 2 + core, z * Y + p // X

    def each(lo, hi, fn):
        lax.fori_loop(lo, hi, lambda k, t: (fn(k), t)[1], 0)

    run = C // LOADS

    def load(i):
        part = pl.ds(i * run, run)
        return pltpu.make_async_copy(mask_hbm.at[part], mask.at[part], load_sem.at[i])

    for i in range(LOADS):
        load(i).start()

    barrier = pltpu.get_barrier_semaphore()

    def hail(c, r):
        pl.semaphore_signal(barrier, inc=1, device_id=(c, r), device_id_type=MESH)

    each(1, C, lambda k: hail((col + k) % C, row))
    each(1, R, lambda k: hail(col, (row + k) % R))
    each(0, (X - 1) * (Y - 1), lambda k: hail(z * Y + (y + 1 + k // (X - 1)) % Y, ((x + 1 + k % (X - 1)) % X) * 2 + core))

    ones = jnp.ones((8, IB), BF16)

    def count(k, part):
        blk = mask[k].astype(F32)
        sums = lax.dot_general(ones, blk.astype(BF16), (((1,), (1,)), ((), ())), preferred_element_type=F32)
        deg_s[k] = sums[0:1]
        return part + jnp.sum(blk.reshape(UD // 8, 8, IB), axis=0)

    part = jnp.zeros((8, IB), F32)
    for i in range(LOADS):
        load(i).wait()
        part = lax.fori_loop(i * run, (i + 1) * run, count, part, unroll=True)
    ideg[row] = jnp.sum(part, axis=0, keepdims=True)
    deg_r[col] = deg_s[col]

    lane_left = lax.broadcasted_iota(jnp.int32, (HS, WIDE), 1) < FEAT

    def pack(v):
        return jnp.where(lane_left, v[:HS], swap(v[HS:]))

    e0 = ei0[...].astype(F32)
    item0 = pack(jnp.concatenate([e0, jnp.zeros_like(e0)], axis=1))
    tbl0[core, q, z] = item0.astype(BF16)
    user0 = eu0[...].astype(F32)
    ed0[...] = jnp.transpose(jnp.concatenate([user0, user0], axis=0)).astype(BF16)
    pl.semaphore_wait(barrier, (C - 1) + (R - 1) + (X - 1) * (Y - 1))

    def gather_z(tbl, sem):
        each(1, Z, lambda k: remote(tbl.at[core, q, z], tbl.at[core, q, z], sem, row, ((z + k) % Z) * Y + y).start())

    def gather_q(tbl, sem):
        await_recv(tbl.at[core, q, pl.ds(0, Z - 1)], sem)
        each(1, Q, lambda k: remote(tbl.at[core, q], tbl.at[core, q], sem + 1, *at_q((q + k) % Q)).start())

    def gather_d(tbl, sem):
        await_recv(tbl.at[core, pl.ds(0, Q - 1)], sem + 1)
        remote(tbl.at[core], tbl.at[core], sem + 2, mate, col).start()

    def gather_end(tbl, sem):
        await_recv(tbl.at[core], sem + 2)

    def gather_sent(tbl, sem):
        await_send(tbl.at[core, q, pl.ds(0, Z - 1)], sem)
        await_send(tbl.at[core, pl.ds(0, Q - 1)], sem + 1)
        await_send(tbl.at[core], sem + 2)

    def rows_of(tbl, c):
        cz, cy = c // Y, c % Y
        parts = []
        for i in range(R):
            v = tbl[i % 2, cy * X + i // 2, cz].astype(F32)
            parts += [v, swap(v)]
        return jnp.concatenate(parts, axis=0).astype(BF16)

    each(1, C, lambda k: remote(deg_s.at[(col + k) % C], deg_r.at[col], DEG, row, (col + k) % C).start())
    each(1, R, lambda k: remote(ideg.at[row], ideg.at[row], IDEG, (row + k) % R, col).start())
    gather_z(tbl0, GATHER0)
    await_recv(deg_r.at[pl.ds(0, C - 1)], DEG)
    own_deg[...] = lax.fori_loop(0, C, lambda k, t: t + deg_r[k], jnp.zeros((1, UD), F32), unroll=True)
    deg_f[col] = own_deg[...]
    each(1, C, lambda k: remote(own_deg, deg_f.at[col], SPREAD, row, (col + k) % C).start())
    await_recv(ideg.at[pl.ds(0, R - 1)], IDEG)
    scale_item = lax.rsqrt(jnp.maximum(lax.fori_loop(0, R, lambda k, t: t + ideg[k], jnp.zeros((1, IB), F32), unroll=True), 1.0))
    gather_q(tbl0, GATHER0)
    await_recv(deg_f.at[pl.ds(0, C - 1)], SPREAD)

    def order(k):
        j, dy = k // Y, (k + 1) % Y
        m = Z // 2 - (j + 1) // 2
        odd = j % 2
        return (odd * m + (1 - odd) * (Z - m)) % Z, dy

    def piece(c):
        scale = lax.rsqrt(jnp.maximum(deg_f[c], 1.0))
        scale = jnp.transpose(jnp.broadcast_to(scale, (IB, UD)))
        return (mask[c].astype(F32) * scale * scale_item).astype(BF16)

    def target(k):
        dz, dy = order(k)
        return ((z + dz) % Z) * Y + (y + dy) % Y

    def ship(k):
        to = target(k)
        remote(send_a.at[to], slab.at[col], ATOA, row, to, recv=a2a_recv.at[col]).start()

    send_a[target(0)] = piece(target(0))

    def make_and_ship(k):
        send_a[target(k)] = piece(target(k))
        ship(k - 1)

    each(1, C - 1, make_and_ship)
    slab[col] = piece(col)
    ship(C - 2)
    gather_d(tbl0, GATHER0)
    gather_end(tbl0, GATHER0)

    def scatter_a(n, g, ed):
        p, rd = rs[n][0], rs[n][1]
        per = Z // groups[n]

        def block(k):
            zi, cy = k // Y, k % Y
            val = jnp.dot(slab_t[(g * per + zi) * Y + cy], ed[...], preferred_element_type=F32)
            for i in range(R):
                p[i % 2, g, cy * X + i // 2, zi] = jnp.where(lane_left, val[i * SH:i * SH + HS], val[i * SH + HS:(i + 1) * SH])

        lax.fori_loop(0, per * Y, lambda k, t: (block(k), t)[1], 0, unroll=4)
        remote(p.at[1 - core, g], rd.at[g], base[n], mate, col, recv=recvs.at[base[n] + g]).start()

    def scatter_b(n, g):
        p, rd, s1, rxy, _, _ = rs[n]
        remote(rd.at[g], rd.at[g], base[n], row, col, recv=recvs.at[base[n] + g]).wait_recv()

        def fold(k):
            to = (q + k) % Q
            s1[g, to] = p[core, g, to] + rd[g, to]

        def go(k):
            to = (q + k) % Q
            remote(s1.at[g, to], rxy.at[g, q], base[n] + 1, *at_q(to), recv=recvs.at[base[n] + groups[n] + g]).start()

        def both(k):
            fold(k)
            go(k - 1)

        fold(1)
        each(2, Q, both)
        rxy[g, q] = p[core, g, q] + rd[g, q]
        go(Q - 1)

    def scatter_c(n, g):
        _, _, _, rxy, s2, rz = rs[n]
        per = Z // groups[n]
        part = rxy.at[g, pl.ds(0, Q - 1)]
        remote(part, part, base[n], row, col, recv=recvs.at[base[n] + groups[n] + g]).wait_recv()
        for zi in range(per):
            to = g * per + zi
            s2[to] = lax.fori_loop(1, Q, lambda k, t: t + rxy[g, k, zi], rxy[g, 0, zi], unroll=True)
        for zi in range(per):
            to = g * per + zi

            @pl.when(to != z)
            def _():
                remote(s2.at[to], rz.at[z], base[n] + 2, row, to * Y + y, recv=recvs.at[base[n] + 2 * groups[n]]).start()

            @pl.when(to == z)
            def _():
                rz[z] = s2[to]

    def scatter_end(n):
        rz = rs[n][5]
        part = rz.at[pl.ds(0, Z - 1)]
        remote(part, part, base[n], row, col, recv=recvs.at[base[n] + 2 * groups[n]]).wait_recv()
        return lax.fori_loop(1, Z, lambda k, t: t + rz[k], rz[0], unroll=True).astype(BF16)

    def scatter_sent(n):
        p, _, s1, _, s2, _ = rs[n]
        await_send(p.at[0], base[n])
        await_send(s1.at[:, pl.ds(0, Q - 1)], base[n] + 1)
        await_send(s2.at[pl.ds(0, Z - 1)], base[n] + 2)

    def source(k):
        dz, dy = order(k)
        return ((z - dz + Z) % Z) * Y + (y - dy + Y) % Y

    def use(c):
        blk = slab[c]
        slab_t[c] = jnp.transpose(blk)
        acc[...] += jnp.dot(blk, rows_of(tbl0, c), preferred_element_type=F32)

    def arrive(k):
        c = source(k)
        pltpu.make_async_remote_copy(src_ref=slab.at[c], dst_ref=slab.at[c], send_sem=sends.at[ATOA], recv_sem=a2a_recv.at[c],
                                     device_id=(col, row), device_id_type=MESH).wait_recv()
        use(c)

    def group(j):
        return source(j * Y) // Y

    acc[...] = jnp.zeros_like(acc)
    use(col)

    def stream(j):
        each(j * Y, (j + 1) * Y, arrive)
        scatter_a(0, group(j), ed0)

        @pl.when(j >= 1)
        def _():
            scatter_b(0, group(j - 1))

        @pl.when(j >= 2)
        def _():
            scatter_c(0, group(j - 2))

    each(0, Z - 1, stream)
    each((Z - 1) * Y, C - 1, arrive)
    wide_left = lax.broadcasted_iota(jnp.int32, (UD, WIDE), 1) < FEAT

    def twice(v):
        return jnp.where(wide_left, v, swap(v)).astype(BF16)

    user1 = acc[...].astype(BF16).astype(F32)
    ed1[...] = twice(user1)
    for g in range(G2):
        scatter_a(1, g, ed1)
        if g > 0:
            scatter_b(1, g - 1)
    scatter_a(0, z, ed0)
    scatter_b(1, G2 - 1)
    scatter_b(0, group(Z - 2))
    scatter_b(0, z)
    if Z > 2:
        scatter_c(0, group(Z - 3))
    scatter_c(1, 0)
    scatter_c(0, group(Z - 2))
    scatter_c(0, z)
    for g in range(1, G2):
        scatter_c(1, g)
    item1 = scatter_end(0).astype(F32)
    item2 = scatter_end(1).astype(F32)
    low = jnp.where(lane_left, item1, swap(item2))
    high = jnp.where(lane_left, swap(item1), item2)
    tbl1[core, q, z] = jnp.concatenate([low, high], axis=0).astype(BF16)
    gather_z(tbl1, GATHER1)
    gather_q(tbl1, GATHER1)
    gather_d(tbl1, GATHER1)
    acc[...] = jnp.zeros_like(acc)
    gather_end(tbl1, GATHER1)

    def absorb(c):
        cz, cy = c // Y, c % Y
        rows = jnp.concatenate([tbl1[i % 2, cy * X + i // 2, cz] for i in range(R)], axis=0)
        acc[...] += jnp.dot(slab[c], rows, preferred_element_type=F32)

    lax.fori_loop(0, C, lambda k, t: (absorb(k), t)[1], 0, unroll=4)
    late = acc[...].astype(BF16).astype(F32)
    ed2[...] = twice(late)
    scatter_a(2, 0, ed2)
    sum_user = ((ed0[...].astype(F32) + ed1[...].astype(F32)) + ed2[...].astype(F32)) + jnp.where(wide_left, swap(late), late)
    user_rows = (sum_user / (LAYERS + 1)).astype(BF16)

    ids = lax.broadcasted_iota(jnp.int32, (UD, TRIPLES), 0) + (row * C + col) * UD
    hit = (ids == trip[0:1, :]).astype(BF16)
    found = lax.dot_general(hit, user_rows, (((0,), (0,)), ((), ())), preferred_element_type=F32)
    pick_left = lax.broadcasted_iota(jnp.int32, (PICKS, WIDE), 1) < FEAT
    for h in range(2):
        lo, hi = h * PICKS, (h + 2) * PICKS
        pk_a[h] = jnp.where(pick_left, found[lo:lo + PICKS], found[hi:hi + PICKS]).astype(BF16)
    remote(pk_a.at[1 - core], pk_b, PICK, mate, col).start()
    for g in range(1, G2):
        scatter_a(2, g, ed2)
        if g == 1:
            await_recv(pk_b, PICK)
            pk_z[z] = (pk_a[core].astype(F32) + pk_b[...].astype(F32)).astype(BF16)
            each(1, Z, lambda k: remote(pk_z.at[z], pk_z.at[z], PICK + 1, row, ((z + k) % Z) * Y + y).start())
        scatter_b(2, g - 1)
    scatter_b(2, G2 - 1)
    out_user[...] = jnp.transpose(user_rows.astype(F32))[:FEAT].astype(BF16)
    await_recv(pk_z.at[pl.ds(0, Z - 1)], PICK + 1)
    pk_q[q] = lax.fori_loop(1, Z, lambda k, t: t + pk_z[k].astype(F32), pk_z[0].astype(F32), unroll=True).astype(BF16)
    each(1, Q, lambda k: remote(pk_q.at[q], pk_q.at[q], PICK + 2, *at_q((q + k) % Q)).start())
    for g in range(G2):
        scatter_c(2, g)
    await_recv(pk_q.at[pl.ds(0, Q - 1)], PICK + 2)
    pk_d[core] = lax.fori_loop(1, Q, lambda k, t: t + pk_q[k].astype(F32), pk_q[0].astype(F32), unroll=True).astype(BF16)
    remote(pk_d.at[core], pk_d.at[core], PICK + 3, mate, col).start()
    item3 = scatter_end(2)
    sum_item = ((item0 + item1) + item2) + item3.astype(F32)
    packed = (sum_item / (LAYERS + 1)).astype(BF16).astype(F32)
    zero = jnp.zeros_like(packed)
    left_rows = [jnp.where(lane_left, packed, zero), jnp.where(lane_left, swap(packed), zero)]
    right_rows = [jnp.where(lane_left, zero, swap(packed)), jnp.where(lane_left, zero, packed)]
    item_rows = jnp.concatenate(left_rows, axis=0).astype(BF16)
    out_item[...] = item_rows[:, :FEAT]

    await_recv(pk_d.at[0], PICK + 3)
    user_vec = jnp.concatenate([pk_d[0], pk_d[1], pk_d[0], pk_d[1]], axis=0)
    nt = (((1,), (1,)), ((), ()))
    dots_l = lax.dot_general(item_rows, user_vec, nt, preferred_element_type=F32)
    dots_r = lax.dot_general(jnp.concatenate(right_rows, axis=0).astype(BF16), user_vec, nt, preferred_element_type=F32)
    dots = jnp.where(lax.broadcasted_iota(jnp.int32, (SH, TRIPLES), 1) < TRIPLES // 2, dots_l, dots_r)
    own = lax.broadcasted_iota(jnp.int32, (SH, TRIPLES), 0) + (col * R + row) * SH
    pos = jnp.sum(jnp.where(own == trip[1:2, :], dots, 0.0), axis=0, keepdims=True)
    neg = jnp.sum(jnp.where(own == trip[2:3, :], dots, 0.0), axis=0, keepdims=True)
    xc[col] = pos - neg
    each(1, C, lambda k: remote(xc.at[col], xc.at[col], MARGIN, row, (col + k) % C).start())
    await_recv(xc.at[pl.ds(0, C - 1)], MARGIN)
    xr[row] = lax.fori_loop(1, C, lambda k, t: t + xc[k], xc[0], unroll=True)
    each(1, R, lambda k: remote(xr.at[row], xr.at[row], MARGIN + 1, (row + k) % R, col).start())
    await_recv(xr.at[pl.ds(0, R - 1)], MARGIN + 1)
    margin = lax.fori_loop(1, R, lambda k, t: t + xr[k], xr[0], unroll=True)
    soft = jnp.maximum(-margin, 0.0) + jnp.log1p(jnp.exp(-jnp.abs(margin)))
    loss[...] = jnp.sum(soft, axis=1, keepdims=True) / TRIPLES

    await_send(deg_s.at[pl.ds(0, C - 1)], DEG)
    await_send(ideg.at[pl.ds(0, R - 1)], IDEG)
    await_send(deg_f.at[pl.ds(0, C - 1)], SPREAD)
    await_send(send_a.at[pl.ds(0, C - 1)], ATOA)
    gather_sent(tbl0, GATHER0)
    gather_sent(tbl1, GATHER1)
    for n in range(3):
        scatter_sent(n)
    await_send(pk_b, PICK)
    await_send(pk_z.at[pl.ds(0, Z - 1)], PICK + 1)
    await_send(pk_q.at[pl.ds(0, Q - 1)], PICK + 2)
    await_send(pk_d.at[0], PICK + 3)
    await_send(xc.at[pl.ds(0, C - 1)], MARGIN)
    await_send(xr.at[pl.ds(0, R - 1)], MARGIN + 1)


def build(mesh, Y, SH, UD, G2):
    C, R = mesh.shape["col"], mesh.shape["row"]
    Z, X = C // Y, R // 2
    Q, IB, HS = Y * X, R * SH, SH // 2
    vm = pltpu.VMEM
    scratch = [
        vm((C, 1, UD), F32), vm((C, 1, UD), F32), vm((C, 1, UD), F32), vm((1, UD), F32), vm((R, 1, IB), F32),
        vm((C, UD, IB), BF16), vm((C, UD, IB), BF16), vm((C, IB, UD), BF16),
        vm((2, Q, Z, HS, WIDE), BF16), vm((2, Q, Z, SH, WIDE), BF16),
        vm((UD, WIDE), F32), vm((UD, WIDE), BF16), vm((UD, WIDE), BF16), vm((UD, WIDE), BF16),
        vm((2, PICKS, WIDE), BF16), vm((PICKS, WIDE), BF16),
        vm((Z, PICKS, WIDE), BF16), vm((Q, PICKS, WIDE), BF16), vm((2, PICKS, WIDE), BF16),
        vm((C, 1, TRIPLES), F32), vm((R, 1, TRIPLES), F32),
    ]
    count = SCATTER1 + sum(2 * g + 1 for g in (Z, G2, G2)) + 1
    scratch += [pltpu.SemaphoreType.DMA((count,)), pltpu.SemaphoreType.DMA((count,)), pltpu.SemaphoreType.DMA((C,)),
                vm((C, UD, IB), jnp.int32), pltpu.SemaphoreType.DMA((LOADS,))]
    for g in (Z, G2, G2):
        scratch += [vm((2, g, Q, Z // g, HS, WIDE), F32)] + [vm((g, Q, Z // g, HS, WIDE), F32)] * 3 + [vm((Z, HS, WIDE), F32)] * 2
    dims = (Z, Y, X, SH, UD, G2)

    def local_prog(mask_blk, user_shard, item_shard, triples):
        out_user, out_item, loss = pl.pallas_call(
            functools.partial(kernel, dims),
            out_shape=(
                jax.ShapeDtypeStruct((FEAT, UD), BF16),
                jax.ShapeDtypeStruct((SH, FEAT), BF16),
                jax.ShapeDtypeStruct((1, 1), F32),
            ),
            in_specs=[pl.BlockSpec(memory_space=pl.ANY)] + [pl.BlockSpec(memory_space=pltpu.VMEM)] * 3,
            out_specs=(pl.BlockSpec(memory_space=pltpu.VMEM),) * 3,
            scratch_shapes=scratch,
            compiler_params=pltpu.CompilerParams(
                collective_id=0, has_side_effects=True, vmem_limit_bytes=60 * 1024 * 1024),
            name="lightgcn",
        )(mask_blk.reshape(C, UD, IB), user_shard.T, item_shard, triples.T)
        return out_user.T, out_item, loss[0, 0]

    return jax.shard_map(
        local_prog, mesh=mesh,
        in_specs=(P("row", "col"), P(("row", "col"), None), P(("col", "row"), None), P(None, None)),
        out_specs=(P(("row", "col"), None), P(("col", "row"), None), P()), check_vma=False)


def solution(mesh):
    return build(mesh, Y=4, SH=16, UD=256, G2=4)
```

```python
import functools

import jax
import jax.numpy as jnp
from jax import lax
from jax.experimental import pallas as pl
from jax.experimental.pallas import tpu as pltpu
from jax.sharding import PartitionSpec as P

MESH = pl.DeviceIdType.MESH
F32 = jnp.float32
BF16 = jnp.bfloat16
FEAT = 64
WIDE = 2 * FEAT
TRIPLES = 128
LAYERS = 3
LOADS = 8
PICKS = TRIPLES // 4

DEG, IDEG, SPREAD, ATOA, GATHER0, GATHER1, PICK, MARGIN, SCATTER1 = 0, 1, 2, 3, 4, 7, 10, 14, 16


def swap(v):
    return pltpu.roll(v, FEAT, 1)


def kernel(dims, mask_hbm, eu0, ei0, trip, out_user, out_item, loss, *scratch):
    Z, Y, X, SH, UD, G2 = dims
    C, R, Q = Z * Y, 2 * X, Y * X
    IB = R * SH
    HS = SH // 2
    (deg_s, deg_r, deg_f, own_deg, ideg, send_a, slab, slab_t, tbl0, tbl1, acc, ed0, ed1, ed2, pk_a, pk_b, pk_z, pk_q, pk_d, xc, xr,
     sends, recvs, a2a_recv, mask, load_sem) = scratch[:26]
    groups = (Z, G2, G2)
    p_1, rd_1, s1_1, rx_1, sy_1, ry_1, s2_1, rz_1, one_send, one_d, one_x, one_yz = scratch[26:38]
    rs = [None] + [scratch[32 + 6 * n:38 + 6 * n] for n in (1, 2)]
    base = [SCATTER1]
    base.append(SCATTER1)
    for n in (1, 2):
        base.append(base[-1] + 2 * groups[n] + 1)
    row = lax.axis_index("row")
    col = lax.axis_index("col")
    core, x = row % 2, row // 2
    z, y = col // Y, col % Y
    q = y * X + x
    mate = x * 2 + (1 - core)

    def remote(src, dst, sem, r, c, recv=None):
        return pltpu.make_async_remote_copy(
            src_ref=src, dst_ref=dst, send_sem=sends.at[sem], recv_sem=recvs.at[sem] if recv is None else recv,
            device_id=(c, r), device_id_type=MESH)

    def await_recv(ref, sem):
        remote(ref, ref, sem, row, col).wait_recv()

    def await_send(ref, sem):
        remote(ref, ref, sem, row, col).wait_send()

    def at_q(p):
        return (p % X) * 2 + core, z * Y + p // X

    def each(lo, hi, fn):
        lax.fori_loop(lo, hi, lambda k, t: (fn(k), t)[1], 0)

    run = C // LOADS

    def load(i):
        part = pl.ds(i * run, run)
        return pltpu.make_async_copy(mask_hbm.at[part], mask.at[part], load_sem.at[i])

    for i in range(LOADS):
        load(i).start()

    barrier = pltpu.get_barrier_semaphore()

    def hail(c, r):
        pl.semaphore_signal(barrier, inc=1, device_id=(c, r), device_id_type=MESH)

    each(1, C, lambda k: hail((col + k) % C, row))
    each(1, R, lambda k: hail(col, (row + k) % R))
    each(0, (X - 1) * (Y - 1), lambda k: hail(z * Y + (y + 1 + k // (X - 1)) % Y, ((x + 1 + k % (X - 1)) % X) * 2 + core))

    ones = jnp.ones((8, IB), BF16)

    def count(k, part):
        blk = mask[k].astype(F32)
        sums = lax.dot_general(ones, blk.astype(BF16), (((1,), (1,)), ((), ())), preferred_element_type=F32)
        deg_s[k] = sums[0:1]
        return part + jnp.sum(blk.reshape(UD // 8, 8, IB), axis=0)

    part = jnp.zeros((8, IB), F32)
    for i in range(LOADS):
        load(i).wait()
        part = lax.fori_loop(i * run, (i + 1) * run, count, part, unroll=True)
    ideg[row] = jnp.sum(part, axis=0, keepdims=True)
    deg_r[col] = deg_s[col]

    lane_left = lax.broadcasted_iota(jnp.int32, (HS, WIDE), 1) < FEAT

    def pack(v):
        return jnp.where(lane_left, v[:HS], swap(v[HS:]))

    e0 = ei0[...].astype(F32)
    item0 = pack(jnp.concatenate([e0, jnp.zeros_like(e0)], axis=1))
    tbl0[core, q, z] = item0.astype(BF16)
    user0 = eu0[...].astype(F32)
    ed0[...] = jnp.transpose(jnp.concatenate([user0, user0], axis=0)).astype(BF16)
    pl.semaphore_wait(barrier, (C - 1) + (R - 1) + (X - 1) * (Y - 1))

    def gather_z(tbl, sem):
        each(1, Z, lambda k: remote(tbl.at[core, q, z], tbl.at[core, q, z], sem, row, ((z + k) % Z) * Y + y).start())

    def gather_q(tbl, sem):
        await_recv(tbl.at[core, q, pl.ds(0, Z - 1)], sem)
        each(1, Q, lambda k: remote(tbl.at[core, q], tbl.at[core, q], sem + 1, *at_q((q + k) % Q)).start())

    def gather_d(tbl, sem):
        await_recv(tbl.at[core, pl.ds(0, Q - 1)], sem + 1)
        remote(tbl.at[core], tbl.at[core], sem + 2, mate, col).start()

    def gather_end(tbl, sem):
        await_recv(tbl.at[core], sem + 2)

    def gather_sent(tbl, sem):
        await_send(tbl.at[core, q, pl.ds(0, Z - 1)], sem)
        await_send(tbl.at[core, pl.ds(0, Q - 1)], sem + 1)
        await_send(tbl.at[core], sem + 2)

    def rows_of(tbl, c):
        cz, cy = c // Y, c % Y
        parts = []
        for i in range(R):
            v = tbl[i % 2, cy * X + i // 2, cz].astype(F32)
            parts += [v, swap(v)]
        return jnp.concatenate(parts, axis=0).astype(BF16)

    each(1, C, lambda k: remote(deg_s.at[(col + k) % C], deg_r.at[col], DEG, row, (col + k) % C).start())
    each(1, R, lambda k: remote(ideg.at[row], ideg.at[row], IDEG, (row + k) % R, col).start())
    gather_z(tbl0, GATHER0)
    await_recv(deg_r.at[pl.ds(0, C - 1)], DEG)
    own_deg[...] = lax.fori_loop(0, C, lambda k, t: t + deg_r[k], jnp.zeros((1, UD), F32), unroll=True)
    deg_f[col] = own_deg[...]
    each(1, C, lambda k: remote(own_deg, deg_f.at[col], SPREAD, row, (col + k) % C).start())
    await_recv(ideg.at[pl.ds(0, R - 1)], IDEG)
    scale_item = lax.rsqrt(jnp.maximum(lax.fori_loop(0, R, lambda k, t: t + ideg[k], jnp.zeros((1, IB), F32), unroll=True), 1.0))
    gather_q(tbl0, GATHER0)
    await_recv(deg_f.at[pl.ds(0, C - 1)], SPREAD)

    def order(k):
        j, dy = k // Y, (k + 1) % Y
        m = Z // 2 - (j + 1) // 2
        odd = j % 2
        return (odd * m + (1 - odd) * (Z - m)) % Z, dy

    def piece(c):
        scale = lax.rsqrt(jnp.maximum(deg_f[c], 1.0))
        scale = jnp.transpose(jnp.broadcast_to(scale, (IB, UD)))
        return (mask[c].astype(F32) * scale * scale_item).astype(BF16)

    def target(k):
        dz, dy = order(k)
        return ((z + dz) % Z) * Y + (y + dy) % Y

    def ship(k):
        to = target(k)
        remote(send_a.at[to], slab.at[col], ATOA, row, to, recv=a2a_recv.at[col]).start()

    send_a[target(0)] = piece(target(0))

    def make_and_ship(k):
        send_a[target(k)] = piece(target(k))
        ship(k - 1)

    each(1, C - 1, make_and_ship)
    slab[col] = piece(col)
    ship(C - 2)
    gather_d(tbl0, GATHER0)
    gather_end(tbl0, GATHER0)

    def scatter_a(n, g, ed):
        p, rd = rs[n][0], rs[n][1]
        per = Z // groups[n]

        def block(k):
            zi, cy = k // Y, k % Y
            val = jnp.dot(slab_t[(g * per + zi) * Y + cy], ed[...], preferred_element_type=F32)
            for i in range(R):
                p[i % 2, g, cy * X + i // 2, zi] = jnp.where(lane_left, val[i * SH:i * SH + HS], val[i * SH + HS:(i + 1) * SH])

        lax.fori_loop(0, per * Y, lambda k, t: (block(k), t)[1], 0, unroll=4)
        remote(p.at[1 - core, g], rd.at[g], base[n], mate, col, recv=recvs.at[base[n] + g]).start()

    def scatter_b(n, g):
        p, rd, s1, rxy, _, _ = rs[n]
        remote(rd.at[g], rd.at[g], base[n], row, col, recv=recvs.at[base[n] + g]).wait_recv()

        def fold(k):
            to = (q + k) % Q
            s1[g, to] = p[core, g, to] + rd[g, to]

        def go(k):
            to = (q + k) % Q
            remote(s1.at[g, to], rxy.at[g, q], base[n] + 1, *at_q(to), recv=recvs.at[base[n] + groups[n] + g]).start()

        def both(k):
            fold(k)
            go(k - 1)

        fold(1)
        each(2, Q, both)
        rxy[g, q] = p[core, g, q] + rd[g, q]
        go(Q - 1)

    def scatter_c(n, g):
        _, _, _, rxy, s2, rz = rs[n]
        per = Z // groups[n]
        part = rxy.at[g, pl.ds(0, Q - 1)]
        remote(part, part, base[n], row, col, recv=recvs.at[base[n] + groups[n] + g]).wait_recv()
        for zi in range(per):
            to = g * per + zi
            s2[to] = lax.fori_loop(1, Q, lambda k, t: t + rxy[g, k, zi], rxy[g, 0, zi], unroll=True)
        for zi in range(per):
            to = g * per + zi

            @pl.when(to != z)
            def _():
                remote(s2.at[to], rz.at[z], base[n] + 2, row, to * Y + y, recv=recvs.at[base[n] + 2 * groups[n]]).start()

            @pl.when(to == z)
            def _():
                rz[z] = s2[to]

    def scatter_end(n):
        rz = rs[n][5]
        part = rz.at[pl.ds(0, Z - 1)]
        remote(part, part, base[n], row, col, recv=recvs.at[base[n] + 2 * groups[n]]).wait_recv()
        return lax.fori_loop(1, Z, lambda k, t: t + rz[k], rz[0], unroll=True).astype(BF16)

    def scatter_sent(n):
        p, _, s1, _, s2, _ = rs[n]
        await_send(p.at[0], base[n])
        await_send(s1.at[:, pl.ds(0, Q - 1)], base[n] + 1)
        await_send(s2.at[pl.ds(0, Z - 1)], base[n] + 2)

    def remote1(src, dst, k, r, c, recv):
        return pltpu.make_async_remote_copy(
            src_ref=src, dst_ref=dst, send_sem=one_send.at[k], recv_sem=recv, device_id=(c, r), device_id_type=MESH)

    def await1(ref, recv):
        remote1(ref, ref, 0, row, col, recv).wait_recv()

    def first_a(g):
        def block(cy):
            val = jnp.dot(slab_t[g * Y + cy], ed0[...], preferred_element_type=F32)
            for i in range(R):
                p_1[i % 2, g, i // 2, cy] = jnp.where(lane_left, val[i * SH:i * SH + HS], val[i * SH + HS:(i + 1) * SH])

        lax.fori_loop(0, Y, lambda k, t: (block(k), t)[1], 0, unroll=4)
        remote1(p_1.at[1 - core, g], rd_1.at[g], 0, mate, col, one_d.at[g]).start()

    def first_b(g):
        await1(rd_1.at[g], one_d.at[g])
        for k in range(1, X):
            to = (x + k) % X
            s1_1[g, to] = p_1[core, g, to] + rd_1[g, to]
        rx_1[g, x] = p_1[core, g, x] + rd_1[g, x]
        for k in range(1, X):
            to = (x + k) % X
            remote1(s1_1.at[g, to], rx_1.at[g, x], 1, to * 2 + core, col, one_x.at[g]).start()

    def first_c(g):
        await1(rx_1.at[g, pl.ds(0, X - 1)], one_x.at[g])
        total = rx_1[g, 0]
        for k in range(1, X):
            total = total + rx_1[g, k]
        for cy in range(Y):
            sy_1[cy, g] = total[cy]

    def first_y():
        for k in range(1, Y):
            to = (y + k) % Y
            remote1(sy_1.at[to], ry_1.at[y], 2, row, z * Y + to, one_yz.at[0]).start()
        ry_1[y] = sy_1[y]

    def first_z():
        await1(ry_1.at[pl.ds(0, Y - 1)], one_yz.at[0])
        total = ry_1[0]
        for k in range(1, Y):
            total = total + ry_1[k]
        s2_1[...] = total
        rz_1[z] = s2_1[z]
        each(1, Z, lambda k: remote1(s2_1.at[(z + k) % Z], rz_1.at[z], 3, row, ((z + k) % Z) * Y + y, one_yz.at[1]).start())

    def first_end():
        await1(rz_1.at[pl.ds(0, Z - 1)], one_yz.at[1])
        return lax.fori_loop(1, Z, lambda k, t: t + rz_1[k], rz_1[0], unroll=True).astype(BF16)

    def first_sent():
        for k, ref in enumerate((p_1.at[0], s1_1.at[:, pl.ds(0, X - 1)], sy_1.at[pl.ds(0, Y - 1)], s2_1.at[pl.ds(0, Z - 1)])):
            remote1(ref, ref, k, row, col, one_yz.at[0]).wait_send()

    def source(k):
        dz, dy = order(k)
        return ((z - dz + Z) % Z) * Y + (y - dy + Y) % Y

    def use(c):
        blk = slab[c]
        slab_t[c] = jnp.transpose(blk)
        acc[...] += jnp.dot(blk, rows_of(tbl0, c), preferred_element_type=F32)

    def arrive(k):
        c = source(k)
        pltpu.make_async_remote_copy(src_ref=slab.at[c], dst_ref=slab.at[c], send_sem=sends.at[ATOA], recv_sem=a2a_recv.at[c],
                                     device_id=(col, row), device_id_type=MESH).wait_recv()
        use(c)

    def group(j):
        return source(j * Y) // Y

    acc[...] = jnp.zeros_like(acc)
    use(col)

    def stream(j):
        each(j * Y, (j + 1) * Y, arrive)
        first_a(group(j))

        @pl.when(j >= 1)
        def _():
            first_b(group(j - 1))

        @pl.when(j >= 2)
        def _():
            first_c(group(j - 2))

    each(0, Z - 1, stream)
    each((Z - 1) * Y, C - 1, arrive)
    wide_left = lax.broadcasted_iota(jnp.int32, (UD, WIDE), 1) < FEAT

    def twice(v):
        return jnp.where(wide_left, v, swap(v)).astype(BF16)

    first_a(z)
    first_b(group(Z - 2))
    user1 = acc[...].astype(BF16).astype(F32)
    ed1[...] = twice(user1)
    for g in range(G2):
        scatter_a(1, g, ed1)
        if g == 0:
            first_b(z)
        else:
            scatter_b(1, g - 1)
    scatter_b(1, G2 - 1)
    if Z > 2:
        first_c(group(Z - 3))
    first_c(group(Z - 2))
    first_c(z)
    first_y()
    for g in range(G2 // 2):
        scatter_c(1, g)
    first_z()
    for g in range(G2 // 2, G2):
        scatter_c(1, g)
    item1 = first_end().astype(F32)
    item2 = scatter_end(1).astype(F32)
    low = jnp.where(lane_left, item1, swap(item2))
    high = jnp.where(lane_left, swap(item1), item2)
    tbl1[core, q, z] = jnp.concatenate([low, high], axis=0).astype(BF16)
    gather_z(tbl1, GATHER1)
    gather_q(tbl1, GATHER1)
    gather_d(tbl1, GATHER1)
    acc[...] = jnp.zeros_like(acc)
    gather_end(tbl1, GATHER1)

    def absorb(c):
        cz, cy = c // Y, c % Y
        rows = jnp.concatenate([tbl1[i % 2, cy * X + i // 2, cz] for i in range(R)], axis=0)
        acc[...] += jnp.dot(slab[c], rows, preferred_element_type=F32)

    lax.fori_loop(0, C, lambda k, t: (absorb(k), t)[1], 0, unroll=4)
    late = acc[...].astype(BF16).astype(F32)
    ed2[...] = twice(late)
    scatter_a(2, 0, ed2)
    sum_user = ((ed0[...].astype(F32) + ed1[...].astype(F32)) + ed2[...].astype(F32)) + jnp.where(wide_left, swap(late), late)
    user_rows = (sum_user / (LAYERS + 1)).astype(BF16)

    ids = lax.broadcasted_iota(jnp.int32, (UD, TRIPLES), 0) + (row * C + col) * UD
    hit = (ids == trip[0:1, :]).astype(BF16)
    found = lax.dot_general(hit, user_rows, (((0,), (0,)), ((), ())), preferred_element_type=F32)
    pick_left = lax.broadcasted_iota(jnp.int32, (PICKS, WIDE), 1) < FEAT
    for h in range(2):
        lo, hi = h * PICKS, (h + 2) * PICKS
        pk_a[h] = jnp.where(pick_left, found[lo:lo + PICKS], found[hi:hi + PICKS]).astype(BF16)
    remote(pk_a.at[1 - core], pk_b, PICK, mate, col).start()
    for g in range(1, G2):
        scatter_a(2, g, ed2)
        if g == 1:
            await_recv(pk_b, PICK)
            pk_z[z] = (pk_a[core].astype(F32) + pk_b[...].astype(F32)).astype(BF16)
            each(1, Z, lambda k: remote(pk_z.at[z], pk_z.at[z], PICK + 1, row, ((z + k) % Z) * Y + y).start())
        scatter_b(2, g - 1)
    scatter_b(2, G2 - 1)
    out_user[...] = jnp.transpose(user_rows.astype(F32))[:FEAT].astype(BF16)
    await_recv(pk_z.at[pl.ds(0, Z - 1)], PICK + 1)
    pk_q[q] = lax.fori_loop(1, Z, lambda k, t: t + pk_z[k].astype(F32), pk_z[0].astype(F32), unroll=True).astype(BF16)
    each(1, Q, lambda k: remote(pk_q.at[q], pk_q.at[q], PICK + 2, *at_q((q + k) % Q)).start())
    for g in range(G2):
        scatter_c(2, g)
    await_recv(pk_q.at[pl.ds(0, Q - 1)], PICK + 2)
    pk_d[core] = lax.fori_loop(1, Q, lambda k, t: t + pk_q[k].astype(F32), pk_q[0].astype(F32), unroll=True).astype(BF16)
    remote(pk_d.at[core], pk_d.at[core], PICK + 3, mate, col).start()
    item3 = scatter_end(2)
    sum_item = ((item0 + item1) + item2) + item3.astype(F32)
    packed = (sum_item / (LAYERS + 1)).astype(BF16).astype(F32)
    zero = jnp.zeros_like(packed)
    left_rows = [jnp.where(lane_left, packed, zero), jnp.where(lane_left, swap(packed), zero)]
    right_rows = [jnp.where(lane_left, zero, swap(packed)), jnp.where(lane_left, zero, packed)]
    item_rows = jnp.concatenate(left_rows, axis=0).astype(BF16)
    out_item[...] = item_rows[:, :FEAT]

    await_recv(pk_d.at[0], PICK + 3)
    user_vec = jnp.concatenate([pk_d[0], pk_d[1], pk_d[0], pk_d[1]], axis=0)
    nt = (((1,), (1,)), ((), ()))
    dots_l = lax.dot_general(item_rows, user_vec, nt, preferred_element_type=F32)
    dots_r = lax.dot_general(jnp.concatenate(right_rows, axis=0).astype(BF16), user_vec, nt, preferred_element_type=F32)
    dots = jnp.where(lax.broadcasted_iota(jnp.int32, (SH, TRIPLES), 1) < TRIPLES // 2, dots_l, dots_r)
    own = lax.broadcasted_iota(jnp.int32, (SH, TRIPLES), 0) + (col * R + row) * SH
    pos = jnp.sum(jnp.where(own == trip[1:2, :], dots, 0.0), axis=0, keepdims=True)
    neg = jnp.sum(jnp.where(own == trip[2:3, :], dots, 0.0), axis=0, keepdims=True)
    xc[col] = pos - neg
    each(1, C, lambda k: remote(xc.at[col], xc.at[col], MARGIN, row, (col + k) % C).start())
    await_recv(xc.at[pl.ds(0, C - 1)], MARGIN)
    xr[row] = lax.fori_loop(1, C, lambda k, t: t + xc[k], xc[0], unroll=True)
    each(1, R, lambda k: remote(xr.at[row], xr.at[row], MARGIN + 1, (row + k) % R, col).start())
    await_recv(xr.at[pl.ds(0, R - 1)], MARGIN + 1)
    margin = lax.fori_loop(1, R, lambda k, t: t + xr[k], xr[0], unroll=True)
    soft = jnp.maximum(-margin, 0.0) + jnp.log1p(jnp.exp(-jnp.abs(margin)))
    loss[...] = jnp.sum(soft, axis=1, keepdims=True) / TRIPLES

    await_send(deg_s.at[pl.ds(0, C - 1)], DEG)
    await_send(ideg.at[pl.ds(0, R - 1)], IDEG)
    await_send(deg_f.at[pl.ds(0, C - 1)], SPREAD)
    await_send(send_a.at[pl.ds(0, C - 1)], ATOA)
    gather_sent(tbl0, GATHER0)
    gather_sent(tbl1, GATHER1)
    first_sent()
    for n in (1, 2):
        scatter_sent(n)
    await_send(pk_b, PICK)
    await_send(pk_z.at[pl.ds(0, Z - 1)], PICK + 1)
    await_send(pk_q.at[pl.ds(0, Q - 1)], PICK + 2)
    await_send(pk_d.at[0], PICK + 3)
    await_send(xc.at[pl.ds(0, C - 1)], MARGIN)
    await_send(xr.at[pl.ds(0, R - 1)], MARGIN + 1)


def build(mesh, Y, SH, UD, G2):
    C, R = mesh.shape["col"], mesh.shape["row"]
    Z, X = C // Y, R // 2
    Q, IB, HS = Y * X, R * SH, SH // 2
    vm = pltpu.VMEM
    scratch = [
        vm((C, 1, UD), F32), vm((C, 1, UD), F32), vm((C, 1, UD), F32), vm((1, UD), F32), vm((R, 1, IB), F32),
        vm((C, UD, IB), BF16), vm((C, UD, IB), BF16), vm((C, IB, UD), BF16),
        vm((2, Q, Z, HS, WIDE), BF16), vm((2, Q, Z, SH, WIDE), BF16),
        vm((UD, WIDE), F32), vm((UD, WIDE), BF16), vm((UD, WIDE), BF16), vm((UD, WIDE), BF16),
        vm((2, PICKS, WIDE), BF16), vm((PICKS, WIDE), BF16),
        vm((Z, PICKS, WIDE), BF16), vm((Q, PICKS, WIDE), BF16), vm((2, PICKS, WIDE), BF16),
        vm((C, 1, TRIPLES), F32), vm((R, 1, TRIPLES), F32),
    ]
    count = SCATTER1 + 2 * (2 * G2 + 1)
    sem = pltpu.SemaphoreType.DMA
    scratch += [sem((count,)), sem((count,)), sem((C,)), vm((C, UD, IB), jnp.int32), sem((LOADS,))]
    scratch += [
        vm((2, Z, X, Y, HS, WIDE), F32), vm((Z, X, Y, HS, WIDE), F32), vm((Z, X, Y, HS, WIDE), F32), vm((Z, X, Y, HS, WIDE), F32),
        vm((Y, Z, HS, WIDE), F32), vm((Y, Z, HS, WIDE), F32), vm((Z, HS, WIDE), F32), vm((Z, HS, WIDE), F32),
        sem((4,)), sem((Z,)), sem((Z,)), sem((2,)),
    ]
    for g in (G2, G2):
        scratch += [vm((2, g, Q, Z // g, HS, WIDE), F32)] + [vm((g, Q, Z // g, HS, WIDE), F32)] * 3 + [vm((Z, HS, WIDE), F32)] * 2
    dims = (Z, Y, X, SH, UD, G2)

    def local_prog(mask_blk, user_shard, item_shard, triples):
        out_user, out_item, loss = pl.pallas_call(
            functools.partial(kernel, dims),
            out_shape=(
                jax.ShapeDtypeStruct((FEAT, UD), BF16),
                jax.ShapeDtypeStruct((SH, FEAT), BF16),
                jax.ShapeDtypeStruct((1, 1), F32),
            ),
            in_specs=[pl.BlockSpec(memory_space=pl.ANY)] + [pl.BlockSpec(memory_space=pltpu.VMEM)] * 3,
            out_specs=(pl.BlockSpec(memory_space=pltpu.VMEM),) * 3,
            scratch_shapes=scratch,
            compiler_params=pltpu.CompilerParams(
                collective_id=0, has_side_effects=True, vmem_limit_bytes=60 * 1024 * 1024),
            name="lightgcn",
        )(mask_blk.reshape(C, UD, IB), user_shard.T, item_shard, triples.T)
        return out_user.T, out_item, loss[0, 0]

    return jax.shard_map(
        local_prog, mesh=mesh,
        in_specs=(P("row", "col"), P(("row", "col"), None), P(("col", "row"), None), P(None, None)),
        out_specs=(P(("row", "col"), None), P(("col", "row"), None), P()), check_vma=False)


def solution(mesh):
    return build(mesh, Y=4, SH=16, UD=256, G2=4)
```

```python
import functools

import jax
import jax.numpy as jnp
from jax import lax
from jax.experimental import pallas as pl
from jax.experimental.pallas import tpu as pltpu
from jax.sharding import PartitionSpec as P

MESH = pl.DeviceIdType.MESH
F32 = jnp.float32
BF16 = jnp.bfloat16
FEAT = 64
WIDE = 2 * FEAT
TRIPLES = 128
LAYERS = 3
LOADS = 8
PICKS = TRIPLES // 4

DEG, IDEG, SPREAD, ATOA, GATHER0, GATHER1, PICK, MARGIN, SCATTER1 = 0, 1, 2, 3, 4, 7, 10, 14, 16


def swap(v):
    return pltpu.roll(v, FEAT, 1)


def kernel(dims, mask_hbm, eu0, ei0, trip, out_user, out_item, loss, *scratch):
    Z, Y, X, SH, UD, G2 = dims
    C, R, Q = Z * Y, 2 * X, Y * X
    IB = R * SH
    HS = SH // 2
    (deg_s, deg_r, deg_f, own_deg, ideg, send_a, slab, slab_t, tbl0, tbl1, acc, ed0, ed1, ed2, pk_a, pk_b, pk_z, pk_q, pk_d, xc, xr,
     sends, recvs, a2a_recv, mask, load_sem) = scratch[:26]
    spread_recv = scratch[50]
    groups = (Z, G2, G2)
    p_1, rd_1, s1_1, rx_1, sy_1, ry_1, s2_1, rz_1, one_send, one_d, one_x, one_yz = scratch[26:38]
    rs = [None] + [scratch[32 + 6 * n:38 + 6 * n] for n in (1, 2)]
    base = [SCATTER1]
    base.append(SCATTER1)
    for n in (1, 2):
        base.append(base[-1] + 2 * groups[n] + 1)
    row = lax.axis_index("row")
    col = lax.axis_index("col")
    core, x = row % 2, row // 2
    z, y = col // Y, col % Y
    q = y * X + x
    mate = x * 2 + (1 - core)

    def remote(src, dst, sem, r, c, recv=None):
        return pltpu.make_async_remote_copy(
            src_ref=src, dst_ref=dst, send_sem=sends.at[sem], recv_sem=recvs.at[sem] if recv is None else recv,
            device_id=(c, r), device_id_type=MESH)

    def await_recv(ref, sem):
        remote(ref, ref, sem, row, col).wait_recv()

    def await_send(ref, sem):
        remote(ref, ref, sem, row, col).wait_send()

    def at_q(p):
        return (p % X) * 2 + core, z * Y + p // X

    def each(lo, hi, fn):
        lax.fori_loop(lo, hi, lambda k, t: (fn(k), t)[1], 0)

    run = C // LOADS

    def load(i):
        part = pl.ds(i * run, run)
        return pltpu.make_async_copy(mask_hbm.at[part], mask.at[part], load_sem.at[i])

    for i in range(LOADS):
        load(i).start()

    barrier = pltpu.get_barrier_semaphore()

    def hail(c, r):
        pl.semaphore_signal(barrier, inc=1, device_id=(c, r), device_id_type=MESH)

    each(1, C, lambda k: hail((col + k) % C, row))
    each(1, R, lambda k: hail(col, (row + k) % R))
    each(0, (X - 1) * (Y - 1), lambda k: hail(z * Y + (y + 1 + k // (X - 1)) % Y, ((x + 1 + k % (X - 1)) % X) * 2 + core))

    ones = jnp.ones((8, IB), BF16)

    def count(k, part):
        blk = mask[k].astype(F32)
        sums = lax.dot_general(ones, blk.astype(BF16), (((1,), (1,)), ((), ())), preferred_element_type=F32)
        deg_s[k] = sums[0:1]
        return part + jnp.sum(blk.reshape(UD // 8, 8, IB), axis=0)

    part = jnp.zeros((8, IB), F32)
    for i in range(LOADS):
        load(i).wait()
        part = lax.fori_loop(i * run, (i + 1) * run, count, part, unroll=True)
    ideg[row] = jnp.sum(part, axis=0, keepdims=True)
    deg_r[col] = deg_s[col]

    lane_left = lax.broadcasted_iota(jnp.int32, (HS, WIDE), 1) < FEAT

    def pack(v):
        return jnp.where(lane_left, v[:HS], swap(v[HS:]))

    e0 = ei0[...].astype(F32)
    item0 = pack(jnp.concatenate([e0, jnp.zeros_like(e0)], axis=1))
    tbl0[core, q, z] = item0.astype(BF16)
    user0 = eu0[...].astype(F32)
    ed0[...] = jnp.transpose(jnp.concatenate([user0, user0], axis=0)).astype(BF16)
    pl.semaphore_wait(barrier, (C - 1) + (R - 1) + (X - 1) * (Y - 1))

    def gather_z(tbl, sem):
        each(1, Z, lambda k: remote(tbl.at[core, q, z], tbl.at[core, q, z], sem, row, ((z + k) % Z) * Y + y).start())

    def gather_q(tbl, sem):
        await_recv(tbl.at[core, q, pl.ds(0, Z - 1)], sem)
        each(1, Q, lambda k: remote(tbl.at[core, q], tbl.at[core, q], sem + 1, *at_q((q + k) % Q)).start())

    def gather_d(tbl, sem):
        await_recv(tbl.at[core, pl.ds(0, Q - 1)], sem + 1)
        remote(tbl.at[core], tbl.at[core], sem + 2, mate, col).start()

    def gather_end(tbl, sem):
        await_recv(tbl.at[core], sem + 2)

    def gather_sent(tbl, sem):
        await_send(tbl.at[core, q, pl.ds(0, Z - 1)], sem)
        await_send(tbl.at[core, pl.ds(0, Q - 1)], sem + 1)
        await_send(tbl.at[core], sem + 2)

    def rows_of(tbl, c):
        cz, cy = c // Y, c % Y
        parts = []
        for i in range(R):
            v = tbl[i % 2, cy * X + i // 2, cz].astype(F32)
            parts += [v, swap(v)]
        return jnp.concatenate(parts, axis=0).astype(BF16)

    def order(k):
        j = k // Y
        m = (j + 1) // 2
        odd = j % 2
        return (odd * m + (1 - odd) * (Z - m)) % Z, k % Y

    def target(k):
        dz, dy = order(k)
        return ((z + dz) % Z) * Y + (y + dy) % Y

    each(1, C, lambda k: remote(deg_s.at[(col + k) % C], deg_r.at[col], DEG, row, (col + k) % C).start())
    each(1, R, lambda k: remote(ideg.at[row], ideg.at[row], IDEG, (row + k) % R, col).start())
    gather_z(tbl0, GATHER0)
    await_recv(deg_r.at[pl.ds(0, C - 1)], DEG)
    own_deg[...] = lax.fori_loop(0, C, lambda k, t: t + deg_r[k], jnp.zeros((1, UD), F32), unroll=True)
    deg_f[col] = own_deg[...]
    each(1, C, lambda k: remote(own_deg, deg_f.at[col], SPREAD, row, target(k), recv=spread_recv.at[col]).start())
    await_recv(ideg.at[pl.ds(0, R - 1)], IDEG)
    scale_item = lax.rsqrt(jnp.maximum(lax.fori_loop(0, R, lambda k, t: t + ideg[k], jnp.zeros((1, IB), F32), unroll=True), 1.0))
    gather_q(tbl0, GATHER0)

    def piece(c):
        scale = lax.rsqrt(jnp.maximum(deg_f[c], 1.0))
        scale = jnp.transpose(jnp.broadcast_to(scale, (IB, UD)))
        return (mask[c].astype(F32) * scale * scale_item).astype(BF16)

    def ship(k):
        to = target(k)
        remote(send_a.at[to], slab.at[col], ATOA, row, to, recv=a2a_recv.at[col]).start()

    def make(k):
        to = target(k)
        remote(deg_f.at[to], deg_f.at[to], SPREAD, row, col, recv=spread_recv.at[to]).wait_recv()
        send_a[to] = piece(to)

    make(1)

    def make_and_ship(k):
        make(k)
        ship(k - 1)

    each(2, C, make_and_ship)
    slab[col] = piece(col)
    ship(C - 1)
    gather_d(tbl0, GATHER0)
    gather_end(tbl0, GATHER0)

    def scatter_a(n, g, ed):
        p, rd = rs[n][0], rs[n][1]
        per = Z // groups[n]

        def block(k):
            zi, cy = k // Y, k % Y
            val = jnp.dot(slab_t[(g * per + zi) * Y + cy], ed[...], preferred_element_type=F32)
            for i in range(R):
                p[i % 2, g, cy * X + i // 2, zi] = jnp.where(lane_left, val[i * SH:i * SH + HS], val[i * SH + HS:(i + 1) * SH])

        lax.fori_loop(0, per * Y, lambda k, t: (block(k), t)[1], 0, unroll=4)
        remote(p.at[1 - core, g], rd.at[g], base[n], mate, col, recv=recvs.at[base[n] + g]).start()

    def scatter_b(n, g):
        p, rd, s1, rxy, _, _ = rs[n]
        remote(rd.at[g], rd.at[g], base[n], row, col, recv=recvs.at[base[n] + g]).wait_recv()

        def fold(k):
            to = (q + k) % Q
            s1[g, to] = p[core, g, to] + rd[g, to]

        def go(k):
            to = (q + k) % Q
            remote(s1.at[g, to], rxy.at[g, q], base[n] + 1, *at_q(to), recv=recvs.at[base[n] + groups[n] + g]).start()

        def both(k):
            fold(k)
            go(k - 1)

        fold(1)
        each(2, Q, both)
        rxy[g, q] = p[core, g, q] + rd[g, q]
        go(Q - 1)

    def scatter_c(n, g):
        _, _, _, rxy, s2, rz = rs[n]
        per = Z // groups[n]
        part = rxy.at[g, pl.ds(0, Q - 1)]
        remote(part, part, base[n], row, col, recv=recvs.at[base[n] + groups[n] + g]).wait_recv()
        for zi in range(per):
            to = g * per + zi
            s2[to] = lax.fori_loop(1, Q, lambda k, t: t + rxy[g, k, zi], rxy[g, 0, zi], unroll=True)
        for zi in range(per):
            to = g * per + zi

            @pl.when(to != z)
            def _():
                remote(s2.at[to], rz.at[z], base[n] + 2, row, to * Y + y, recv=recvs.at[base[n] + 2 * groups[n]]).start()

            @pl.when(to == z)
            def _():
                rz[z] = s2[to]

    def scatter_end(n):
        rz = rs[n][5]
        part = rz.at[pl.ds(0, Z - 1)]
        remote(part, part, base[n], row, col, recv=recvs.at[base[n] + 2 * groups[n]]).wait_recv()
        return lax.fori_loop(1, Z, lambda k, t: t + rz[k], rz[0], unroll=True).astype(BF16)

    def scatter_sent(n):
        p, _, s1, _, s2, _ = rs[n]
        await_send(p.at[0], base[n])
        await_send(s1.at[:, pl.ds(0, Q - 1)], base[n] + 1)
        await_send(s2.at[pl.ds(0, Z - 1)], base[n] + 2)

    def remote1(src, dst, k, r, c, recv):
        return pltpu.make_async_remote_copy(
            src_ref=src, dst_ref=dst, send_sem=one_send.at[k], recv_sem=recv, device_id=(c, r), device_id_type=MESH)

    def await1(ref, recv):
        remote1(ref, ref, 0, row, col, recv).wait_recv()

    def first_a(g):
        def block(cy):
            val = jnp.dot(slab_t[g * Y + cy], ed0[...], preferred_element_type=F32)
            for i in range(R):
                p_1[i % 2, g, i // 2, cy] = jnp.where(lane_left, val[i * SH:i * SH + HS], val[i * SH + HS:(i + 1) * SH])

        lax.fori_loop(0, Y, lambda k, t: (block(k), t)[1], 0, unroll=4)
        remote1(p_1.at[1 - core, g], rd_1.at[g], 0, mate, col, one_d.at[g]).start()

    def first_b(g):
        await1(rd_1.at[g], one_d.at[g])
        for k in range(1, X):
            to = (x + k) % X
            s1_1[g, to] = p_1[core, g, to] + rd_1[g, to]
        rx_1[g, x] = p_1[core, g, x] + rd_1[g, x]
        for k in range(1, X):
            to = (x + k) % X
            remote1(s1_1.at[g, to], rx_1.at[g, x], 1, to * 2 + core, col, one_x.at[g]).start()

    def first_c(g):
        await1(rx_1.at[g, pl.ds(0, X - 1)], one_x.at[g])
        total = rx_1[g, 0]
        for k in range(1, X):
            total = total + rx_1[g, k]
        for cy in range(Y):
            sy_1[cy, g] = total[cy]

    def first_y():
        for k in range(1, Y):
            to = (y + k) % Y
            remote1(sy_1.at[to], ry_1.at[y], 2, row, z * Y + to, one_yz.at[0]).start()
        ry_1[y] = sy_1[y]

    def first_z():
        await1(ry_1.at[pl.ds(0, Y - 1)], one_yz.at[0])
        total = ry_1[0]
        for k in range(1, Y):
            total = total + ry_1[k]
        s2_1[...] = total
        rz_1[z] = s2_1[z]
        each(1, Z, lambda k: remote1(s2_1.at[(z + k) % Z], rz_1.at[z], 3, row, ((z + k) % Z) * Y + y, one_yz.at[1]).start())

    def first_end():
        await1(rz_1.at[pl.ds(0, Z - 1)], one_yz.at[1])
        return lax.fori_loop(1, Z, lambda k, t: t + rz_1[k], rz_1[0], unroll=True).astype(BF16)

    def first_sent():
        for k, ref in enumerate((p_1.at[0], s1_1.at[:, pl.ds(0, X - 1)], sy_1.at[pl.ds(0, Y - 1)], s2_1.at[pl.ds(0, Z - 1)])):
            remote1(ref, ref, k, row, col, one_yz.at[0]).wait_send()

    def source(k):
        dz, dy = order(k)
        return ((z - dz + Z) % Z) * Y + (y - dy + Y) % Y

    def use(c):
        blk = slab[c]
        slab_t[c] = jnp.transpose(blk)
        acc[...] += jnp.dot(blk, rows_of(tbl0, c), preferred_element_type=F32)

    def arrive(k):
        c = source(k)
        pltpu.make_async_remote_copy(src_ref=slab.at[c], dst_ref=slab.at[c], send_sem=sends.at[ATOA], recv_sem=a2a_recv.at[c],
                                     device_id=(col, row), device_id_type=MESH).wait_recv()
        use(c)

    def group(j):
        return source(j * Y) // Y

    acc[...] = jnp.zeros_like(acc)
    use(col)
    each(1, Y, arrive)
    first_a(z)

    def stream(j):
        each(j * Y, (j + 1) * Y, arrive)
        first_a(group(j))
        first_b(group(j - 1))

        @pl.when(j >= 2)
        def _():
            first_c(group(j - 2))

    each(1, Z, stream)
    wide_left = lax.broadcasted_iota(jnp.int32, (UD, WIDE), 1) < FEAT

    def twice(v):
        return jnp.where(wide_left, v, swap(v)).astype(BF16)

    user1 = acc[...].astype(BF16).astype(F32)
    ed1[...] = twice(user1)
    for g in range(G2):
        scatter_a(1, g, ed1)
        if g == 0:
            first_b(group(Z - 1))
        else:
            scatter_b(1, g - 1)
    scatter_b(1, G2 - 1)
    first_c(group(Z - 2))
    first_c(group(Z - 1))
    first_y()
    for g in range(G2 // 2):
        scatter_c(1, g)
    first_z()
    for g in range(G2 // 2, G2):
        scatter_c(1, g)
    item1 = first_end().astype(F32)
    item2 = scatter_end(1).astype(F32)
    low = jnp.where(lane_left, item1, swap(item2))
    high = jnp.where(lane_left, swap(item1), item2)
    tbl1[core, q, z] = jnp.concatenate([low, high], axis=0).astype(BF16)
    gather_z(tbl1, GATHER1)
    gather_q(tbl1, GATHER1)
    gather_d(tbl1, GATHER1)
    acc[...] = jnp.zeros_like(acc)
    gather_end(tbl1, GATHER1)

    def absorb(c):
        cz, cy = c // Y, c % Y
        rows = jnp.concatenate([tbl1[i % 2, cy * X + i // 2, cz] for i in range(R)], axis=0)
        acc[...] += jnp.dot(slab[c], rows, preferred_element_type=F32)

    lax.fori_loop(0, C, lambda k, t: (absorb(k), t)[1], 0, unroll=4)
    late = acc[...].astype(BF16).astype(F32)
    ed2[...] = twice(late)
    scatter_a(2, 0, ed2)
    sum_user = ((ed0[...].astype(F32) + ed1[...].astype(F32)) + ed2[...].astype(F32)) + jnp.where(wide_left, swap(late), late)
    user_rows = (sum_user / (LAYERS + 1)).astype(BF16)

    ids = lax.broadcasted_iota(jnp.int32, (UD, TRIPLES), 0) + (row * C + col) * UD
    hit = (ids == trip[0:1, :]).astype(BF16)
    found = lax.dot_general(hit, user_rows, (((0,), (0,)), ((), ())), preferred_element_type=F32)
    pick_left = lax.broadcasted_iota(jnp.int32, (PICKS, WIDE), 1) < FEAT
    for h in range(2):
        lo, hi = h * PICKS, (h + 2) * PICKS
        pk_a[h] = jnp.where(pick_left, found[lo:lo + PICKS], found[hi:hi + PICKS]).astype(BF16)
    remote(pk_a.at[1 - core], pk_b, PICK, mate, col).start()
    for g in range(1, G2):
        scatter_a(2, g, ed2)
        if g == 1:
            await_recv(pk_b, PICK)
            pk_z[z] = (pk_a[core].astype(F32) + pk_b[...].astype(F32)).astype(BF16)
            each(1, Z, lambda k: remote(pk_z.at[z], pk_z.at[z], PICK + 1, row, ((z + k) % Z) * Y + y).start())
        scatter_b(2, g - 1)
    scatter_b(2, G2 - 1)
    out_user[...] = jnp.transpose(user_rows.astype(F32))[:FEAT].astype(BF16)
    await_recv(pk_z.at[pl.ds(0, Z - 1)], PICK + 1)
    pk_q[q] = lax.fori_loop(1, Z, lambda k, t: t + pk_z[k].astype(F32), pk_z[0].astype(F32), unroll=True).astype(BF16)
    each(1, Q, lambda k: remote(pk_q.at[q], pk_q.at[q], PICK + 2, *at_q((q + k) % Q)).start())
    for g in range(G2):
        scatter_c(2, g)
    await_recv(pk_q.at[pl.ds(0, Q - 1)], PICK + 2)
    pk_d[core] = lax.fori_loop(1, Q, lambda k, t: t + pk_q[k].astype(F32), pk_q[0].astype(F32), unroll=True).astype(BF16)
    remote(pk_d.at[core], pk_d.at[core], PICK + 3, mate, col).start()
    item3 = scatter_end(2)
    sum_item = ((item0 + item1) + item2) + item3.astype(F32)
    packed = (sum_item / (LAYERS + 1)).astype(BF16).astype(F32)
    zero = jnp.zeros_like(packed)
    left_rows = [jnp.where(lane_left, packed, zero), jnp.where(lane_left, swap(packed), zero)]
    right_rows = [jnp.where(lane_left, zero, swap(packed)), jnp.where(lane_left, zero, packed)]
    item_rows = jnp.concatenate(left_rows, axis=0).astype(BF16)
    out_item[...] = item_rows[:, :FEAT]

    await_recv(pk_d.at[0], PICK + 3)
    user_vec = jnp.concatenate([pk_d[0], pk_d[1], pk_d[0], pk_d[1]], axis=0)
    nt = (((1,), (1,)), ((), ()))
    dots_l = lax.dot_general(item_rows, user_vec, nt, preferred_element_type=F32)
    dots_r = lax.dot_general(jnp.concatenate(right_rows, axis=0).astype(BF16), user_vec, nt, preferred_element_type=F32)
    dots = jnp.where(lax.broadcasted_iota(jnp.int32, (SH, TRIPLES), 1) < TRIPLES // 2, dots_l, dots_r)
    own = lax.broadcasted_iota(jnp.int32, (SH, TRIPLES), 0) + (col * R + row) * SH
    pos = jnp.sum(jnp.where(own == trip[1:2, :], dots, 0.0), axis=0, keepdims=True)
    neg = jnp.sum(jnp.where(own == trip[2:3, :], dots, 0.0), axis=0, keepdims=True)
    xc[col] = pos - neg
    each(1, C, lambda k: remote(xc.at[col], xc.at[col], MARGIN, row, (col + k) % C).start())
    await_recv(xc.at[pl.ds(0, C - 1)], MARGIN)
    xr[row] = lax.fori_loop(1, C, lambda k, t: t + xc[k], xc[0], unroll=True)
    each(1, R, lambda k: remote(xr.at[row], xr.at[row], MARGIN + 1, (row + k) % R, col).start())
    await_recv(xr.at[pl.ds(0, R - 1)], MARGIN + 1)
    margin = lax.fori_loop(1, R, lambda k, t: t + xr[k], xr[0], unroll=True)
    soft = jnp.maximum(-margin, 0.0) + jnp.log1p(jnp.exp(-jnp.abs(margin)))
    loss[...] = jnp.sum(soft, axis=1, keepdims=True) / TRIPLES

    await_send(deg_s.at[pl.ds(0, C - 1)], DEG)
    await_send(ideg.at[pl.ds(0, R - 1)], IDEG)
    await_send(deg_f.at[pl.ds(0, C - 1)], SPREAD)
    await_send(send_a.at[pl.ds(0, C - 1)], ATOA)
    gather_sent(tbl0, GATHER0)
    gather_sent(tbl1, GATHER1)
    first_sent()
    for n in (1, 2):
        scatter_sent(n)
    await_send(pk_b, PICK)
    await_send(pk_z.at[pl.ds(0, Z - 1)], PICK + 1)
    await_send(pk_q.at[pl.ds(0, Q - 1)], PICK + 2)
    await_send(pk_d.at[0], PICK + 3)
    await_send(xc.at[pl.ds(0, C - 1)], MARGIN)
    await_send(xr.at[pl.ds(0, R - 1)], MARGIN + 1)


def build(mesh, Y, SH, UD, G2):
    C, R = mesh.shape["col"], mesh.shape["row"]
    Z, X = C // Y, R // 2
    Q, IB, HS = Y * X, R * SH, SH // 2
    vm = pltpu.VMEM
    scratch = [
        vm((C, 1, UD), F32), vm((C, 1, UD), F32), vm((C, 1, UD), F32), vm((1, UD), F32), vm((R, 1, IB), F32),
        vm((C, UD, IB), BF16), vm((C, UD, IB), BF16), vm((C, IB, UD), BF16),
        vm((2, Q, Z, HS, WIDE), BF16), vm((2, Q, Z, SH, WIDE), BF16),
        vm((UD, WIDE), F32), vm((UD, WIDE), BF16), vm((UD, WIDE), BF16), vm((UD, WIDE), BF16),
        vm((2, PICKS, WIDE), BF16), vm((PICKS, WIDE), BF16),
        vm((Z, PICKS, WIDE), BF16), vm((Q, PICKS, WIDE), BF16), vm((2, PICKS, WIDE), BF16),
        vm((C, 1, TRIPLES), F32), vm((R, 1, TRIPLES), F32),
    ]
    count = SCATTER1 + 2 * (2 * G2 + 1)
    sem = pltpu.SemaphoreType.DMA
    scratch += [sem((count,)), sem((count,)), sem((C,)), vm((C, UD, IB), jnp.int32), sem((LOADS,))]
    scratch += [
        vm((2, Z, X, Y, HS, WIDE), F32), vm((Z, X, Y, HS, WIDE), F32), vm((Z, X, Y, HS, WIDE), F32), vm((Z, X, Y, HS, WIDE), F32),
        vm((Y, Z, HS, WIDE), F32), vm((Y, Z, HS, WIDE), F32), vm((Z, HS, WIDE), F32), vm((Z, HS, WIDE), F32),
        sem((4,)), sem((Z,)), sem((Z,)), sem((2,)),
    ]
    for g in (G2, G2):
        scratch += [vm((2, g, Q, Z // g, HS, WIDE), F32)] + [vm((g, Q, Z // g, HS, WIDE), F32)] * 3 + [vm((Z, HS, WIDE), F32)] * 2
    scratch += [sem((C,))]
    dims = (Z, Y, X, SH, UD, G2)

    def local_prog(mask_blk, user_shard, item_shard, triples):
        out_user, out_item, loss = pl.pallas_call(
            functools.partial(kernel, dims),
            out_shape=(
                jax.ShapeDtypeStruct((FEAT, UD), BF16),
                jax.ShapeDtypeStruct((SH, FEAT), BF16),
                jax.ShapeDtypeStruct((1, 1), F32),
            ),
            in_specs=[pl.BlockSpec(memory_space=pl.ANY)] + [pl.BlockSpec(memory_space=pltpu.VMEM)] * 3,
            out_specs=(pl.BlockSpec(memory_space=pltpu.VMEM),) * 3,
            scratch_shapes=scratch,
            compiler_params=pltpu.CompilerParams(
                collective_id=0, has_side_effects=True, vmem_limit_bytes=60 * 1024 * 1024),
            name="lightgcn",
        )(mask_blk.reshape(C, UD, IB), user_shard.T, item_shard, triples.T)
        return out_user.T, out_item, loss[0, 0]

    return jax.shard_map(
        local_prog, mesh=mesh,
        in_specs=(P("row", "col"), P(("row", "col"), None), P(("col", "row"), None), P(None, None)),
        out_specs=(P(("row", "col"), None), P(("col", "row"), None), P()), check_vma=False)


def solution(mesh):
    return build(mesh, Y=4, SH=16, UD=256, G2=4)
```

```python
import functools

import jax
import jax.numpy as jnp
from jax import lax
from jax.experimental import pallas as pl
from jax.experimental.pallas import tpu as pltpu
from jax.sharding import PartitionSpec as P

MESH = pl.DeviceIdType.MESH
F32 = jnp.float32
BF16 = jnp.bfloat16
FEAT = 64
WIDE = 2 * FEAT
TRIPLES = 128
LAYERS = 3
LOADS = 8
PICKS = TRIPLES // 4

DEG, IDEG, SPREAD, ATOA, GATHER0, GATHER1, PICK, MARGIN, SCATTER1 = 0, 1, 2, 3, 4, 7, 10, 14, 16


def swap(v):
    return pltpu.roll(v, FEAT, 1)


def kernel(dims, mask_hbm, eu0, ei0, trip, out_user, out_item, loss, *scratch):
    Z, Y, X, SH, UD, G2 = dims
    C, R, Q = Z * Y, 2 * X, Y * X
    IB = R * SH
    HS = SH // 2
    (deg_s, deg_r, deg_f, own_deg, ideg, send_a, slab, slab_t, tbl0, tbl1, acc, ed0, ed1, ed2, pk_a, pk_b, pk_z, pk_q, pk_d, xc, xr,
     sends, recvs, a2a_recv, mask, load_sem) = scratch[:26]
    spread_recv = scratch[50]
    groups = (Z, G2, G2)
    p_1, rd_1, s1_1, rx_1, sy_1, ry_1, s2_1, rz_1, one_send, one_d, one_x, one_yz = scratch[26:38]
    rs = [None] + [scratch[32 + 6 * n:38 + 6 * n] for n in (1, 2)]
    base = [SCATTER1]
    base.append(SCATTER1)
    for n in (1, 2):
        base.append(base[-1] + 2 * groups[n] + 1)
    row = lax.axis_index("row")
    col = lax.axis_index("col")
    core, x = row % 2, row // 2
    z, y = col // Y, col % Y
    q = y * X + x
    mate = x * 2 + (1 - core)

    def remote(src, dst, sem, r, c, recv=None):
        return pltpu.make_async_remote_copy(
            src_ref=src, dst_ref=dst, send_sem=sends.at[sem], recv_sem=recvs.at[sem] if recv is None else recv,
            device_id=(c, r), device_id_type=MESH)

    def await_recv(ref, sem):
        remote(ref, ref, sem, row, col).wait_recv()

    def await_send(ref, sem):
        remote(ref, ref, sem, row, col).wait_send()

    def at_q(p):
        return (p % X) * 2 + core, z * Y + p // X

    def each(lo, hi, fn):
        lax.fori_loop(lo, hi, lambda k, t: (fn(k), t)[1], 0)

    run = C // LOADS

    def load(i):
        part = pl.ds(i * run, run)
        return pltpu.make_async_copy(mask_hbm.at[part], mask.at[part], load_sem.at[i])

    for i in range(LOADS):
        load(i).start()

    barrier = pltpu.get_barrier_semaphore()

    def hail(c, r):
        pl.semaphore_signal(barrier, inc=1, device_id=(c, r), device_id_type=MESH)

    each(1, C, lambda k: hail((col + k) % C, row))
    each(1, Y, lambda k: hail(z * Y + (y + k) % Y, mate))
    each(1, R, lambda k: hail(col, (row + k) % R))
    def hail_diagonal(k):
        i = k // 2
        hail(z * Y + (y + 1 + i // (X - 1)) % Y, ((x + 1 + i % (X - 1)) % X) * 2 + k % 2)

    each(0, 2 * (X - 1) * (Y - 1), hail_diagonal)

    ones = jnp.ones((8, IB), BF16)

    def count(k, part):
        blk = mask[k].astype(F32)
        sums = lax.dot_general(ones, blk.astype(BF16), (((1,), (1,)), ((), ())), preferred_element_type=F32)
        deg_s[k] = sums[0:1]
        return part + jnp.sum(blk.reshape(UD // 8, 8, IB), axis=0)

    part = jnp.zeros((8, IB), F32)
    for i in range(LOADS):
        load(i).wait()
        part = lax.fori_loop(i * run, (i + 1) * run, count, part, unroll=True)
    ideg[row] = jnp.sum(part, axis=0, keepdims=True)
    deg_r[col] = deg_s[col]

    lane_left = lax.broadcasted_iota(jnp.int32, (HS, WIDE), 1) < FEAT

    def pack(v):
        return jnp.where(lane_left, v[:HS], swap(v[HS:]))

    e0 = ei0[...].astype(F32)
    item0 = pack(jnp.concatenate([e0, jnp.zeros_like(e0)], axis=1))
    tbl0[core, q, z] = item0.astype(BF16)
    user0 = eu0[...].astype(F32)
    ed0[...] = jnp.transpose(jnp.concatenate([user0, user0], axis=0)).astype(BF16)
    pl.semaphore_wait(barrier, (C - 1) + (Y - 1) + (R - 1) + 2 * (X - 1) * (Y - 1))

    def gather_z(tbl, sem):
        each(1, Z, lambda k: remote(tbl.at[core, q, z], tbl.at[core, q, z], sem, row, ((z + k) % Z) * Y + y).start())

    def gather_q(tbl, sem):
        await_recv(tbl.at[core, q, pl.ds(0, Z - 1)], sem)
        each(1, Q, lambda k: remote(tbl.at[core, q], tbl.at[core, q], sem + 1, *at_q((q + k) % Q)).start())

    def gather_d(tbl, sem):
        await_recv(tbl.at[core, pl.ds(0, Q - 1)], sem + 1)
        remote(tbl.at[core], tbl.at[core], sem + 2, mate, col).start()

    def gather_end(tbl, sem):
        await_recv(tbl.at[core], sem + 2)

    def gather_sent(tbl, sem):
        await_send(tbl.at[core, q, pl.ds(0, Z - 1)], sem)
        await_send(tbl.at[core, pl.ds(0, Q - 1)], sem + 1)
        await_send(tbl.at[core], sem + 2)

    def rows_of(tbl, c):
        cz, cy = c // Y, c % Y
        parts = []
        for i in range(R):
            v = tbl[i % 2, cy * X + i // 2, cz].astype(F32)
            parts += [v, swap(v)]
        return jnp.concatenate(parts, axis=0).astype(BF16)

    def order(k):
        j = k // Y
        m = (j + 1) // 2
        odd = j % 2
        return (odd * m + (1 - odd) * (Z - m)) % Z, k % Y

    def target(k):
        dz, dy = order(k)
        return ((z + dz) % Z) * Y + (y + dy) % Y

    each(1, C, lambda k: remote(deg_s.at[(col + k) % C], deg_r.at[col], DEG, row, (col + k) % C).start())
    each(1, R, lambda k: remote(ideg.at[row], ideg.at[row], IDEG, (row + k) % R, col).start())
    gather_z(tbl0, GATHER0)
    await_recv(deg_r.at[pl.ds(0, C - 1)], DEG)
    own_deg[...] = lax.fori_loop(0, C, lambda k, t: t + deg_r[k], jnp.zeros((1, UD), F32), unroll=True)
    deg_f[col] = own_deg[...]
    each(1, C, lambda k: remote(own_deg, deg_f.at[col], SPREAD, row, target(k), recv=spread_recv.at[col]).start())
    await_recv(ideg.at[pl.ds(0, R - 1)], IDEG)
    scale_item = lax.rsqrt(jnp.maximum(lax.fori_loop(0, R, lambda k, t: t + ideg[k], jnp.zeros((1, IB), F32), unroll=True), 1.0))
    gather_q(tbl0, GATHER0)

    def piece(c):
        scale = lax.rsqrt(jnp.maximum(deg_f[c], 1.0))
        scale = jnp.transpose(jnp.broadcast_to(scale, (IB, UD)))
        return (mask[c].astype(F32) * scale * scale_item).astype(BF16)

    def ship(k):
        to = target(k)
        remote(send_a.at[to], slab.at[col], ATOA, row, to, recv=a2a_recv.at[col]).start()

    def make(k):
        to = target(k)
        remote(deg_f.at[to], deg_f.at[to], SPREAD, row, col, recv=spread_recv.at[to]).wait_recv()
        send_a[to] = piece(to)

    make(1)

    def make_and_ship(k):
        make(k)
        ship(k - 1)

    each(2, C, make_and_ship)
    slab[col] = piece(col)
    ship(C - 1)
    gather_d(tbl0, GATHER0)
    gather_end(tbl0, GATHER0)

    def scatter_a(n, g, ed):
        p, rd = rs[n][0], rs[n][1]
        per = Z // groups[n]

        def block(k):
            zi, cy = k // Y, k % Y
            val = jnp.dot(slab_t[(g * per + zi) * Y + cy], ed[...], preferred_element_type=F32)
            for i in range(R):
                p[i % 2, g, cy * X + i // 2, zi] = jnp.where(lane_left, val[i * SH:i * SH + HS], val[i * SH + HS:(i + 1) * SH])

        lax.fori_loop(0, per * Y, lambda k, t: (block(k), t)[1], 0, unroll=4)
        remote(p.at[1 - core, g], rd.at[g], base[n], mate, col, recv=recvs.at[base[n] + g]).start()

    def scatter_b(n, g):
        p, rd, s1, rxy, _, _ = rs[n]
        remote(rd.at[g], rd.at[g], base[n], row, col, recv=recvs.at[base[n] + g]).wait_recv()

        def fold(k):
            to = (q + k) % Q
            s1[g, to] = p[core, g, to] + rd[g, to]

        def go(k):
            to = (q + k) % Q
            remote(s1.at[g, to], rxy.at[g, q], base[n] + 1, *at_q(to), recv=recvs.at[base[n] + groups[n] + g]).start()

        def both(k):
            fold(k)
            go(k - 1)

        fold(1)
        each(2, Q, both)
        rxy[g, q] = p[core, g, q] + rd[g, q]
        go(Q - 1)

    def scatter_c(n, g):
        _, _, _, rxy, s2, rz = rs[n]
        per = Z // groups[n]
        part = rxy.at[g, pl.ds(0, Q - 1)]
        remote(part, part, base[n], row, col, recv=recvs.at[base[n] + groups[n] + g]).wait_recv()
        for zi in range(per):
            to = g * per + zi
            s2[to] = lax.fori_loop(1, Q, lambda k, t: t + rxy[g, k, zi], rxy[g, 0, zi], unroll=True)
        for zi in range(per):
            to = g * per + zi

            @pl.when(to != z)
            def _():
                remote(s2.at[to], rz.at[z], base[n] + 2, row, to * Y + y, recv=recvs.at[base[n] + 2 * groups[n]]).start()

            @pl.when(to == z)
            def _():
                rz[z] = s2[to]

    def scatter_end(n):
        rz = rs[n][5]
        part = rz.at[pl.ds(0, Z - 1)]
        remote(part, part, base[n], row, col, recv=recvs.at[base[n] + 2 * groups[n]]).wait_recv()
        return lax.fori_loop(1, Z, lambda k, t: t + rz[k], rz[0], unroll=True).astype(BF16)

    def scatter_sent(n):
        p, _, s1, _, s2, _ = rs[n]
        await_send(p.at[0], base[n])
        await_send(s1.at[:, pl.ds(0, Q - 1)], base[n] + 1)
        await_send(s2.at[pl.ds(0, Z - 1)], base[n] + 2)

    def remote1(src, dst, k, r, c, recv):
        return pltpu.make_async_remote_copy(
            src_ref=src, dst_ref=dst, send_sem=one_send.at[k], recv_sem=recv, device_id=(c, r), device_id_type=MESH)

    def await1(ref, recv):
        remote1(ref, ref, 0, row, col, recv).wait_recv()

    def first_a(g):
        def block(cy):
            val = jnp.dot(slab_t[g * Y + cy], ed0[...], preferred_element_type=F32)
            for i in range(R):
                p_1[i % 2, g, i // 2, cy] = jnp.where(lane_left, val[i * SH:i * SH + HS], val[i * SH + HS:(i + 1) * SH])

        lax.fori_loop(0, Y, lambda k, t: (block(k), t)[1], 0, unroll=4)
        remote1(p_1.at[1 - core, g], rd_1.at[g], 0, mate, col, one_d.at[g]).start()

    def first_b(g):
        await1(rd_1.at[g], one_d.at[g])
        for k in range(1, X):
            to = (x + k) % X
            s1_1[g, to] = p_1[core, g, to] + rd_1[g, to]
        rx_1[g, x] = p_1[core, g, x] + rd_1[g, x]
        for k in range(1, X):
            to = (x + k) % X
            remote1(s1_1.at[g, to], rx_1.at[g, x], 1, to * 2 + core, col, one_x.at[g]).start()

    def first_c(g):
        await1(rx_1.at[g, pl.ds(0, X - 1)], one_x.at[g])
        total = rx_1[g, 0]
        for k in range(1, X):
            total = total + rx_1[g, k]
        for cy in range(Y):
            sy_1[cy, g] = total[cy]

    def first_y():
        for k in range(1, Y):
            to = (y + k) % Y
            remote1(sy_1.at[to], ry_1.at[y], 2, row, z * Y + to, one_yz.at[0]).start()
        ry_1[y] = sy_1[y]

    def first_z():
        await1(ry_1.at[pl.ds(0, Y - 1)], one_yz.at[0])
        total = ry_1[0]
        for k in range(1, Y):
            total = total + ry_1[k]
        s2_1[...] = total
        rz_1[z] = s2_1[z]
        each(1, Z, lambda k: remote1(s2_1.at[(z + k) % Z], rz_1.at[z], 3, row, ((z + k) % Z) * Y + y, one_yz.at[1]).start())

    def first_end():
        await1(rz_1.at[pl.ds(0, Z - 1)], one_yz.at[1])
        return lax.fori_loop(1, Z, lambda k, t: t + rz_1[k], rz_1[0], unroll=True).astype(BF16)

    def first_sent():
        for k, ref in enumerate((p_1.at[0], s1_1.at[:, pl.ds(0, X - 1)], sy_1.at[pl.ds(0, Y - 1)], s2_1.at[pl.ds(0, Z - 1)])):
            remote1(ref, ref, k, row, col, one_yz.at[0]).wait_send()

    def source(k):
        dz, dy = order(k)
        return ((z - dz + Z) % Z) * Y + (y - dy + Y) % Y

    def use(c):
        blk = slab[c]
        slab_t[c] = jnp.transpose(blk)
        acc[...] += jnp.dot(blk, rows_of(tbl0, c), preferred_element_type=F32)

    def arrive(k):
        c = source(k)
        pltpu.make_async_remote_copy(src_ref=slab.at[c], dst_ref=slab.at[c], send_sem=sends.at[ATOA], recv_sem=a2a_recv.at[c],
                                     device_id=(col, row), device_id_type=MESH).wait_recv()
        use(c)

    def group(j):
        return source(j * Y) // Y

    acc[...] = jnp.zeros_like(acc)
    use(col)
    each(1, Y, arrive)
    first_a(z)

    def stream(j):
        each(j * Y, (j + 1) * Y, arrive)
        first_a(group(j))
        first_b(group(j - 1))

        @pl.when(j >= 2)
        def _():
            first_c(group(j - 2))

    each(1, Z, stream)
    wide_left = lax.broadcasted_iota(jnp.int32, (UD, WIDE), 1) < FEAT

    def twice(v):
        return jnp.where(wide_left, v, swap(v)).astype(BF16)

    user1 = acc[...].astype(BF16).astype(F32)
    ed1[...] = twice(user1)
    for g in range(G2):
        scatter_a(1, g, ed1)
        if g == 0:
            first_b(group(Z - 1))
        else:
            scatter_b(1, g - 1)
    scatter_b(1, G2 - 1)
    first_c(group(Z - 2))
    first_c(group(Z - 1))
    first_y()
    for g in range(G2 // 2):
        scatter_c(1, g)
    first_z()
    for g in range(G2 // 2, G2):
        scatter_c(1, g)
    item1 = first_end().astype(F32)
    item2 = scatter_end(1).astype(F32)
    low = jnp.where(lane_left, item1, swap(item2))
    high = jnp.where(lane_left, swap(item1), item2)
    tbl1[core, q, z] = jnp.concatenate([low, high], axis=0).astype(BF16)
    gather_z(tbl1, GATHER1)
    gather_q(tbl1, GATHER1)
    gather_d(tbl1, GATHER1)
    acc[...] = jnp.zeros_like(acc)
    gather_end(tbl1, GATHER1)

    def absorb(c):
        cz, cy = c // Y, c % Y
        rows = jnp.concatenate([tbl1[i % 2, cy * X + i // 2, cz] for i in range(R)], axis=0)
        acc[...] += jnp.dot(slab[c], rows, preferred_element_type=F32)

    lax.fori_loop(0, C, lambda k, t: (absorb(k), t)[1], 0, unroll=4)
    late = acc[...].astype(BF16).astype(F32)
    ed2[...] = twice(late)
    scatter_a(2, 0, ed2)
    sum_user = ((ed0[...].astype(F32) + ed1[...].astype(F32)) + ed2[...].astype(F32)) + jnp.where(wide_left, swap(late), late)
    user_rows = (sum_user / (LAYERS + 1)).astype(BF16)

    ids = lax.broadcasted_iota(jnp.int32, (UD, TRIPLES), 0) + (row * C + col) * UD
    hit = (ids == trip[0:1, :]).astype(BF16)
    found = lax.dot_general(hit, user_rows, (((0,), (0,)), ((), ())), preferred_element_type=F32)
    pick_left = lax.broadcasted_iota(jnp.int32, (PICKS, WIDE), 1) < FEAT
    for h in range(2):
        lo, hi = h * PICKS, (h + 2) * PICKS
        pk_a[h] = jnp.where(pick_left, found[lo:lo + PICKS], found[hi:hi + PICKS]).astype(BF16)
    remote(pk_a.at[1 - core], pk_b, PICK, mate, col).start()
    for g in range(1, G2):
        scatter_a(2, g, ed2)
        if g == 1:
            await_recv(pk_b, PICK)
            pk_z[z] = (pk_a[core].astype(F32) + pk_b[...].astype(F32)).astype(BF16)
            each(1, Z, lambda k: remote(pk_z.at[z], pk_z.at[z], PICK + 1, row, ((z + k) % Z) * Y + y).start())
        scatter_b(2, g - 1)
    scatter_b(2, G2 - 1)
    out_user[...] = jnp.transpose(user_rows.astype(F32))[:FEAT].astype(BF16)
    await_recv(pk_z.at[pl.ds(0, Z - 1)], PICK + 1)
    pk_q[q] = lax.fori_loop(1, Z, lambda k, t: t + pk_z[k].astype(F32), pk_z[0].astype(F32), unroll=True).astype(BF16)
    each(1, Q, lambda k: remote(pk_q.at[q], pk_q.at[q], PICK + 2, *at_q((q + k) % Q)).start())
    for g in range(G2):
        scatter_c(2, g)
    await_recv(pk_q.at[pl.ds(0, Q - 1)], PICK + 2)
    pk_d[core] = lax.fori_loop(1, Q, lambda k, t: t + pk_q[k].astype(F32), pk_q[0].astype(F32), unroll=True).astype(BF16)
    remote(pk_d.at[core], pk_d.at[core], PICK + 3, mate, col).start()
    item3 = scatter_end(2)
    sum_item = ((item0 + item1) + item2) + item3.astype(F32)
    packed = (sum_item / (LAYERS + 1)).astype(BF16).astype(F32)
    zero = jnp.zeros_like(packed)
    left_rows = [jnp.where(lane_left, packed, zero), jnp.where(lane_left, swap(packed), zero)]
    right_rows = [jnp.where(lane_left, zero, swap(packed)), jnp.where(lane_left, zero, packed)]
    item_rows = jnp.concatenate(left_rows, axis=0).astype(BF16)
    out_item[...] = item_rows[:, :FEAT]

    await_recv(pk_d.at[0], PICK + 3)
    user_vec = jnp.concatenate([pk_d[0], pk_d[1], pk_d[0], pk_d[1]], axis=0)
    nt = (((1,), (1,)), ((), ()))
    dots_l = lax.dot_general(item_rows, user_vec, nt, preferred_element_type=F32)
    dots_r = lax.dot_general(jnp.concatenate(right_rows, axis=0).astype(BF16), user_vec, nt, preferred_element_type=F32)
    dots = jnp.where(lax.broadcasted_iota(jnp.int32, (SH, TRIPLES), 1) < TRIPLES // 2, dots_l, dots_r)
    own = lax.broadcasted_iota(jnp.int32, (SH, TRIPLES), 0) + (col * R + row) * SH
    pos = jnp.sum(jnp.where(own == trip[1:2, :], dots, 0.0), axis=0, keepdims=True)
    neg = jnp.sum(jnp.where(own == trip[2:3, :], dots, 0.0), axis=0, keepdims=True)
    mine = q * 2 + core
    xc[mine] = pos - neg

    def spread_margin(k):
        to = (mine + k) % (2 * Q)
        remote(xc.at[mine], xc.at[mine], MARGIN, ((to // 2) % X) * 2 + to % 2, z * Y + to // (2 * X)).start()

    each(1, 2 * Q, spread_margin)
    await_recv(xc.at[pl.ds(0, 2 * Q - 1)], MARGIN)
    xr[z] = lax.fori_loop(1, 2 * Q, lambda k, t: t + xc[k], xc[0], unroll=True)
    each(1, Z, lambda k: remote(xr.at[z], xr.at[z], MARGIN + 1, row, ((z + k) % Z) * Y + y).start())
    await_recv(xr.at[pl.ds(0, Z - 1)], MARGIN + 1)
    margin = lax.fori_loop(1, Z, lambda k, t: t + xr[k], xr[0], unroll=True)
    soft = jnp.maximum(-margin, 0.0) + jnp.log1p(jnp.exp(-jnp.abs(margin)))
    loss[...] = jnp.sum(soft, axis=1, keepdims=True) / TRIPLES

    await_send(deg_s.at[pl.ds(0, C - 1)], DEG)
    await_send(ideg.at[pl.ds(0, R - 1)], IDEG)
    await_send(deg_f.at[pl.ds(0, C - 1)], SPREAD)
    await_send(send_a.at[pl.ds(0, C - 1)], ATOA)
    gather_sent(tbl0, GATHER0)
    gather_sent(tbl1, GATHER1)
    first_sent()
    for n in (1, 2):
        scatter_sent(n)
    await_send(pk_b, PICK)
    await_send(pk_z.at[pl.ds(0, Z - 1)], PICK + 1)
    await_send(pk_q.at[pl.ds(0, Q - 1)], PICK + 2)
    await_send(pk_d.at[0], PICK + 3)
    await_send(xc.at[pl.ds(0, 2 * Q - 1)], MARGIN)
    await_send(xr.at[pl.ds(0, Z - 1)], MARGIN + 1)


def emit(user_in, item_in, loss_in, user_out, item_out, loss_out):
    user_out[...] = user_in[...]
    item_out[...] = item_in[...]
    loss_out[...] = loss_in[...]


def build(mesh, Y, SH, UD, G2):
    C, R = mesh.shape["col"], mesh.shape["row"]
    Z, X = C // Y, R // 2
    Q, IB, HS = Y * X, R * SH, SH // 2
    vm = pltpu.VMEM
    scratch = [
        vm((C, 1, UD), F32), vm((C, 1, UD), F32), vm((C, 1, UD), F32), vm((1, UD), F32), vm((R, 1, IB), F32),
        vm((C, UD, IB), BF16), vm((C, UD, IB), BF16), vm((C, IB, UD), BF16),
        vm((2, Q, Z, HS, WIDE), BF16), vm((2, Q, Z, SH, WIDE), BF16),
        vm((UD, WIDE), F32), vm((UD, WIDE), BF16), vm((UD, WIDE), BF16), vm((UD, WIDE), BF16),
        vm((2, PICKS, WIDE), BF16), vm((PICKS, WIDE), BF16),
        vm((Z, PICKS, WIDE), BF16), vm((Q, PICKS, WIDE), BF16), vm((2, PICKS, WIDE), BF16),
        vm((2 * Q, 1, TRIPLES), F32), vm((Z, 1, TRIPLES), F32),
    ]
    count = SCATTER1 + 2 * (2 * G2 + 1)
    sem = pltpu.SemaphoreType.DMA
    scratch += [sem((count,)), sem((count,)), sem((C,)), vm((C, UD, IB), jnp.int32), sem((LOADS,))]
    scratch += [
        vm((2, Z, X, Y, HS, WIDE), F32), vm((Z, X, Y, HS, WIDE), F32), vm((Z, X, Y, HS, WIDE), F32), vm((Z, X, Y, HS, WIDE), F32),
        vm((Y, Z, HS, WIDE), F32), vm((Y, Z, HS, WIDE), F32), vm((Z, HS, WIDE), F32), vm((Z, HS, WIDE), F32),
        sem((4,)), sem((Z,)), sem((Z,)), sem((2,)),
    ]
    for g in (G2, G2):
        scratch += [vm((2, g, Q, Z // g, HS, WIDE), F32)] + [vm((g, Q, Z // g, HS, WIDE), F32)] * 3 + [vm((Z, HS, WIDE), F32)] * 2
    scratch += [sem((C,))]
    dims = (Z, Y, X, SH, UD, G2)

    def local_prog(mask_blk, user_shard, item_shard, triples):
        out_user, out_item, loss = pl.pallas_call(
            functools.partial(kernel, dims),
            out_shape=(
                jax.ShapeDtypeStruct((FEAT, UD), BF16),
                jax.ShapeDtypeStruct((SH, FEAT), BF16),
                jax.ShapeDtypeStruct((1, 1), F32),
            ),
            in_specs=[pl.BlockSpec(memory_space=pl.ANY)] + [pl.BlockSpec(memory_space=pltpu.VMEM)] * 3,
            out_specs=(pl.BlockSpec(memory_space=pltpu.VMEM),) * 3,
            scratch_shapes=scratch,
            compiler_params=pltpu.CompilerParams(
                collective_id=0, has_side_effects=True, vmem_limit_bytes=60 * 1024 * 1024),
            name="lightgcn",
        )(mask_blk.reshape(C, UD, IB), user_shard.T, item_shard, triples.T)
        out_user, out_item, loss = pl.pallas_call(
            emit,
            out_shape=(
                jax.ShapeDtypeStruct((FEAT, UD), BF16),
                jax.ShapeDtypeStruct((SH, FEAT), BF16),
                jax.ShapeDtypeStruct((1, 1), F32),
            ),
            in_specs=[pl.BlockSpec(memory_space=pltpu.VMEM)] * 3,
            out_specs=(pl.BlockSpec(memory_space=pltpu.VMEM),) * 3,
            name="emit",
        )(out_user, out_item, loss)
        return out_user.T, out_item, loss[0, 0]

    return jax.shard_map(
        local_prog, mesh=mesh,
        in_specs=(P("row", "col"), P(("row", "col"), None), P(("col", "row"), None), P(None, None)),
        out_specs=(P(("row", "col"), None), P(("col", "row"), None), P()), check_vma=False)


def solution(mesh):
    return build(mesh, Y=4, SH=16, UD=256, G2=4)
```

```python
import functools

import jax
import jax.numpy as jnp
from jax import lax
from jax.experimental import pallas as pl
from jax.experimental.pallas import tpu as pltpu
from jax.sharding import PartitionSpec as P

MESH = pl.DeviceIdType.MESH
F32 = jnp.float32
BF16 = jnp.bfloat16
FEAT = 64
WIDE = 2 * FEAT
TRIPLES = 128
LAYERS = 3
LOADS = 8
PICKS = TRIPLES // 4

DEG, IDEG, SPREAD, ATOA, GATHER0, GATHER1, PICK, MARGIN, SCATTER1 = 0, 1, 2, 3, 4, 7, 10, 14, 16


def swap(v):
    return pltpu.roll(v, FEAT, 1)


def kernel(dims, mask_hbm, eu0, ei0, trip, out_user, out_item, loss, *scratch):
    Z, Y, X, SH, UD, G2 = dims
    C, R, Q = Z * Y, 2 * X, Y * X
    IB = R * SH
    HS = SH // 2
    (deg_s, deg_r, deg_f, own_deg, ideg, send_a, slab, slab_t, tbl0, tbl1, acc, ed0, ed1, ed2, pk_a, pk_b, pk_z, pk_q, pk_d, xc, xr,
     sends, recvs, a2a_recv, mask, load_sem) = scratch[:26]
    spread_recv = scratch[50]
    groups = (Z, G2, G2)
    p_1, rd_1, s1_1, rx_1, sy_1, ry_1, s2_1, rz_1, one_send, one_d, one_x, one_yz = scratch[26:38]
    rs = [None] + [scratch[32 + 6 * n:38 + 6 * n] for n in (1, 2)]
    base = [SCATTER1]
    base.append(SCATTER1)
    for n in (1, 2):
        base.append(base[-1] + 2 * groups[n] + 1)
    row = lax.axis_index("row")
    col = lax.axis_index("col")
    core, x = row % 2, row // 2
    z, y = col // Y, col % Y
    q = y * X + x
    mate = x * 2 + (1 - core)

    def remote(src, dst, sem, r, c, recv=None):
        return pltpu.make_async_remote_copy(
            src_ref=src, dst_ref=dst, send_sem=sends.at[sem], recv_sem=recvs.at[sem] if recv is None else recv,
            device_id=(c, r), device_id_type=MESH)

    def await_recv(ref, sem):
        remote(ref, ref, sem, row, col).wait_recv()

    def await_send(ref, sem):
        remote(ref, ref, sem, row, col).wait_send()

    def at_q(p):
        return (p % X) * 2 + core, z * Y + p // X

    def each(lo, hi, fn):
        lax.fori_loop(lo, hi, lambda k, t: (fn(k), t)[1], 0)

    run = C // LOADS

    def load(i):
        part = pl.ds(i * run, run)
        return pltpu.make_async_copy(mask_hbm.at[part], mask.at[part], load_sem.at[i])

    for i in range(LOADS):
        load(i).start()

    barrier = pltpu.get_barrier_semaphore()

    def hail(c, r):
        pl.semaphore_signal(barrier, inc=1, device_id=(c, r), device_id_type=MESH)

    each(1, C, lambda k: hail((col + k) % C, row))
    each(1, Y, lambda k: hail(z * Y + (y + k) % Y, mate))
    each(1, R, lambda k: hail(col, (row + k) % R))
    def hail_diagonal(k):
        i = k // 2
        hail(z * Y + (y + 1 + i // (X - 1)) % Y, ((x + 1 + i % (X - 1)) % X) * 2 + k % 2)

    each(0, 2 * (X - 1) * (Y - 1), hail_diagonal)

    ones = jnp.ones((8, IB), BF16)

    def count(k, part):
        blk = mask[k].astype(F32)
        sums = lax.dot_general(ones, blk.astype(BF16), (((1,), (1,)), ((), ())), preferred_element_type=F32)
        deg_s[k] = sums[0:1]
        return part + jnp.sum(blk.reshape(UD // 8, 8, IB), axis=0)

    part = jnp.zeros((8, IB), F32)
    for i in range(LOADS):
        load(i).wait()
        part = lax.fori_loop(i * run, (i + 1) * run, count, part, unroll=True)
    ideg[row] = jnp.sum(part, axis=0, keepdims=True)
    deg_r[col] = deg_s[col]

    lane_left = lax.broadcasted_iota(jnp.int32, (HS, WIDE), 1) < FEAT

    def pack(v):
        return jnp.where(lane_left, v[:HS], swap(v[HS:]))

    e0 = ei0[...].astype(F32)
    item0 = pack(jnp.concatenate([e0, jnp.zeros_like(e0)], axis=1))
    tbl0[core, q, z] = item0.astype(BF16)
    user0 = eu0[...].astype(F32)
    ed0[...] = jnp.transpose(jnp.concatenate([user0, user0], axis=0)).astype(BF16)
    pl.semaphore_wait(barrier, (C - 1) + (Y - 1) + (R - 1) + 2 * (X - 1) * (Y - 1))

    def gather_z(tbl, sem):
        each(1, Z, lambda k: remote(tbl.at[core, q, z], tbl.at[core, q, z], sem, row, ((z + k) % Z) * Y + y).start())

    def gather_q(tbl, sem):
        await_recv(tbl.at[core, q, pl.ds(0, Z - 1)], sem)
        each(1, Q, lambda k: remote(tbl.at[core, q], tbl.at[core, q], sem + 1, *at_q((q + k) % Q)).start())

    def gather_d(tbl, sem):
        await_recv(tbl.at[core, pl.ds(0, Q - 1)], sem + 1)
        remote(tbl.at[core], tbl.at[core], sem + 2, mate, col).start()

    def gather_end(tbl, sem):
        await_recv(tbl.at[core], sem + 2)

    def gather_sent(tbl, sem):
        await_send(tbl.at[core, q, pl.ds(0, Z - 1)], sem)
        await_send(tbl.at[core, pl.ds(0, Q - 1)], sem + 1)
        await_send(tbl.at[core], sem + 2)

    def rows_of(tbl, c):
        cz, cy = c // Y, c % Y
        parts = []
        for i in range(R):
            v = tbl[i % 2, cy * X + i // 2, cz].astype(F32)
            parts += [v, swap(v)]
        return jnp.concatenate(parts, axis=0).astype(BF16)

    def order(k):
        j = k // Y
        m = (j + 1) // 2
        odd = j % 2
        return (odd * m + (1 - odd) * (Z - m)) % Z, k % Y

    def target(k):
        dz, dy = order(k)
        return ((z + dz) % Z) * Y + (y + dy) % Y

    each(1, C, lambda k: remote(deg_s.at[(col + k) % C], deg_r.at[col], DEG, row, (col + k) % C).start())
    each(1, R, lambda k: remote(ideg.at[row], ideg.at[row], IDEG, (row + k) % R, col).start())
    gather_z(tbl0, GATHER0)
    await_recv(deg_r.at[pl.ds(0, C - 1)], DEG)
    own_deg[...] = lax.fori_loop(0, C, lambda k, t: t + deg_r[k], jnp.zeros((1, UD), F32), unroll=True)
    deg_f[col] = own_deg[...]
    each(1, C, lambda k: remote(own_deg, deg_f.at[col], SPREAD, row, target(k), recv=spread_recv.at[col]).start())
    await_recv(ideg.at[pl.ds(0, R - 1)], IDEG)
    scale_item = lax.rsqrt(jnp.maximum(lax.fori_loop(0, R, lambda k, t: t + ideg[k], jnp.zeros((1, IB), F32), unroll=True), 1.0))
    gather_q(tbl0, GATHER0)

    def piece(c):
        scale = lax.rsqrt(jnp.maximum(deg_f[c], 1.0))
        scale = jnp.transpose(jnp.broadcast_to(scale, (IB, UD)))
        return (mask[c].astype(F32) * scale * scale_item).astype(BF16)

    def ship(k):
        to = target(k)
        remote(send_a.at[to], slab.at[col], ATOA, row, to, recv=a2a_recv.at[col]).start()

    def make(k):
        to = target(k)
        remote(deg_f.at[to], deg_f.at[to], SPREAD, row, col, recv=spread_recv.at[to]).wait_recv()
        send_a[to] = piece(to)

    make(1)

    def make_and_ship(k):
        make(k)
        ship(k - 1)

    each(2, C, make_and_ship)
    slab[col] = piece(col)
    ship(C - 1)
    gather_d(tbl0, GATHER0)
    gather_end(tbl0, GATHER0)

    def scatter_a(n, g, ed):
        p, rd = rs[n][0], rs[n][1]
        per = Z // groups[n]

        def block(k):
            zi, cy = k // Y, k % Y
            val = jnp.dot(slab_t[(g * per + zi) * Y + cy], ed[...], preferred_element_type=F32)
            for i in range(R):
                p[i % 2, g, cy * X + i // 2, zi] = jnp.where(lane_left, val[i * SH:i * SH + HS], val[i * SH + HS:(i + 1) * SH])

        lax.fori_loop(0, per * Y, lambda k, t: (block(k), t)[1], 0, unroll=4)
        remote(p.at[1 - core, g], rd.at[g], base[n], mate, col, recv=recvs.at[base[n] + g]).start()

    def scatter_b(n, g):
        p, rd, s1, rxy, _, _ = rs[n]
        remote(rd.at[g], rd.at[g], base[n], row, col, recv=recvs.at[base[n] + g]).wait_recv()

        def fold(k):
            to = (q + k) % Q
            s1[g, to] = p[core, g, to] + rd[g, to]

        def go(k):
            to = (q + k) % Q
            remote(s1.at[g, to], rxy.at[g, q], base[n] + 1, *at_q(to), recv=recvs.at[base[n] + groups[n] + g]).start()

        def both(k):
            fold(k)
            go(k - 1)

        fold(1)
        each(2, Q, both)
        rxy[g, q] = p[core, g, q] + rd[g, q]
        go(Q - 1)

    def scatter_c(n, g):
        _, _, _, rxy, s2, rz = rs[n]
        per = Z // groups[n]
        part = rxy.at[g, pl.ds(0, Q - 1)]
        remote(part, part, base[n], row, col, recv=recvs.at[base[n] + groups[n] + g]).wait_recv()
        for zi in range(per):
            to = g * per + zi
            s2[to] = lax.fori_loop(1, Q, lambda k, t: t + rxy[g, k, zi], rxy[g, 0, zi], unroll=True)
        for zi in range(per):
            to = g * per + zi

            @pl.when(to != z)
            def _():
                remote(s2.at[to], rz.at[z], base[n] + 2, row, to * Y + y, recv=recvs.at[base[n] + 2 * groups[n]]).start()

            @pl.when(to == z)
            def _():
                rz[z] = s2[to]

    def scatter_end(n):
        rz = rs[n][5]
        part = rz.at[pl.ds(0, Z - 1)]
        remote(part, part, base[n], row, col, recv=recvs.at[base[n] + 2 * groups[n]]).wait_recv()
        return lax.fori_loop(1, Z, lambda k, t: t + rz[k], rz[0], unroll=True).astype(BF16)

    def scatter_sent(n):
        p, _, s1, _, s2, _ = rs[n]
        await_send(p.at[0], base[n])
        await_send(s1.at[:, pl.ds(0, Q - 1)], base[n] + 1)
        await_send(s2.at[pl.ds(0, Z - 1)], base[n] + 2)

    def remote1(src, dst, k, r, c, recv):
        return pltpu.make_async_remote_copy(
            src_ref=src, dst_ref=dst, send_sem=one_send.at[k], recv_sem=recv, device_id=(c, r), device_id_type=MESH)

    def await1(ref, recv):
        remote1(ref, ref, 0, row, col, recv).wait_recv()

    def first_a(g):
        def block(cy):
            val = jnp.dot(slab_t[g * Y + cy], ed0[...], preferred_element_type=F32)
            for i in range(R):
                p_1[i % 2, g, i // 2, cy] = jnp.where(lane_left, val[i * SH:i * SH + HS], val[i * SH + HS:(i + 1) * SH])

        lax.fori_loop(0, Y, lambda k, t: (block(k), t)[1], 0, unroll=4)
        remote1(p_1.at[1 - core, g], rd_1.at[g], 0, mate, col, one_d.at[g]).start()

    def first_b(g):
        await1(rd_1.at[g], one_d.at[g])
        for k in range(1, X):
            to = (x + k) % X
            s1_1[g, to] = p_1[core, g, to] + rd_1[g, to]
        rx_1[g, x] = p_1[core, g, x] + rd_1[g, x]
        for k in range(1, X):
            to = (x + k) % X
            remote1(s1_1.at[g, to], rx_1.at[g, x], 1, to * 2 + core, col, one_x.at[g]).start()

    def first_c(g):
        await1(rx_1.at[g, pl.ds(0, X - 1)], one_x.at[g])
        total = rx_1[g, 0]
        for k in range(1, X):
            total = total + rx_1[g, k]
        for cy in range(Y):
            sy_1[cy, g] = total[cy]

    def first_y():
        for k in range(1, Y):
            to = (y + k) % Y
            remote1(sy_1.at[to], ry_1.at[y], 2, row, z * Y + to, one_yz.at[0]).start()
        ry_1[y] = sy_1[y]

    def first_z():
        await1(ry_1.at[pl.ds(0, Y - 1)], one_yz.at[0])
        total = ry_1[0]
        for k in range(1, Y):
            total = total + ry_1[k]
        s2_1[...] = total
        rz_1[z] = s2_1[z]
        each(1, Z, lambda k: remote1(s2_1.at[(z + k) % Z], rz_1.at[z], 3, row, ((z + k) % Z) * Y + y, one_yz.at[1]).start())

    def first_end():
        await1(rz_1.at[pl.ds(0, Z - 1)], one_yz.at[1])
        return lax.fori_loop(1, Z, lambda k, t: t + rz_1[k], rz_1[0], unroll=True).astype(BF16)

    def first_sent():
        for k, ref in enumerate((p_1.at[0], s1_1.at[:, pl.ds(0, X - 1)], sy_1.at[pl.ds(0, Y - 1)], s2_1.at[pl.ds(0, Z - 1)])):
            remote1(ref, ref, k, row, col, one_yz.at[0]).wait_send()

    def source(k):
        dz, dy = order(k)
        return ((z - dz + Z) % Z) * Y + (y - dy + Y) % Y

    def use(c):
        blk = slab[c]
        slab_t[c] = jnp.transpose(blk)
        acc[...] += jnp.dot(blk, rows_of(tbl0, c), preferred_element_type=F32)

    def arrive(k):
        c = source(k)
        pltpu.make_async_remote_copy(src_ref=slab.at[c], dst_ref=slab.at[c], send_sem=sends.at[ATOA], recv_sem=a2a_recv.at[c],
                                     device_id=(col, row), device_id_type=MESH).wait_recv()
        use(c)

    def group(j):
        return source(j * Y) // Y

    acc[...] = jnp.zeros_like(acc)
    use(col)
    each(1, Y, arrive)
    first_a(z)

    def stream(j):
        each(j * Y, (j + 1) * Y, arrive)
        first_a(group(j))
        first_b(group(j - 1))

        @pl.when(j >= 2)
        def _():
            first_c(group(j - 2))

    each(1, Z, stream)
    wide_left = lax.broadcasted_iota(jnp.int32, (UD, WIDE), 1) < FEAT

    def twice(v):
        return jnp.where(wide_left, v, swap(v)).astype(BF16)

    user1 = acc[...].astype(BF16).astype(F32)
    ed1[...] = twice(user1)
    for g in range(G2):
        scatter_a(1, g, ed1)
        if g == 0:
            first_b(group(Z - 1))
        else:
            scatter_b(1, g - 1)
    scatter_b(1, G2 - 1)
    first_c(group(Z - 2))
    first_c(group(Z - 1))
    first_y()
    for g in range(G2 // 2):
        scatter_c(1, g)
    first_z()
    for g in range(G2 // 2, G2):
        scatter_c(1, g)
    item1 = first_end().astype(F32)
    item2 = scatter_end(1).astype(F32)
    low = jnp.where(lane_left, item1, swap(item2))
    high = jnp.where(lane_left, swap(item1), item2)
    tbl1[core, q, z] = jnp.concatenate([low, high], axis=0).astype(BF16)
    gather_z(tbl1, GATHER1)
    gather_q(tbl1, GATHER1)
    gather_d(tbl1, GATHER1)
    acc[...] = jnp.zeros_like(acc)
    gather_end(tbl1, GATHER1)

    def absorb(c):
        cz, cy = c // Y, c % Y
        rows = jnp.concatenate([tbl1[i % 2, cy * X + i // 2, cz] for i in range(R)], axis=0)
        acc[...] += jnp.dot(slab[c], rows, preferred_element_type=F32)

    lax.fori_loop(0, C, lambda k, t: (absorb(k), t)[1], 0, unroll=4)
    late = acc[...].astype(BF16).astype(F32)
    ed2[...] = twice(late)
    scatter_a(2, 0, ed2)
    sum_user = ((ed0[...].astype(F32) + ed1[...].astype(F32)) + ed2[...].astype(F32)) + jnp.where(wide_left, swap(late), late)
    user_rows = (sum_user / (LAYERS + 1)).astype(BF16)

    ids = lax.broadcasted_iota(jnp.int32, (UD, TRIPLES), 0) + (row * C + col) * UD
    hit = (ids == trip[0:1, :]).astype(BF16)
    found = lax.dot_general(hit, user_rows, (((0,), (0,)), ((), ())), preferred_element_type=F32)
    pick_left = lax.broadcasted_iota(jnp.int32, (PICKS, WIDE), 1) < FEAT
    for h in range(2):
        lo, hi = h * PICKS, (h + 2) * PICKS
        pk_a[h] = jnp.where(pick_left, found[lo:lo + PICKS], found[hi:hi + PICKS]).astype(BF16)
    remote(pk_a.at[1 - core], pk_b, PICK, mate, col).start()
    for g in range(1, G2):
        scatter_a(2, g, ed2)
        if g == 1:
            await_recv(pk_b, PICK)
            pk_z[z] = (pk_a[core].astype(F32) + pk_b[...].astype(F32)).astype(BF16)
            each(1, Z, lambda k: remote(pk_z.at[z], pk_z.at[z], PICK + 1, row, ((z + k) % Z) * Y + y).start())
        scatter_b(2, g - 1)
    scatter_b(2, G2 - 1)
    out_user[...] = jnp.transpose(user_rows.astype(F32))[:FEAT].astype(BF16)
    await_recv(pk_z.at[pl.ds(0, Z - 1)], PICK + 1)
    pk_q[q] = lax.fori_loop(1, Z, lambda k, t: t + pk_z[k].astype(F32), pk_z[0].astype(F32), unroll=True).astype(BF16)
    each(1, Q, lambda k: remote(pk_q.at[q], pk_q.at[q], PICK + 2, *at_q((q + k) % Q)).start())
    for g in range(G2):
        scatter_c(2, g)
    await_recv(pk_q.at[pl.ds(0, Q - 1)], PICK + 2)
    pk_d[core] = lax.fori_loop(1, Q, lambda k, t: t + pk_q[k].astype(F32), pk_q[0].astype(F32), unroll=True).astype(BF16)
    remote(pk_d.at[core], pk_d.at[core], PICK + 3, mate, col).start()
    item3 = scatter_end(2)
    sum_item = ((item0 + item1) + item2) + item3.astype(F32)
    packed = (sum_item / (LAYERS + 1)).astype(BF16).astype(F32)
    zero = jnp.zeros_like(packed)
    left_rows = [jnp.where(lane_left, packed, zero), jnp.where(lane_left, swap(packed), zero)]
    right_rows = [jnp.where(lane_left, zero, swap(packed)), jnp.where(lane_left, zero, packed)]
    item_rows = jnp.concatenate(left_rows, axis=0).astype(BF16)
    out_item[...] = item_rows[:, :FEAT]

    await_recv(pk_d.at[0], PICK + 3)
    user_vec = jnp.concatenate([pk_d[0], pk_d[1], pk_d[0], pk_d[1]], axis=0)
    nt = (((1,), (1,)), ((), ()))
    dots_l = lax.dot_general(item_rows, user_vec, nt, preferred_element_type=F32)
    dots_r = lax.dot_general(jnp.concatenate(right_rows, axis=0).astype(BF16), user_vec, nt, preferred_element_type=F32)
    dots = jnp.where(lax.broadcasted_iota(jnp.int32, (SH, TRIPLES), 1) < TRIPLES // 2, dots_l, dots_r)
    own = lax.broadcasted_iota(jnp.int32, (SH, TRIPLES), 0) + (col * R + row) * SH
    pos = jnp.sum(jnp.where(own == trip[1:2, :], dots, 0.0), axis=0, keepdims=True)
    neg = jnp.sum(jnp.where(own == trip[2:3, :], dots, 0.0), axis=0, keepdims=True)
    mine = q * 2 + core
    xc[mine] = pos - neg

    def spread_margin(k):
        to = (mine + k) % (2 * Q)
        remote(xc.at[mine], xc.at[mine], MARGIN, ((to // 2) % X) * 2 + to % 2, z * Y + to // (2 * X)).start()

    each(1, 2 * Q, spread_margin)
    await_recv(xc.at[pl.ds(0, 2 * Q - 1)], MARGIN)
    xr[z] = lax.fori_loop(1, 2 * Q, lambda k, t: t + xc[k], xc[0], unroll=True)
    each(1, Z, lambda k: remote(xr.at[z], xr.at[z], MARGIN + 1, row, ((z + k) % Z) * Y + y).start())
    await_recv(xr.at[pl.ds(0, Z - 1)], MARGIN + 1)
    margin = lax.fori_loop(1, Z, lambda k, t: t + xr[k], xr[0], unroll=True)
    soft = jnp.maximum(-margin, 0.0) + jnp.log1p(jnp.exp(-jnp.abs(margin)))
    loss[...] = jnp.sum(soft, axis=1, keepdims=True) / TRIPLES

    await_send(deg_s.at[pl.ds(0, C - 1)], DEG)
    await_send(ideg.at[pl.ds(0, R - 1)], IDEG)
    await_send(deg_f.at[pl.ds(0, C - 1)], SPREAD)
    await_send(send_a.at[pl.ds(0, C - 1)], ATOA)
    gather_sent(tbl0, GATHER0)
    gather_sent(tbl1, GATHER1)
    first_sent()
    for n in (1, 2):
        scatter_sent(n)
    await_send(pk_b, PICK)
    await_send(pk_z.at[pl.ds(0, Z - 1)], PICK + 1)
    await_send(pk_q.at[pl.ds(0, Q - 1)], PICK + 2)
    await_send(pk_d.at[0], PICK + 3)
    await_send(xc.at[pl.ds(0, 2 * Q - 1)], MARGIN)
    await_send(xr.at[pl.ds(0, Z - 1)], MARGIN + 1)


def emit(user_in, item_in, loss_in, user_out, item_out, loss_out):
    user_out[...] = user_in[...]
    item_out[...] = item_in[...]
    loss_out[...] = loss_in[...]


def build(mesh, Y, SH, UD, G2):
    C, R = mesh.shape["col"], mesh.shape["row"]
    Z, X = C // Y, R // 2
    Q, IB, HS = Y * X, R * SH, SH // 2
    vm = pltpu.VMEM
    scratch = [
        vm((C, 1, UD), F32), vm((C, 1, UD), F32), vm((C, 1, UD), F32), vm((1, UD), F32), vm((R, 1, IB), F32),
        vm((C, UD, IB), BF16), vm((C, UD, IB), BF16), vm((C, IB, UD), BF16),
        vm((2, Q, Z, HS, WIDE), BF16), vm((2, Q, Z, SH, WIDE), BF16),
        vm((UD, WIDE), F32), vm((UD, WIDE), BF16), vm((UD, WIDE), BF16), vm((UD, WIDE), BF16),
        vm((2, PICKS, WIDE), BF16), vm((PICKS, WIDE), BF16),
        vm((Z, PICKS, WIDE), BF16), vm((Q, PICKS, WIDE), BF16), vm((2, PICKS, WIDE), BF16),
        vm((2 * Q, 1, TRIPLES), F32), vm((Z, 1, TRIPLES), F32),
    ]
    count = SCATTER1 + 2 * (2 * G2 + 1)
    sem = pltpu.SemaphoreType.DMA
    scratch += [sem((count,)), sem((count,)), sem((C,)), vm((C, UD, IB), jnp.int32), sem((LOADS,))]
    scratch += [
        vm((2, Z, X, Y, HS, WIDE), F32), vm((Z, X, Y, HS, WIDE), F32), vm((Z, X, Y, HS, WIDE), F32), vm((Z, X, Y, HS, WIDE), F32),
        vm((Y, Z, HS, WIDE), F32), vm((Y, Z, HS, WIDE), F32), vm((Z, HS, WIDE), F32), vm((Z, HS, WIDE), F32),
        sem((4,)), sem((Z,)), sem((Z,)), sem((2,)),
    ]
    for g in (G2, G2):
        scratch += [vm((2, g, Q, Z // g, HS, WIDE), F32)] + [vm((g, Q, Z // g, HS, WIDE), F32)] * 3 + [vm((Z, HS, WIDE), F32)] * 2
    scratch += [sem((C,))]
    dims = (Z, Y, X, SH, UD, G2)

    def local_prog(mask_blk, user_shard, item_shard, triples):
        out_user, out_item, loss = pl.pallas_call(
            functools.partial(kernel, dims),
            out_shape=(
                jax.ShapeDtypeStruct((FEAT, UD), BF16),
                jax.ShapeDtypeStruct((SH, FEAT), BF16),
                jax.ShapeDtypeStruct((1, 1), F32),
            ),
            in_specs=[pl.BlockSpec(memory_space=pl.ANY)] + [pl.BlockSpec(memory_space=pltpu.VMEM)] * 3,
            out_specs=(pl.BlockSpec(memory_space=pltpu.VMEM),) * 3,
            scratch_shapes=scratch,
            compiler_params=pltpu.CompilerParams(
                collective_id=0, has_side_effects=True, vmem_limit_bytes=60 * 1024 * 1024),
            name="lightgcn",
        )(mask_blk.reshape(C, UD, IB), user_shard.T, item_shard, triples.T)
        out_user, out_item, loss = pl.pallas_call(
            emit,
            out_shape=(
                jax.ShapeDtypeStruct((FEAT, UD), BF16),
                jax.ShapeDtypeStruct((SH, FEAT), BF16),
                jax.ShapeDtypeStruct((1, 1), F32),
            ),
            in_specs=[pl.BlockSpec(memory_space=pltpu.VMEM)] * 3,
            out_specs=(pl.BlockSpec(memory_space=pltpu.VMEM),) * 3,
            name="emit",
        )(out_user, out_item, loss)
        return out_user.T, out_item, loss[0, 0]

    return jax.shard_map(
        local_prog, mesh=mesh,
        in_specs=(P("row", "col"), P(("row", "col"), None), P(("col", "row"), None), P(None, None)),
        out_specs=(P(("row", "col"), None), P(("col", "row"), None), P()), check_vma=False)


def solution(mesh):
    return build(mesh, Y=4, SH=16, UD=256, G2=8)
```

```python
import functools

import jax
import jax.numpy as jnp
from jax import lax
from jax.experimental import pallas as pl
from jax.experimental.pallas import tpu as pltpu
from jax.sharding import PartitionSpec as P

MESH = pl.DeviceIdType.MESH
F32 = jnp.float32
BF16 = jnp.bfloat16
FEAT = 64
WIDE = 2 * FEAT
TRIPLES = 128
LAYERS = 3
LOADS = 8
PICKS = TRIPLES // 4

DEG, IDEG, SPREAD, ATOA, GATHER0, GATHER1, PICK, MARGIN, SCATTER1 = 0, 1, 2, 3, 4, 7, 10, 14, 16


def swap(v):
    return pltpu.roll(v, FEAT, 1)


def kernel(dims, mask_hbm, eu0, ei0, trip, out_user, out_item, loss, *scratch):
    Z, Y, X, SH, UD, G2 = dims
    C, R, Q = Z * Y, 2 * X, Y * X
    IB = R * SH
    HS = SH // 2
    (deg_s, deg_r, deg_f, own_deg, ideg, send_a, slab, slab_t, tbl0, tbl1, acc, ed0, ed1, ed2, pk_a, pk_b, pk_z, pk_q, pk_d, xc, xr,
     sends, recvs, a2a_recv, mask, load_sem) = scratch[:26]
    spread_recv = scratch[50]
    groups = (Z, G2, G2)
    p_1, rd_1, s1_1, rx_1, sy_1, ry_1, s2_1, rz_1, one_send, one_d, one_x, one_yz = scratch[26:38]
    rs = [None] + [scratch[32 + 6 * n:38 + 6 * n] for n in (1, 2)]
    base = [SCATTER1]
    base.append(SCATTER1)
    for n in (1, 2):
        base.append(base[-1] + 2 * groups[n] + 1)
    row = lax.axis_index("row")
    col = lax.axis_index("col")
    core, x = row % 2, row // 2
    z, y = col // Y, col % Y
    q = y * X + x
    mate = x * 2 + (1 - core)

    def remote(src, dst, sem, r, c, recv=None):
        return pltpu.make_async_remote_copy(
            src_ref=src, dst_ref=dst, send_sem=sends.at[sem], recv_sem=recvs.at[sem] if recv is None else recv,
            device_id=(c, r), device_id_type=MESH)

    def await_recv(ref, sem):
        remote(ref, ref, sem, row, col).wait_recv()

    def await_send(ref, sem):
        remote(ref, ref, sem, row, col).wait_send()

    def at_q(p):
        return (p % X) * 2 + core, z * Y + p // X

    def each(lo, hi, fn):
        lax.fori_loop(lo, hi, lambda k, t: (fn(k), t)[1], 0)

    run = C // LOADS

    def load(i):
        part = pl.ds(i * run, run)
        return pltpu.make_async_copy(mask_hbm.at[part], mask.at[part], load_sem.at[i])

    for i in range(LOADS):
        load(i).start()

    barrier = pltpu.get_barrier_semaphore()

    def hail(c, r):
        pl.semaphore_signal(barrier, inc=1, device_id=(c, r), device_id_type=MESH)

    each(1, C, lambda k: hail((col + k) % C, row))
    each(1, Y, lambda k: hail(z * Y + (y + k) % Y, mate))
    each(1, R, lambda k: hail(col, (row + k) % R))
    def hail_diagonal(k):
        i = k // 2
        hail(z * Y + (y + 1 + i // (X - 1)) % Y, ((x + 1 + i % (X - 1)) % X) * 2 + k % 2)

    each(0, 2 * (X - 1) * (Y - 1), hail_diagonal)

    ones = jnp.ones((8, IB), BF16)

    def count(k, part):
        blk = mask[k].astype(F32)
        sums = lax.dot_general(ones, blk.astype(BF16), (((1,), (1,)), ((), ())), preferred_element_type=F32)
        deg_s[k] = sums[0:1]
        return part + jnp.sum(blk.reshape(UD // 8, 8, IB), axis=0)

    part = jnp.zeros((8, IB), F32)
    for i in range(LOADS):
        load(i).wait()
        part = lax.fori_loop(i * run, (i + 1) * run, count, part, unroll=True)
    ideg[row] = jnp.sum(part, axis=0, keepdims=True)
    deg_r[col] = deg_s[col]

    lane_left = lax.broadcasted_iota(jnp.int32, (HS, WIDE), 1) < FEAT

    def pack(v):
        return jnp.where(lane_left, v[:HS], swap(v[HS:]))

    e0 = ei0[...].astype(F32)
    item0 = pack(jnp.concatenate([e0, jnp.zeros_like(e0)], axis=1))
    tbl0[core, q, z] = item0.astype(BF16)
    user0 = eu0[...].astype(F32)
    ed0[...] = jnp.transpose(jnp.concatenate([user0, user0], axis=0)).astype(BF16)
    pl.semaphore_wait(barrier, (C - 1) + (Y - 1) + (R - 1) + 2 * (X - 1) * (Y - 1))

    def gather_z(tbl, sem):
        each(1, Z, lambda k: remote(tbl.at[core, q, z], tbl.at[core, q, z], sem, row, ((z + k) % Z) * Y + y).start())

    def gather_q(tbl, sem):
        await_recv(tbl.at[core, q, pl.ds(0, Z - 1)], sem)
        each(1, Q, lambda k: remote(tbl.at[core, q], tbl.at[core, q], sem + 1, *at_q((q + k) % Q)).start())

    def gather_d(tbl, sem):
        await_recv(tbl.at[core, pl.ds(0, Q - 1)], sem + 1)
        remote(tbl.at[core], tbl.at[core], sem + 2, mate, col).start()

    def gather_end(tbl, sem):
        await_recv(tbl.at[core], sem + 2)

    def gather_sent(tbl, sem):
        await_send(tbl.at[core, q, pl.ds(0, Z - 1)], sem)
        await_send(tbl.at[core, pl.ds(0, Q - 1)], sem + 1)
        await_send(tbl.at[core], sem + 2)

    def rows_of(tbl, c):
        cz, cy = c // Y, c % Y
        parts = []
        for i in range(R):
            v = tbl[i % 2, cy * X + i // 2, cz].astype(F32)
            parts += [v, swap(v)]
        return jnp.concatenate(parts, axis=0).astype(BF16)

    def order(k):
        j = k // Y
        m = (j + 1) // 2
        odd = j % 2
        return (odd * m + (1 - odd) * (Z - m)) % Z, k % Y

    def target(k):
        dz, dy = order(k)
        return ((z + dz) % Z) * Y + (y + dy) % Y

    each(1, C, lambda k: remote(deg_s.at[(col + k) % C], deg_r.at[col], DEG, row, (col + k) % C).start())
    each(1, R, lambda k: remote(ideg.at[row], ideg.at[row], IDEG, (row + k) % R, col).start())
    gather_z(tbl0, GATHER0)
    await_recv(deg_r.at[pl.ds(0, C - 1)], DEG)
    own_deg[...] = lax.fori_loop(0, C, lambda k, t: t + deg_r[k], jnp.zeros((1, UD), F32), unroll=True)
    deg_f[col] = own_deg[...]
    each(1, C, lambda k: remote(own_deg, deg_f.at[col], SPREAD, row, target(k), recv=spread_recv.at[col]).start())
    await_recv(ideg.at[pl.ds(0, R - 1)], IDEG)
    scale_item = lax.rsqrt(jnp.maximum(lax.fori_loop(0, R, lambda k, t: t + ideg[k], jnp.zeros((1, IB), F32), unroll=True), 1.0))
    gather_q(tbl0, GATHER0)

    def piece(c):
        scale = lax.rsqrt(jnp.maximum(deg_f[c], 1.0))
        scale = jnp.transpose(jnp.broadcast_to(scale, (IB, UD)))
        return (mask[c].astype(F32) * scale * scale_item).astype(BF16)

    def ship(k):
        to = target(k)
        remote(send_a.at[to], slab.at[col], ATOA, row, to, recv=a2a_recv.at[col]).start()

    def make(k):
        to = target(k)
        remote(deg_f.at[to], deg_f.at[to], SPREAD, row, col, recv=spread_recv.at[to]).wait_recv()
        send_a[to] = piece(to)

    make(1)

    def make_and_ship(k):
        make(k)
        ship(k - 1)

    each(2, C, make_and_ship)
    slab[col] = piece(col)
    ship(C - 1)
    gather_d(tbl0, GATHER0)
    gather_end(tbl0, GATHER0)

    def scatter_a(n, g, ed):
        p, rd = rs[n][0], rs[n][1]
        per = Z // groups[n]

        def block(k):
            zi, cy = k // Y, k % Y
            val = jnp.dot(slab_t[(g * per + zi) * Y + cy], ed[...], preferred_element_type=F32)
            for i in range(R):
                p[i % 2, g, cy * X + i // 2, zi] = jnp.where(lane_left, val[i * SH:i * SH + HS], val[i * SH + HS:(i + 1) * SH])

        lax.fori_loop(0, per * Y, lambda k, t: (block(k), t)[1], 0, unroll=4)
        remote(p.at[1 - core, g], rd.at[g], base[n], mate, col, recv=recvs.at[base[n] + g]).start()

    def scatter_b(n, g):
        p, rd, s1, rxy, _, _ = rs[n]
        remote(rd.at[g], rd.at[g], base[n], row, col, recv=recvs.at[base[n] + g]).wait_recv()

        def fold(k):
            to = (q + k) % Q
            s1[g, to] = p[core, g, to] + rd[g, to]

        def go(k):
            to = (q + k) % Q
            remote(s1.at[g, to], rxy.at[g, q], base[n] + 1, *at_q(to), recv=recvs.at[base[n] + groups[n] + g]).start()

        def both(k):
            fold(k)
            go(k - 1)

        fold(1)
        each(2, Q, both)
        rxy[g, q] = p[core, g, q] + rd[g, q]
        go(Q - 1)

    def scatter_c(n, g):
        _, _, _, rxy, s2, rz = rs[n]
        per = Z // groups[n]
        part = rxy.at[g, pl.ds(0, Q - 1)]
        remote(part, part, base[n], row, col, recv=recvs.at[base[n] + groups[n] + g]).wait_recv()
        for zi in range(per):
            to = g * per + zi
            s2[to] = lax.fori_loop(1, Q, lambda k, t: t + rxy[g, k, zi], rxy[g, 0, zi], unroll=True)
        for zi in range(per):
            to = g * per + zi

            @pl.when(to != z)
            def _():
                remote(s2.at[to], rz.at[z], base[n] + 2, row, to * Y + y, recv=recvs.at[base[n] + 2 * groups[n]]).start()

            @pl.when(to == z)
            def _():
                rz[z] = s2[to]

    def scatter_end(n):
        rz = rs[n][5]
        part = rz.at[pl.ds(0, Z - 1)]
        remote(part, part, base[n], row, col, recv=recvs.at[base[n] + 2 * groups[n]]).wait_recv()
        return lax.fori_loop(1, Z, lambda k, t: t + rz[k], rz[0], unroll=True).astype(BF16)

    def scatter_sent(n):
        p, _, s1, _, s2, _ = rs[n]
        await_send(p.at[0], base[n])
        await_send(s1.at[:, pl.ds(0, Q - 1)], base[n] + 1)
        await_send(s2.at[pl.ds(0, Z - 1)], base[n] + 2)

    def remote1(src, dst, k, r, c, recv):
        return pltpu.make_async_remote_copy(
            src_ref=src, dst_ref=dst, send_sem=one_send.at[k], recv_sem=recv, device_id=(c, r), device_id_type=MESH)

    def await1(ref, recv):
        remote1(ref, ref, 0, row, col, recv).wait_recv()

    def first_a(g):
        def block(cy):
            val = jnp.dot(slab_t[g * Y + cy], ed0[...], preferred_element_type=F32)
            for i in range(R):
                p_1[i % 2, g, i // 2, cy] = jnp.where(lane_left, val[i * SH:i * SH + HS], val[i * SH + HS:(i + 1) * SH])

        lax.fori_loop(0, Y, lambda k, t: (block(k), t)[1], 0, unroll=4)
        remote1(p_1.at[1 - core, g], rd_1.at[g], 0, mate, col, one_d.at[g]).start()

    def first_b(g):
        await1(rd_1.at[g], one_d.at[g])
        for k in range(1, X):
            to = (x + k) % X
            s1_1[g, to] = p_1[core, g, to] + rd_1[g, to]
        rx_1[g, x] = p_1[core, g, x] + rd_1[g, x]
        for k in range(1, X):
            to = (x + k) % X
            remote1(s1_1.at[g, to], rx_1.at[g, x], 1, to * 2 + core, col, one_x.at[g]).start()

    def first_c(g):
        await1(rx_1.at[g, pl.ds(0, X - 1)], one_x.at[g])
        total = rx_1[g, 0]
        for k in range(1, X):
            total = total + rx_1[g, k]
        for cy in range(Y):
            sy_1[cy, g] = total[cy]

    def first_y():
        for k in range(1, Y):
            to = (y + k) % Y
            remote1(sy_1.at[to], ry_1.at[y], 2, row, z * Y + to, one_yz.at[0]).start()
        ry_1[y] = sy_1[y]

    def first_z():
        await1(ry_1.at[pl.ds(0, Y - 1)], one_yz.at[0])
        total = ry_1[0]
        for k in range(1, Y):
            total = total + ry_1[k]
        s2_1[...] = total
        rz_1[z] = s2_1[z]
        each(1, Z, lambda k: remote1(s2_1.at[(z + k) % Z], rz_1.at[z], 3, row, ((z + k) % Z) * Y + y, one_yz.at[1]).start())

    def first_end():
        await1(rz_1.at[pl.ds(0, Z - 1)], one_yz.at[1])
        return lax.fori_loop(1, Z, lambda k, t: t + rz_1[k], rz_1[0], unroll=True).astype(BF16)

    def first_sent():
        for k, ref in enumerate((p_1.at[0], s1_1.at[:, pl.ds(0, X - 1)], sy_1.at[pl.ds(0, Y - 1)], s2_1.at[pl.ds(0, Z - 1)])):
            remote1(ref, ref, k, row, col, one_yz.at[0]).wait_send()

    def source(k):
        dz, dy = order(k)
        return ((z - dz + Z) % Z) * Y + (y - dy + Y) % Y

    def use(c):
        blk = slab[c]
        slab_t[c] = jnp.transpose(blk)
        acc[...] += jnp.dot(blk, rows_of(tbl0, c), preferred_element_type=F32)

    def arrive(k):
        c = source(k)
        pltpu.make_async_remote_copy(src_ref=slab.at[c], dst_ref=slab.at[c], send_sem=sends.at[ATOA], recv_sem=a2a_recv.at[c],
                                     device_id=(col, row), device_id_type=MESH).wait_recv()
        use(c)

    def group(j):
        return source(j * Y) // Y

    acc[...] = jnp.zeros_like(acc)
    use(col)
    each(1, Y, arrive)
    first_a(z)

    def stream(j):
        each(j * Y, (j + 1) * Y, arrive)
        first_a(group(j))
        first_b(group(j - 1))

        @pl.when(j >= 2)
        def _():
            first_c(group(j - 2))

    each(1, Z, stream)
    wide_left = lax.broadcasted_iota(jnp.int32, (UD, WIDE), 1) < FEAT

    def twice(v):
        return jnp.where(wide_left, v, swap(v)).astype(BF16)

    user1 = acc[...].astype(BF16).astype(F32)
    ed1[...] = twice(user1)
    for g in range(G2):
        scatter_a(1, g, ed1)
        if g == 0:
            first_b(group(Z - 1))
        else:
            scatter_b(1, g - 1)
    first_c(group(Z - 2))
    first_c(group(Z - 1))
    first_y()
    scatter_b(1, G2 - 1)
    first_z()
    for g in range(G2):
        scatter_c(1, g)
    item1 = first_end().astype(F32)
    item2 = scatter_end(1).astype(F32)
    low = jnp.where(lane_left, item1, swap(item2))
    high = jnp.where(lane_left, swap(item1), item2)
    tbl1[core, q, z] = jnp.concatenate([low, high], axis=0).astype(BF16)
    gather_z(tbl1, GATHER1)
    gather_q(tbl1, GATHER1)
    gather_d(tbl1, GATHER1)
    acc[...] = jnp.zeros_like(acc)
    gather_end(tbl1, GATHER1)

    def absorb(c):
        cz, cy = c // Y, c % Y
        rows = jnp.concatenate([tbl1[i % 2, cy * X + i // 2, cz] for i in range(R)], axis=0)
        acc[...] += jnp.dot(slab[c], rows, preferred_element_type=F32)

    lax.fori_loop(0, C, lambda k, t: (absorb(k), t)[1], 0, unroll=4)
    late = acc[...].astype(BF16).astype(F32)
    ed2[...] = twice(late)
    scatter_a(2, 0, ed2)
    sum_user = ((ed0[...].astype(F32) + ed1[...].astype(F32)) + ed2[...].astype(F32)) + jnp.where(wide_left, swap(late), late)
    user_rows = (sum_user / (LAYERS + 1)).astype(BF16)

    ids = lax.broadcasted_iota(jnp.int32, (UD, TRIPLES), 0) + (row * C + col) * UD
    hit = (ids == trip[0:1, :]).astype(BF16)
    found = lax.dot_general(hit, user_rows, (((0,), (0,)), ((), ())), preferred_element_type=F32)
    pick_left = lax.broadcasted_iota(jnp.int32, (PICKS, WIDE), 1) < FEAT
    for h in range(2):
        lo, hi = h * PICKS, (h + 2) * PICKS
        pk_a[h] = jnp.where(pick_left, found[lo:lo + PICKS], found[hi:hi + PICKS]).astype(BF16)
    remote(pk_a.at[1 - core], pk_b, PICK, mate, col).start()
    for g in range(1, G2):
        scatter_a(2, g, ed2)
        if g == 1:
            await_recv(pk_b, PICK)
            pk_z[z] = (pk_a[core].astype(F32) + pk_b[...].astype(F32)).astype(BF16)
            each(1, Z, lambda k: remote(pk_z.at[z], pk_z.at[z], PICK + 1, row, ((z + k) % Z) * Y + y).start())
        scatter_b(2, g - 1)
    scatter_b(2, G2 - 1)
    out_user[...] = jnp.transpose(user_rows.astype(F32))[:FEAT].astype(BF16)
    await_recv(pk_z.at[pl.ds(0, Z - 1)], PICK + 1)
    pk_q[q] = lax.fori_loop(1, Z, lambda k, t: t + pk_z[k].astype(F32), pk_z[0].astype(F32), unroll=True).astype(BF16)
    each(1, Q, lambda k: remote(pk_q.at[q], pk_q.at[q], PICK + 2, *at_q((q + k) % Q)).start())
    for g in range(G2):
        scatter_c(2, g)
    await_recv(pk_q.at[pl.ds(0, Q - 1)], PICK + 2)
    pk_d[core] = lax.fori_loop(1, Q, lambda k, t: t + pk_q[k].astype(F32), pk_q[0].astype(F32), unroll=True).astype(BF16)
    remote(pk_d.at[core], pk_d.at[core], PICK + 3, mate, col).start()
    item3 = scatter_end(2)
    sum_item = ((item0 + item1) + item2) + item3.astype(F32)
    packed = (sum_item / (LAYERS + 1)).astype(BF16).astype(F32)
    zero = jnp.zeros_like(packed)
    left_rows = [jnp.where(lane_left, packed, zero), jnp.where(lane_left, swap(packed), zero)]
    right_rows = [jnp.where(lane_left, zero, swap(packed)), jnp.where(lane_left, zero, packed)]
    item_rows = jnp.concatenate(left_rows, axis=0).astype(BF16)
    out_item[...] = item_rows[:, :FEAT]

    await_recv(pk_d.at[0], PICK + 3)
    user_vec = jnp.concatenate([pk_d[0], pk_d[1], pk_d[0], pk_d[1]], axis=0)
    nt = (((1,), (1,)), ((), ()))
    dots_l = lax.dot_general(item_rows, user_vec, nt, preferred_element_type=F32)
    dots_r = lax.dot_general(jnp.concatenate(right_rows, axis=0).astype(BF16), user_vec, nt, preferred_element_type=F32)
    dots = jnp.where(lax.broadcasted_iota(jnp.int32, (SH, TRIPLES), 1) < TRIPLES // 2, dots_l, dots_r)
    own = lax.broadcasted_iota(jnp.int32, (SH, TRIPLES), 0) + (col * R + row) * SH
    pos = jnp.sum(jnp.where(own == trip[1:2, :], dots, 0.0), axis=0, keepdims=True)
    neg = jnp.sum(jnp.where(own == trip[2:3, :], dots, 0.0), axis=0, keepdims=True)
    mine = q * 2 + core
    xc[mine] = pos - neg

    def spread_margin(k):
        to = (mine + k) % (2 * Q)
        remote(xc.at[mine], xc.at[mine], MARGIN, ((to // 2) % X) * 2 + to % 2, z * Y + to // (2 * X)).start()

    each(1, 2 * Q, spread_margin)
    await_recv(xc.at[pl.ds(0, 2 * Q - 1)], MARGIN)
    xr[z] = lax.fori_loop(1, 2 * Q, lambda k, t: t + xc[k], xc[0], unroll=True)
    each(1, Z, lambda k: remote(xr.at[z], xr.at[z], MARGIN + 1, row, ((z + k) % Z) * Y + y).start())
    await_recv(xr.at[pl.ds(0, Z - 1)], MARGIN + 1)
    margin = lax.fori_loop(1, Z, lambda k, t: t + xr[k], xr[0], unroll=True)
    soft = jnp.maximum(-margin, 0.0) + jnp.log1p(jnp.exp(-jnp.abs(margin)))
    loss[...] = jnp.sum(soft, axis=1, keepdims=True) / TRIPLES

    await_send(deg_s.at[pl.ds(0, C - 1)], DEG)
    await_send(ideg.at[pl.ds(0, R - 1)], IDEG)
    await_send(deg_f.at[pl.ds(0, C - 1)], SPREAD)
    await_send(send_a.at[pl.ds(0, C - 1)], ATOA)
    gather_sent(tbl0, GATHER0)
    gather_sent(tbl1, GATHER1)
    first_sent()
    for n in (1, 2):
        scatter_sent(n)
    await_send(pk_b, PICK)
    await_send(pk_z.at[pl.ds(0, Z - 1)], PICK + 1)
    await_send(pk_q.at[pl.ds(0, Q - 1)], PICK + 2)
    await_send(pk_d.at[0], PICK + 3)
    await_send(xc.at[pl.ds(0, 2 * Q - 1)], MARGIN)
    await_send(xr.at[pl.ds(0, Z - 1)], MARGIN + 1)


def emit(user_in, item_in, loss_in, user_out, item_out, loss_out):
    user_out[...] = user_in[...]
    item_out[...] = item_in[...]
    loss_out[...] = loss_in[...]


def build(mesh, Y, SH, UD, G2):
    C, R = mesh.shape["col"], mesh.shape["row"]
    Z, X = C // Y, R // 2
    Q, IB, HS = Y * X, R * SH, SH // 2
    vm = pltpu.VMEM
    scratch = [
        vm((C, 1, UD), F32), vm((C, 1, UD), F32), vm((C, 1, UD), F32), vm((1, UD), F32), vm((R, 1, IB), F32),
        vm((C, UD, IB), BF16), vm((C, UD, IB), BF16), vm((C, IB, UD), BF16),
        vm((2, Q, Z, HS, WIDE), BF16), vm((2, Q, Z, SH, WIDE), BF16),
        vm((UD, WIDE), F32), vm((UD, WIDE), BF16), vm((UD, WIDE), BF16), vm((UD, WIDE), BF16),
        vm((2, PICKS, WIDE), BF16), vm((PICKS, WIDE), BF16),
        vm((Z, PICKS, WIDE), BF16), vm((Q, PICKS, WIDE), BF16), vm((2, PICKS, WIDE), BF16),
        vm((2 * Q, 1, TRIPLES), F32), vm((Z, 1, TRIPLES), F32),
    ]
    count = SCATTER1 + 2 * (2 * G2 + 1)
    sem = pltpu.SemaphoreType.DMA
    scratch += [sem((count,)), sem((count,)), sem((C,)), vm((C, UD, IB), jnp.int32), sem((LOADS,))]
    scratch += [
        vm((2, Z, X, Y, HS, WIDE), F32), vm((Z, X, Y, HS, WIDE), F32), vm((Z, X, Y, HS, WIDE), F32), vm((Z, X, Y, HS, WIDE), F32),
        vm((Y, Z, HS, WIDE), F32), vm((Y, Z, HS, WIDE), F32), vm((Z, HS, WIDE), F32), vm((Z, HS, WIDE), F32),
        sem((4,)), sem((Z,)), sem((Z,)), sem((2,)),
    ]
    for g in (G2, G2):
        scratch += [vm((2, g, Q, Z // g, HS, WIDE), F32)] + [vm((g, Q, Z // g, HS, WIDE), F32)] * 3 + [vm((Z, HS, WIDE), F32)] * 2
    scratch += [sem((C,))]
    dims = (Z, Y, X, SH, UD, G2)

    def local_prog(mask_blk, user_shard, item_shard, triples):
        out_user, out_item, loss = pl.pallas_call(
            functools.partial(kernel, dims),
            out_shape=(
                jax.ShapeDtypeStruct((FEAT, UD), BF16),
                jax.ShapeDtypeStruct((SH, FEAT), BF16),
                jax.ShapeDtypeStruct((1, 1), F32),
            ),
            in_specs=[pl.BlockSpec(memory_space=pl.ANY)] + [pl.BlockSpec(memory_space=pltpu.VMEM)] * 3,
            out_specs=(pl.BlockSpec(memory_space=pltpu.VMEM),) * 3,
            scratch_shapes=scratch,
            compiler_params=pltpu.CompilerParams(
                collective_id=0, has_side_effects=True, vmem_limit_bytes=60 * 1024 * 1024),
            name="lightgcn",
        )(mask_blk.reshape(C, UD, IB), user_shard.T, item_shard, triples.T)
        out_user, out_item, loss = pl.pallas_call(
            emit,
            out_shape=(
                jax.ShapeDtypeStruct((FEAT, UD), BF16),
                jax.ShapeDtypeStruct((SH, FEAT), BF16),
                jax.ShapeDtypeStruct((1, 1), F32),
            ),
            in_specs=[pl.BlockSpec(memory_space=pltpu.VMEM)] * 3,
            out_specs=(pl.BlockSpec(memory_space=pltpu.VMEM),) * 3,
            name="emit",
        )(out_user, out_item, loss)
        return out_user.T, out_item, loss[0, 0]

    return jax.shard_map(
        local_prog, mesh=mesh,
        in_specs=(P("row", "col"), P(("row", "col"), None), P(("col", "row"), None), P(None, None)),
        out_specs=(P(("row", "col"), None), P(("col", "row"), None), P()), check_vma=False)


def solution(mesh):
    return build(mesh, Y=4, SH=16, UD=256, G2=8)
```

```python
import functools

import jax
import jax.numpy as jnp
from jax import lax
from jax.experimental import pallas as pl
from jax.experimental.pallas import tpu as pltpu
from jax.sharding import PartitionSpec as P

MESH = pl.DeviceIdType.MESH
F32 = jnp.float32
BF16 = jnp.bfloat16
FEAT = 64
WIDE = 2 * FEAT
TRIPLES = 128
LAYERS = 3
LOADS = 8
PICKS = TRIPLES // 4

DEG, IDEG, SPREAD, ATOA, GATHER0, GATHER1, PICK, MARGIN, SCATTER1 = 0, 1, 2, 3, 4, 7, 10, 14, 16


def swap(v):
    return pltpu.roll(v, FEAT, 1)


def kernel(dims, mask_hbm, eu0, ei0, trip, out_user, out_item, loss, *scratch):
    Z, Y, X, SH, UD, G2 = dims
    C, R, Q = Z * Y, 2 * X, Y * X
    IB = R * SH
    HS = SH // 2
    (deg_s, deg_r, deg_f, own_deg, ideg, send_a, slab, slab_t, tbl0, tbl1, acc, ed0, ed1, ed2, pk_a, pk_b, pk_z, pk_q, pk_d, xc, xr,
     sends, recvs, a2a_recv, mask, load_sem) = scratch[:26]
    spread_recv = scratch[50]
    groups = (Z, G2, G2)
    p_1, rd_1, s1_1, rx_1, sy_1, ry_1, s2_1, rz_1, one_send, one_d, one_x, one_yz = scratch[26:38]
    rs = [None] + [scratch[32 + 6 * n:38 + 6 * n] for n in (1, 2)]
    base = [SCATTER1]
    base.append(SCATTER1)
    for n in (1, 2):
        base.append(base[-1] + 2 * groups[n] + 1)
    row = lax.axis_index("row")
    col = lax.axis_index("col")
    core, x = row % 2, row // 2
    z, y = col // Y, col % Y
    q = y * X + x
    mate = x * 2 + (1 - core)

    def remote(src, dst, sem, r, c, recv=None):
        return pltpu.make_async_remote_copy(
            src_ref=src, dst_ref=dst, send_sem=sends.at[sem], recv_sem=recvs.at[sem] if recv is None else recv,
            device_id=(c, r), device_id_type=MESH)

    def await_recv(ref, sem):
        remote(ref, ref, sem, row, col).wait_recv()

    def await_send(ref, sem):
        remote(ref, ref, sem, row, col).wait_send()

    def at_q(p):
        return (p % X) * 2 + core, z * Y + p // X

    def each(lo, hi, fn):
        lax.fori_loop(lo, hi, lambda k, t: (fn(k), t)[1], 0)

    run = C // LOADS

    def load(i):
        part = pl.ds(i * run, run)
        return pltpu.make_async_copy(mask_hbm.at[part], mask.at[part], load_sem.at[i])

    for i in range(LOADS):
        load(i).start()

    barrier = pltpu.get_barrier_semaphore()

    def hail(c, r):
        pl.semaphore_signal(barrier, inc=1, device_id=(c, r), device_id_type=MESH)

    each(1, C, lambda k: hail((col + k) % C, row))
    each(1, Y, lambda k: hail(z * Y + (y + k) % Y, mate))
    each(1, R, lambda k: hail(col, (row + k) % R))
    def hail_diagonal(k):
        i = k // 2
        hail(z * Y + (y + 1 + i // (X - 1)) % Y, ((x + 1 + i % (X - 1)) % X) * 2 + k % 2)

    each(0, 2 * (X - 1) * (Y - 1), hail_diagonal)

    ones = jnp.ones((8, IB), BF16)

    def count(k, part):
        blk = mask[k].astype(F32)
        sums = lax.dot_general(ones, blk.astype(BF16), (((1,), (1,)), ((), ())), preferred_element_type=F32)
        deg_s[k] = sums[0:1]
        return part + jnp.sum(blk.reshape(UD // 8, 8, IB), axis=0)

    part = jnp.zeros((8, IB), F32)
    for i in range(LOADS):
        load(i).wait()
        part = lax.fori_loop(i * run, (i + 1) * run, count, part, unroll=True)
    ideg[row] = jnp.sum(part, axis=0, keepdims=True)
    deg_r[col] = deg_s[col]

    lane_left = lax.broadcasted_iota(jnp.int32, (HS, WIDE), 1) < FEAT

    def pack(v):
        return jnp.where(lane_left, v[:HS], swap(v[HS:]))

    e0 = ei0[...].astype(F32)
    item0 = pack(jnp.concatenate([e0, jnp.zeros_like(e0)], axis=1))
    tbl0[core, q, z] = item0.astype(BF16)
    user0 = eu0[...].astype(F32)
    ed0[...] = jnp.transpose(jnp.concatenate([user0, user0], axis=0)).astype(BF16)
    pl.semaphore_wait(barrier, (C - 1) + (Y - 1) + (R - 1) + 2 * (X - 1) * (Y - 1))

    def gather_z(tbl, sem):
        each(1, Z, lambda k: remote(tbl.at[core, q, z], tbl.at[core, q, z], sem, row, ((z + k) % Z) * Y + y).start())

    def gather_q(tbl, sem):
        await_recv(tbl.at[core, q, pl.ds(0, Z - 1)], sem)
        each(1, Q, lambda k: remote(tbl.at[core, q], tbl.at[core, q], sem + 1, *at_q((q + k) % Q)).start())

    def gather_d(tbl, sem):
        await_recv(tbl.at[core, pl.ds(0, Q - 1)], sem + 1)
        remote(tbl.at[core], tbl.at[core], sem + 2, mate, col).start()

    def gather_end(tbl, sem):
        await_recv(tbl.at[core], sem + 2)

    def gather_sent(tbl, sem):
        await_send(tbl.at[core, q, pl.ds(0, Z - 1)], sem)
        await_send(tbl.at[core, pl.ds(0, Q - 1)], sem + 1)
        await_send(tbl.at[core], sem + 2)

    def rows_of(tbl, c):
        cz, cy = c // Y, c % Y
        parts = []
        for i in range(R):
            v = tbl[i % 2, cy * X + i // 2, cz].astype(F32)
            parts += [v, swap(v)]
        return jnp.concatenate(parts, axis=0).astype(BF16)

    def order(k):
        j = k // Y
        m = (j + 1) // 2
        odd = j % 2
        return (odd * m + (1 - odd) * (Z - m)) % Z, k % Y

    def target(k):
        dz, dy = order(k)
        return ((z + dz) % Z) * Y + (y + dy) % Y

    each(1, C, lambda k: remote(deg_s.at[(col + k) % C], deg_r.at[col], DEG, row, (col + k) % C).start())
    each(1, R, lambda k: remote(ideg.at[row], ideg.at[row], IDEG, (row + k) % R, col).start())
    gather_z(tbl0, GATHER0)
    await_recv(deg_r.at[pl.ds(0, C - 1)], DEG)
    own_deg[...] = lax.fori_loop(0, C, lambda k, t: t + deg_r[k], jnp.zeros((1, UD), F32), unroll=True)
    deg_f[col] = own_deg[...]
    each(1, C, lambda k: remote(own_deg, deg_f.at[col], SPREAD, row, target(k), recv=spread_recv.at[col]).start())
    await_recv(ideg.at[pl.ds(0, R - 1)], IDEG)
    scale_item = lax.rsqrt(jnp.maximum(lax.fori_loop(0, R, lambda k, t: t + ideg[k], jnp.zeros((1, IB), F32), unroll=True), 1.0))
    gather_q(tbl0, GATHER0)

    def piece(c):
        scale = lax.rsqrt(jnp.maximum(deg_f[c], 1.0))
        scale = jnp.transpose(jnp.broadcast_to(scale, (IB, UD)))
        return (mask[c].astype(F32) * scale * scale_item).astype(BF16)

    def ship(k):
        to = target(k)
        remote(send_a.at[to], slab.at[col], ATOA, row, to, recv=a2a_recv.at[col]).start()

    def make(k):
        to = target(k)
        remote(deg_f.at[to], deg_f.at[to], SPREAD, row, col, recv=spread_recv.at[to]).wait_recv()
        send_a[to] = piece(to)

    make(1)

    def make_and_ship(k):
        make(k)
        ship(k - 1)

    each(2, C, make_and_ship)
    slab[col] = piece(col)
    ship(C - 1)
    gather_d(tbl0, GATHER0)
    gather_end(tbl0, GATHER0)

    def scatter_a(n, g, ed):
        p, rd = rs[n][0], rs[n][1]
        per = Z // groups[n]

        def block(k):
            zi, cy = k // Y, k % Y
            val = jnp.dot(slab_t[(g * per + zi) * Y + cy], ed[...], preferred_element_type=F32)
            for i in range(R):
                p[i % 2, g, cy * X + i // 2, zi] = jnp.where(lane_left, val[i * SH:i * SH + HS], val[i * SH + HS:(i + 1) * SH])

        lax.fori_loop(0, per * Y, lambda k, t: (block(k), t)[1], 0, unroll=4)
        remote(p.at[1 - core, g], rd.at[g], base[n], mate, col, recv=recvs.at[base[n] + g]).start()

    def scatter_b(n, g):
        p, rd, s1, rxy, _, _ = rs[n]
        remote(rd.at[g], rd.at[g], base[n], row, col, recv=recvs.at[base[n] + g]).wait_recv()

        def fold(k):
            to = (q + k) % Q
            s1[g, to] = p[core, g, to] + rd[g, to]

        def go(k):
            to = (q + k) % Q
            remote(s1.at[g, to], rxy.at[g, q], base[n] + 1, *at_q(to), recv=recvs.at[base[n] + groups[n] + g]).start()

        def both(k):
            fold(k)
            go(k - 1)

        fold(1)
        each(2, Q, both)
        rxy[g, q] = p[core, g, q] + rd[g, q]
        go(Q - 1)

    def scatter_c(n, g):
        _, _, _, rxy, s2, rz = rs[n]
        per = Z // groups[n]
        part = rxy.at[g, pl.ds(0, Q - 1)]
        remote(part, part, base[n], row, col, recv=recvs.at[base[n] + groups[n] + g]).wait_recv()
        for zi in range(per):
            to = g * per + zi
            s2[to] = lax.fori_loop(1, Q, lambda k, t: t + rxy[g, k, zi], rxy[g, 0, zi], unroll=True)
        for zi in range(per):
            to = g * per + zi

            @pl.when(to != z)
            def _():
                remote(s2.at[to], rz.at[z], base[n] + 2, row, to * Y + y, recv=recvs.at[base[n] + 2 * groups[n]]).start()

            @pl.when(to == z)
            def _():
                rz[z] = s2[to]

    def scatter_end(n):
        rz = rs[n][5]
        part = rz.at[pl.ds(0, Z - 1)]
        remote(part, part, base[n], row, col, recv=recvs.at[base[n] + 2 * groups[n]]).wait_recv()
        return lax.fori_loop(1, Z, lambda k, t: t + rz[k], rz[0], unroll=True).astype(BF16)

    def scatter_sent(n):
        p, _, s1, _, s2, _ = rs[n]
        await_send(p.at[0], base[n])
        await_send(s1.at[:, pl.ds(0, Q - 1)], base[n] + 1)
        await_send(s2.at[pl.ds(0, Z - 1)], base[n] + 2)

    def remote1(src, dst, k, r, c, recv):
        return pltpu.make_async_remote_copy(
            src_ref=src, dst_ref=dst, send_sem=one_send.at[k], recv_sem=recv, device_id=(c, r), device_id_type=MESH)

    def await1(ref, recv):
        remote1(ref, ref, 0, row, col, recv).wait_recv()

    def first_a(g):
        def block(cy):
            val = jnp.dot(slab_t[g * Y + cy], ed0[...], preferred_element_type=F32)
            for i in range(R):
                p_1[i % 2, g, i // 2, cy] = jnp.where(lane_left, val[i * SH:i * SH + HS], val[i * SH + HS:(i + 1) * SH])

        lax.fori_loop(0, Y, lambda k, t: (block(k), t)[1], 0, unroll=4)
        remote1(p_1.at[1 - core, g], rd_1.at[g], 0, mate, col, one_d.at[g]).start()

    def first_b(g):
        await1(rd_1.at[g], one_d.at[g])
        for k in range(1, X):
            to = (x + k) % X
            s1_1[g, to] = p_1[core, g, to] + rd_1[g, to]
        rx_1[g, x] = p_1[core, g, x] + rd_1[g, x]
        for k in range(1, X):
            to = (x + k) % X
            remote1(s1_1.at[g, to], rx_1.at[g, x], 1, to * 2 + core, col, one_x.at[g]).start()

    def first_c(g):
        await1(rx_1.at[g, pl.ds(0, X - 1)], one_x.at[g])
        total = rx_1[g, 0]
        for k in range(1, X):
            total = total + rx_1[g, k]
        for cy in range(Y):
            sy_1[cy, g] = total[cy]

    def first_y():
        for k in range(1, Y):
            to = (y + k) % Y
            remote1(sy_1.at[to], ry_1.at[y], 2, row, z * Y + to, one_yz.at[0]).start()
        ry_1[y] = sy_1[y]

    def first_z():
        await1(ry_1.at[pl.ds(0, Y - 1)], one_yz.at[0])
        total = ry_1[0]
        for k in range(1, Y):
            total = total + ry_1[k]
        s2_1[...] = total
        rz_1[z] = s2_1[z]
        each(1, Z, lambda k: remote1(s2_1.at[(z + k) % Z], rz_1.at[z], 3, row, ((z + k) % Z) * Y + y, one_yz.at[1]).start())

    def first_end():
        await1(rz_1.at[pl.ds(0, Z - 1)], one_yz.at[1])
        return lax.fori_loop(1, Z, lambda k, t: t + rz_1[k], rz_1[0], unroll=True).astype(BF16)

    def first_sent():
        for k, ref in enumerate((p_1.at[0], s1_1.at[:, pl.ds(0, X - 1)], sy_1.at[pl.ds(0, Y - 1)], s2_1.at[pl.ds(0, Z - 1)])):
            remote1(ref, ref, k, row, col, one_yz.at[0]).wait_send()

    def source(k):
        dz, dy = order(k)
        return ((z - dz + Z) % Z) * Y + (y - dy + Y) % Y

    def use(c):
        blk = slab[c]
        slab_t[c] = jnp.transpose(blk)
        acc[...] += jnp.dot(blk, rows_of(tbl0, c), preferred_element_type=F32)

    def arrive(k):
        c = source(k)
        pltpu.make_async_remote_copy(src_ref=slab.at[c], dst_ref=slab.at[c], send_sem=sends.at[ATOA], recv_sem=a2a_recv.at[c],
                                     device_id=(col, row), device_id_type=MESH).wait_recv()
        use(c)

    def group(j):
        return source(j * Y) // Y

    acc[...] = jnp.zeros_like(acc)
    use(col)
    each(1, Y, arrive)
    first_a(z)

    def stream(j):
        each(j * Y, (j + 1) * Y, arrive)
        first_a(group(j))
        first_b(group(j - 1))

        @pl.when(j >= 2)
        def _():
            first_c(group(j - 2))

    each(1, Z, stream)
    wide_left = lax.broadcasted_iota(jnp.int32, (UD, WIDE), 1) < FEAT

    def twice(v):
        return jnp.where(wide_left, v, swap(v)).astype(BF16)

    user1 = acc[...].astype(BF16).astype(F32)
    ed1[...] = twice(user1)
    for g in range(G2):
        scatter_a(1, g, ed1)
        if g == 0:
            first_b(group(Z - 1))
        else:
            scatter_b(1, g - 1)
    first_c(group(Z - 2))
    first_c(group(Z - 1))
    first_y()
    scatter_b(1, G2 - 1)
    first_z()
    for g in range(G2):
        scatter_c(1, g)
    item1 = first_end().astype(F32)
    item2 = scatter_end(1).astype(F32)
    low = jnp.where(lane_left, item1, swap(item2))
    high = jnp.where(lane_left, swap(item1), item2)
    tbl1[core, q, z] = jnp.concatenate([low, high], axis=0).astype(BF16)
    gather_z(tbl1, GATHER1)
    gather_q(tbl1, GATHER1)
    gather_d(tbl1, GATHER1)
    acc[...] = jnp.zeros_like(acc)
    gather_end(tbl1, GATHER1)

    def absorb(c):
        cz, cy = c // Y, c % Y
        rows = jnp.concatenate([tbl1[i % 2, cy * X + i // 2, cz] for i in range(R)], axis=0)
        acc[...] += jnp.dot(slab[c], rows, preferred_element_type=F32)

    lax.fori_loop(0, C, lambda k, t: (absorb(k), t)[1], 0, unroll=4)
    late = acc[...].astype(BF16).astype(F32)
    ed2[...] = twice(late)
    sum_user = ((ed0[...].astype(F32) + ed1[...].astype(F32)) + ed2[...].astype(F32)) + jnp.where(wide_left, swap(late), late)
    user_rows = (sum_user / (LAYERS + 1)).astype(BF16)

    ids = lax.broadcasted_iota(jnp.int32, (UD, TRIPLES), 0) + (row * C + col) * UD
    hit = (ids == trip[0:1, :]).astype(BF16)
    found = lax.dot_general(hit, user_rows, (((0,), (0,)), ((), ())), preferred_element_type=F32)
    pick_left = lax.broadcasted_iota(jnp.int32, (PICKS, WIDE), 1) < FEAT
    for h in range(2):
        lo, hi = h * PICKS, (h + 2) * PICKS
        pk_a[h] = jnp.where(pick_left, found[lo:lo + PICKS], found[hi:hi + PICKS]).astype(BF16)
    remote(pk_a.at[1 - core], pk_b, PICK, mate, col).start()
    scatter_a(2, 0, ed2)
    for g in range(1, G2):
        scatter_a(2, g, ed2)
        if g == 1:
            await_recv(pk_b, PICK)
            pk_z[z] = (pk_a[core].astype(F32) + pk_b[...].astype(F32)).astype(BF16)
            each(1, Z, lambda k: remote(pk_z.at[z], pk_z.at[z], PICK + 1, row, ((z + k) % Z) * Y + y).start())
        scatter_b(2, g - 1)
    scatter_b(2, G2 - 1)
    out_user[...] = jnp.transpose(user_rows.astype(F32))[:FEAT].astype(BF16)
    await_recv(pk_z.at[pl.ds(0, Z - 1)], PICK + 1)
    pk_q[q] = lax.fori_loop(1, Z, lambda k, t: t + pk_z[k].astype(F32), pk_z[0].astype(F32), unroll=True).astype(BF16)
    each(1, Q, lambda k: remote(pk_q.at[q], pk_q.at[q], PICK + 2, *at_q((q + k) % Q)).start())
    for g in range(G2):
        scatter_c(2, g)
    await_recv(pk_q.at[pl.ds(0, Q - 1)], PICK + 2)
    pk_d[core] = lax.fori_loop(1, Q, lambda k, t: t + pk_q[k].astype(F32), pk_q[0].astype(F32), unroll=True).astype(BF16)
    remote(pk_d.at[core], pk_d.at[core], PICK + 3, mate, col).start()
    item3 = scatter_end(2)
    sum_item = ((item0 + item1) + item2) + item3.astype(F32)
    packed = (sum_item / (LAYERS + 1)).astype(BF16).astype(F32)
    zero = jnp.zeros_like(packed)
    left_rows = [jnp.where(lane_left, packed, zero), jnp.where(lane_left, swap(packed), zero)]
    right_rows = [jnp.where(lane_left, zero, swap(packed)), jnp.where(lane_left, zero, packed)]
    item_rows = jnp.concatenate(left_rows, axis=0).astype(BF16)
    out_item[...] = item_rows[:, :FEAT]

    await_recv(pk_d.at[0], PICK + 3)
    user_vec = jnp.concatenate([pk_d[0], pk_d[1], pk_d[0], pk_d[1]], axis=0)
    nt = (((1,), (1,)), ((), ()))
    dots_l = lax.dot_general(item_rows, user_vec, nt, preferred_element_type=F32)
    dots_r = lax.dot_general(jnp.concatenate(right_rows, axis=0).astype(BF16), user_vec, nt, preferred_element_type=F32)
    dots = jnp.where(lax.broadcasted_iota(jnp.int32, (SH, TRIPLES), 1) < TRIPLES // 2, dots_l, dots_r)
    own = lax.broadcasted_iota(jnp.int32, (SH, TRIPLES), 0) + (col * R + row) * SH
    pos = jnp.sum(jnp.where(own == trip[1:2, :], dots, 0.0), axis=0, keepdims=True)
    neg = jnp.sum(jnp.where(own == trip[2:3, :], dots, 0.0), axis=0, keepdims=True)
    mine = q * 2 + core
    xc[mine] = pos - neg

    def spread_margin(k):
        to = (mine + k) % (2 * Q)
        remote(xc.at[mine], xc.at[mine], MARGIN, ((to // 2) % X) * 2 + to % 2, z * Y + to // (2 * X)).start()

    each(1, 2 * Q, spread_margin)
    await_recv(xc.at[pl.ds(0, 2 * Q - 1)], MARGIN)
    xr[z] = lax.fori_loop(1, 2 * Q, lambda k, t: t + xc[k], xc[0], unroll=True)
    each(1, Z, lambda k: remote(xr.at[z], xr.at[z], MARGIN + 1, row, ((z + k) % Z) * Y + y).start())
    await_recv(xr.at[pl.ds(0, Z - 1)], MARGIN + 1)
    margin = lax.fori_loop(1, Z, lambda k, t: t + xr[k], xr[0], unroll=True)
    soft = jnp.maximum(-margin, 0.0) + jnp.log1p(jnp.exp(-jnp.abs(margin)))
    loss[...] = jnp.sum(soft, axis=1, keepdims=True) / TRIPLES

    await_send(deg_s.at[pl.ds(0, C - 1)], DEG)
    await_send(ideg.at[pl.ds(0, R - 1)], IDEG)
    await_send(deg_f.at[pl.ds(0, C - 1)], SPREAD)
    await_send(send_a.at[pl.ds(0, C - 1)], ATOA)
    gather_sent(tbl0, GATHER0)
    gather_sent(tbl1, GATHER1)
    first_sent()
    for n in (1, 2):
        scatter_sent(n)
    await_send(pk_b, PICK)
    await_send(pk_z.at[pl.ds(0, Z - 1)], PICK + 1)
    await_send(pk_q.at[pl.ds(0, Q - 1)], PICK + 2)
    await_send(pk_d.at[0], PICK + 3)
    await_send(xc.at[pl.ds(0, 2 * Q - 1)], MARGIN)
    await_send(xr.at[pl.ds(0, Z - 1)], MARGIN + 1)


def emit(user_in, item_in, loss_in, user_out, item_out, loss_out):
    user_out[...] = user_in[...]
    item_out[...] = item_in[...]
    loss_out[...] = loss_in[...]


def build(mesh, Y, SH, UD, G2):
    C, R = mesh.shape["col"], mesh.shape["row"]
    Z, X = C // Y, R // 2
    Q, IB, HS = Y * X, R * SH, SH // 2
    vm = pltpu.VMEM
    scratch = [
        vm((C, 1, UD), F32), vm((C, 1, UD), F32), vm((C, 1, UD), F32), vm((1, UD), F32), vm((R, 1, IB), F32),
        vm((C, UD, IB), BF16), vm((C, UD, IB), BF16), vm((C, IB, UD), BF16),
        vm((2, Q, Z, HS, WIDE), BF16), vm((2, Q, Z, SH, WIDE), BF16),
        vm((UD, WIDE), F32), vm((UD, WIDE), BF16), vm((UD, WIDE), BF16), vm((UD, WIDE), BF16),
        vm((2, PICKS, WIDE), BF16), vm((PICKS, WIDE), BF16),
        vm((Z, PICKS, WIDE), BF16), vm((Q, PICKS, WIDE), BF16), vm((2, PICKS, WIDE), BF16),
        vm((2 * Q, 1, TRIPLES), F32), vm((Z, 1, TRIPLES), F32),
    ]
    count = SCATTER1 + 2 * (2 * G2 + 1)
    sem = pltpu.SemaphoreType.DMA
    scratch += [sem((count,)), sem((count,)), sem((C,)), vm((C, UD, IB), jnp.int32), sem((LOADS,))]
    scratch += [
        vm((2, Z, X, Y, HS, WIDE), F32), vm((Z, X, Y, HS, WIDE), F32), vm((Z, X, Y, HS, WIDE), F32), vm((Z, X, Y, HS, WIDE), F32),
        vm((Y, Z, HS, WIDE), F32), vm((Y, Z, HS, WIDE), F32), vm((Z, HS, WIDE), F32), vm((Z, HS, WIDE), F32),
        sem((4,)), sem((Z,)), sem((Z,)), sem((2,)),
    ]
    for g in (G2, G2):
        scratch += [vm((2, g, Q, Z // g, HS, WIDE), F32)] + [vm((g, Q, Z // g, HS, WIDE), F32)] * 3 + [vm((Z, HS, WIDE), F32)] * 2
    scratch += [sem((C,))]
    dims = (Z, Y, X, SH, UD, G2)

    def local_prog(mask_blk, user_shard, item_shard, triples):
        out_user, out_item, loss = pl.pallas_call(
            functools.partial(kernel, dims),
            out_shape=(
                jax.ShapeDtypeStruct((FEAT, UD), BF16),
                jax.ShapeDtypeStruct((SH, FEAT), BF16),
                jax.ShapeDtypeStruct((1, 1), F32),
            ),
            in_specs=[pl.BlockSpec(memory_space=pl.ANY)] + [pl.BlockSpec(memory_space=pltpu.VMEM)] * 3,
            out_specs=(pl.BlockSpec(memory_space=pltpu.VMEM),) * 3,
            scratch_shapes=scratch,
            compiler_params=pltpu.CompilerParams(
                collective_id=0, has_side_effects=True, vmem_limit_bytes=60 * 1024 * 1024),
            name="lightgcn",
        )(mask_blk.reshape(C, UD, IB), user_shard.T, item_shard, triples.T)
        out_user, out_item, loss = pl.pallas_call(
            emit,
            out_shape=(
                jax.ShapeDtypeStruct((FEAT, UD), BF16),
                jax.ShapeDtypeStruct((SH, FEAT), BF16),
                jax.ShapeDtypeStruct((1, 1), F32),
            ),
            in_specs=[pl.BlockSpec(memory_space=pltpu.VMEM)] * 3,
            out_specs=(pl.BlockSpec(memory_space=pltpu.VMEM),) * 3,
            name="emit",
        )(out_user, out_item, loss)
        return out_user.T, out_item, loss[0, 0]

    return jax.shard_map(
        local_prog, mesh=mesh,
        in_specs=(P("row", "col"), P(("row", "col"), None), P(("col", "row"), None), P(None, None)),
        out_specs=(P(("row", "col"), None), P(("col", "row"), None), P()), check_vma=False)


def solution(mesh):
    return build(mesh, Y=4, SH=16, UD=256, G2=8)
```
